32 devices in a mesh: dp: 4 (over z), ctx: 8 (over y, x, core).
Axes of the slice: x: 2, y: 2, z: 4, core: 2. Of those that a mesh axis runs over, the one named last changes fastest.
Arguments:
- tokens: bfloat16 [4, 4096, 1024], P('dp', 'ctx'), may hold values from -60 to 60
- kept: int32 [4, 2048], P('dp', 'ctx'), may hold values from 0 to 4095, as said below
- gain_attn: float32 [1024], replicated, may hold values from 0.25 to 1.75
- gain_ffn: float32 [1024], replicated, may hold values from 0.25 to 1.75
- w_query: bfloat16 [1024, 512], P(None, 'ctx'), may hold values from -4 to 4
- w_key: bfloat16 [1024, 512], P(None, 'ctx'), may hold values from -4 to 4
- w_value: bfloat16 [1024, 512], P(None, 'ctx'), may hold values from -0.1875 to 0.1875
- w_out: bfloat16 [512, 1024], P('ctx'), may hold values from -0.25 to 0.25
- expert_ids: int32 [4, 2048, 1], P('dp', 'ctx'), may hold values from 0 to 31; in each aligned block of 256 rows (0 to 255, 256 to 511, ..., all dimensions but the last counted through in order) at most 16 rows name the same one
- w_in: bfloat16 [32, 1024, 2816], P(('dp', 'ctx')), may hold values from -0.1875 to 0.1875
- w_back: bfloat16 [32, 2816, 1024], P(('dp', 'ctx')), may hold values from -0.109375 to 0.109375
Outputs:
- blended: bfloat16 [4, 4096, 1024], P('dp', 'ctx')
The draws below stay inside these ranges and needn't reach their ends.
Inputs may be any that keep to these rules, and one draw needn't show every extreme that they name: `kept`: in each document row, entries j * 256 to (j + 1) * 256 - 1 are strictly increasing positions from j * 512 to (j + 1) * 512 - 1. `expert_ids`: in each aligned block of 256 rows (the kept positions of one block b) no expert is named more than 16 times.
All inputs are finite; a program needn't handle non-finite values.
Results may differ from the reference program's by a relative error of at most 0.007.
Values may be sent and summed in bfloat16 or wider, within the bound.
A program may use at most 64 MiB of HBM per device.

```python
import math
import jax
import jax.numpy as jnp
import numpy as np
from jax import lax

D = 1024
HS = 64
FF = 2816
SHARD_DEV = 512
HEADS = 8
EXPERTS = 32
INNER = 512
KEEP_DEV = 256
KEEP = 2048
SEQ = 4096
DOCS = 4
CAP = 16
DEVICES = 32


def draw_tokens(key, part):
    noise = jax.random.normal(jax.random.fold_in(key, 1), (DOCS, SEQ, D), jnp.float32)
    return jnp.clip(noise, -6.0, 6.0).astype(jnp.bfloat16)


def draw_projection(key, salt):
    base = jax.random.normal(jax.random.fold_in(key, salt), (D, INNER), jnp.float32) / math.sqrt(D)
    return jnp.clip(base, -4.0, 4.0).astype(jnp.bfloat16)


def draw_w_query(key, part):
    return draw_projection(key, 3)


def draw_w_key(key, part):
    return draw_projection(key, 4)


def draw_kept(key, part):
    shards = SEQ // SHARD_DEV
    streams = jax.random.split(jax.random.fold_in(key, 5), DOCS * shards)

    def choose_some(stream):
        return jnp.sort(jax.random.permutation(stream, SHARD_DEV)[:KEEP_DEV].astype(jnp.int32))
    chosen = jax.vmap(choose_some)(streams).reshape(DOCS, shards, KEEP_DEV)
    offsets = (jnp.arange(shards, dtype=jnp.int32) * SHARD_DEV)[None, :, None]
    return (chosen + offsets).reshape(DOCS, KEEP).astype(jnp.int32)


def level_of(stream_key, shape, cuts, smallest, largest):
    level = 1.0
    for dim, parts in cuts:
        draws = jax.random.uniform(jax.random.fold_in(jax.random.fold_in(stream_key, 6), dim), (parts,), jnp.float32, smallest / len(cuts), largest / len(cuts))
        level = level * jnp.repeat(jnp.exp(draws), shape[dim] // parts).reshape((-1,) + (1,) * (len(shape) - 1 - dim))
    return level


def deal_out(own_key, own, number, rows, count, top, limit, skew):
    order = jax.random.permutation(own_key, count)
    crowded, ordinary = shares(count, rows * top, limit, skew, True), shares(count, rows * top, limit, skew, False)
    places = jnp.arange(count)

    def named(tallies, offset_by):
        used = int((tallies > 0).sum())
        fixed = max(1, used // 4)
        shifted = fixed + (places - fixed + offset_by * (used - fixed)) % max(1, count - fixed)
        return jnp.zeros((count,), jnp.int32).at[order[jnp.where(places < fixed, places, shifted)]].set(jnp.asarray(tallies, jnp.int32))

    tallies = jnp.where(number % 4 == 0, named(crowded, number // 4), named(ordinary, number - number // 4 - 1))
    mixed = jax.random.permutation(jax.random.fold_in(own, 3), count)
    donor, taker = mixed[0:count // 2 * 2:2], mixed[1:count // 2 * 2:2]
    room = jnp.minimum(tallies[donor] - 1, limit - tallies[taker]) // 2
    room = jnp.where((donor == order[0]) | (taker == order[0]) | (tallies[taker] == 0), 0, jnp.maximum(room, 0))
    shifted = jax.random.randint(jax.random.fold_in(own, 4), (count // 2,), 0, 1 << 20) % (room + 1)
    tallies = tallies.at[donor].add(-shifted).at[taker].add(shifted)
    labels = jnp.searchsorted(jnp.cumsum(tallies), jnp.arange(rows * top), side="right").astype(jnp.int32)
    table = labels.reshape(top, rows).T
    table = table[jax.random.permutation(jax.random.fold_in(own, 1), rows)]
    offset_by = jax.random.randint(jax.random.fold_in(own, 2), (rows, 1), 0, top)
    return jnp.take_along_axis(table, (jnp.arange(top)[None, :] + offset_by) % top, axis=1)


def shares(number_of, total, most, skew, full):
    portions = [(1 << 20) // math.isqrt(standing ** skew) + 1 for standing in range(1, number_of + 1)]
    largest = most if full else min(most, max(-(-total // number_of), total * portions[0] // sum(portions)))
    least = 1 if total - largest >= number_of - 1 else 0
    holding, rest = [largest] + [least] * (number_of - 1), total - largest - least * (number_of - 1)
    while rest > 0:
        movable = [i for i in range(1, number_of) if holding[i] < largest] or [i for i in range(1, number_of) if holding[i] < most]
        whole, budget = sum([portions[i] for i in movable]), rest
        for i in movable:
            addition = min(most - holding[i], max(1, budget * portions[i] // whole), rest)
            holding[i] = holding[i] + addition
            rest = rest - addition
    return np.array(holding)


def normal_values(stream_key, shape, deviation, limit, cuts=(), kind=jnp.bfloat16):
    level = level_of(stream_key, shape, cuts, -0.22, 0.18) if cuts else 1.0
    values = jax.random.normal(stream_key, shape, jnp.float32) * deviation * level
    return jnp.minimum(jnp.maximum(values, -limit), limit).astype(kind)


def setup_inputs(seed: int = 0) -> dict:
    splits = jax.random.split(jax.random.key(seed), 12)
    tokens = draw_tokens(jax.random.fold_in(splits[11], 71), 0)
    kept = draw_kept(jax.random.fold_in(splits[11], 71), 0)
    gain_attn = jnp.clip(1.0 + 0.15 * jax.random.normal(splits[2], (D,), jnp.float32), 0.25, 1.75)
    gain_ffn = jnp.clip(1.0 + 0.15 * jax.random.normal(splits[3], (D,), jnp.float32), 0.25, 1.75)
    w_query = draw_w_query(jax.random.fold_in(splits[11], 71), 0)
    w_key = draw_w_key(jax.random.fold_in(splits[11], 71), 0)
    w_value = normal_values(splits[6], (D, INNER), D ** -0.5, 0.1875, ((1, 8),))
    w_out = normal_values(splits[7], (INNER, D), INNER ** -0.5, 0.25, ((0, 8),))
    expert_ids_keys = jax.random.split(jax.random.fold_in(splits[8], 1), DOCS * KEEP // KEEP_DEV)
    expert_ids_turns = jax.random.permutation(jax.random.fold_in(splits[8], 3), DOCS * KEEP // KEEP_DEV)
    expert_ids = jax.vmap(lambda own, number: deal_out(jax.random.fold_in(splits[8], 2), own, number, KEEP_DEV, EXPERTS, 1, CAP, 1))(expert_ids_keys, expert_ids_turns).reshape((DOCS, KEEP, 1))
    w_in = normal_values(splits[9], (EXPERTS, D, FF), D ** -0.5, 0.1875, ((0, 32),))
    w_back = normal_values(splits[10], (EXPERTS, FF, D), FF ** -0.5, 0.109375, ((0, 32),))
    return {"tokens": tokens, "kept": kept, "gain_attn": gain_attn, "gain_ffn": gain_ffn, "w_query": w_query, "w_key": w_key, "w_value": w_value, "w_out": w_out, "expert_ids": expert_ids, "w_in": w_in, "w_back": w_back}


eps_norm = 1e-06
score_gain = 2.5

def rms_scale(values, gain):
    values = values.astype(jnp.float32)
    power = lax.optimization_barrier(jnp.mean(values * values, axis=-1, keepdims=True))
    return values * lax.rsqrt(power + eps_norm) * gain

def attend_document(triple):
    queries, keys, values = triple
    scale = score_gain / math.sqrt(HS)
    keys_wide = keys.astype(jnp.float32)
    values_wide = values.astype(jnp.float32)
    blocks = queries.reshape(KEEP // 512, 512, HEADS, HS)

    def one_block(block_rows):
        scores = jnp.einsum('qhd,khd->hqk', block_rows.astype(jnp.float32), keys_wide) * scale
        top = lax.optimization_barrier(jnp.max(scores, axis=-1, keepdims=True))
        weights = jnp.exp(scores - top)
        probs = (weights / lax.optimization_barrier(jnp.sum(weights, axis=-1, keepdims=True))).astype(jnp.bfloat16)
        mixed = jnp.einsum('hqk,khd->qhd', probs.astype(jnp.float32), values_wide)
        return mixed.astype(jnp.bfloat16)
    return lax.map(one_block, blocks).reshape(KEEP, HEADS * HS)

def reference(tokens, kept, gain_attn, gain_ffn, w_query, w_key, w_value, w_out, expert_ids, w_in, w_back):
    rows = jax.vmap(lambda doc, where: jnp.take(doc, where, axis=0))(tokens, kept)
    normed = rms_scale(rows, gain_attn).astype(jnp.bfloat16).reshape(DOCS * KEEP, D)
    queries = jnp.dot(normed, w_query, preferred_element_type=jnp.float32).astype(jnp.bfloat16)
    keys = jnp.dot(normed, w_key, preferred_element_type=jnp.float32).astype(jnp.bfloat16)
    values = jnp.dot(normed, w_value, preferred_element_type=jnp.float32).astype(jnp.bfloat16)
    shape4 = (DOCS, KEEP, HEADS, HS)
    mixed = lax.map(attend_document, (queries.reshape(shape4), keys.reshape(shape4), values.reshape(shape4)))
    attn = jnp.dot(mixed.reshape(DOCS * KEEP, INNER), w_out, preferred_element_type=jnp.float32)
    first = rows.reshape(DOCS * KEEP, D).astype(jnp.float32) + attn
    ffn_in = rms_scale(first, gain_ffn).astype(jnp.bfloat16)
    ids = expert_ids.reshape(DEVICES, KEEP_DEV).astype(jnp.int32)
    onehot = (ids[:, :, None] == jnp.arange(EXPERTS, dtype=jnp.int32)[None, None, :]).astype(jnp.int32)
    before = jnp.cumsum(onehot, axis=1) - onehot
    slots = lax.optimization_barrier(jnp.sum(before * onehot, axis=2)).astype(jnp.int32)
    place = (ids * CAP + slots).astype(jnp.int32)
    source = jnp.broadcast_to(jnp.arange(DEVICES, dtype=jnp.int32)[:, None], (DEVICES, KEEP_DEV))
    buffers = jnp.zeros((DEVICES, EXPERTS * CAP, D), jnp.bfloat16)
    buffers = buffers.at[source, place].set(ffn_in.reshape(DEVICES, KEEP_DEV, D))
    slabs = jnp.transpose(buffers.reshape(DEVICES, EXPERTS, CAP, D), (1, 0, 2, 3))

    def run_expert(args):
        slab, first_weight, second_weight = args
        flat_in = slab.reshape(DEVICES * CAP, D)
        hidden = jnp.maximum(jnp.dot(flat_in, first_weight, preferred_element_type=jnp.float32), 0.0)
        hidden = hidden.astype(jnp.bfloat16)
        answer = jnp.dot(hidden, second_weight, preferred_element_type=jnp.float32).astype(jnp.bfloat16)
        return answer.reshape(DEVICES, CAP, D)
    answers = lax.map(run_expert, (slabs, w_in, w_back))
    back = jnp.transpose(answers, (1, 0, 2, 3)).reshape(DEVICES, EXPERTS * CAP, D)
    taken = jnp.take_along_axis(back, place[:, :, None], axis=1)
    second = (first + taken.reshape(DOCS * KEEP, D).astype(jnp.float32)).astype(jnp.bfloat16)
    second = second.reshape(DOCS, KEEP, D)
    return jax.vmap(lambda doc, where, fresh: doc.at[where].set(fresh))(tokens, kept, second)
```

```python
import functools
import math

import jax
import jax.numpy as jnp
from jax import lax
from jax.experimental import pallas as pl
from jax.experimental.pallas import tpu as pltpu
from jax.sharding import PartitionSpec as P

HS = 64
MESH = pl.DeviceIdType.MESH
LAST = (((1,), (1,)), ((), ()))

eps_norm = 1e-06
score_gain = 2.5


def rms_scale(values, gain):
    values = values.astype(jnp.float32)
    power = jnp.mean(values * values, axis=-1, keepdims=True)
    return values * lax.rsqrt(power + eps_norm) * gain


class Gather:
    def __init__(self, n, me, own, slots, send, recv):
        self.n, self.me, self.own, self.slots = n, me, own, slots
        self.send, self.recv = send, recv
        self.core, self.chip = me % 2, me // 2
        self.partner = me + 1 - 2 * self.core
        self.started = []

    def copy(self, ident, src, dst, target):
        return pltpu.make_async_remote_copy(
            src_ref=src,
            dst_ref=dst,
            send_sem=self.send.at[ident],
            recv_sem=self.recv.at[ident],
            device_id={"ctx": target},
            device_id_type=MESH,
        )

    def peers(self):
        chips = self.n // 2
        if chips == 4:
            x, y = self.chip % 2, self.chip // 2
            nx, ny = y * 2 + (1 - x), (1 - y) * 2 + x
            return [(nx, nx), (ny, ny)]
        return [
            ((self.chip + d) % chips, (self.chip + chips - d) % chips) for d in range(1, chips)
        ]

    def begin(self):
        own_to = self.slots.at[self.me]
        self.first = [
            self.copy(i, self.own, own_to, to * 2 + self.core)
            for i, (to, _) in enumerate(self.peers())
        ]
        self.base = len(self.first)
        self.twin = self.copy(self.base, self.own, own_to, self.partner)
        for c in self.first:
            c.start()
        self.twin.start()
        self.started = self.first + [self.twin]

    def relay(self):
        here, self.passed, self.late = [], [], []
        ident = self.base + 1
        peers = self.peers()
        square = self.n // 2 == 4
        half = self.own.shape[0] // 2
        for i, (_, source) in enumerate(peers):
            self.first[i].wait_recv()
            block = source * 2 + self.core
            here.append(block)
            if square:
                piece = self.slots.at[block, pl.ds(i * half, half)]
                c = self.copy(ident, piece, piece, peers[1 - i][0] * 2 + self.core)
                c.start()
                self.late.append(c)
                ident += 1
            c = self.copy(ident, self.slots.at[block], self.slots.at[block], self.partner)
            c.start()
            self.passed.append((source * 2 + 1 - self.core, c))
            ident += 1
        self.ident = ident
        self.started += self.late + [c for _, c in self.passed]
        return here

    def diagonal(self):
        if not self.late:
            return None
        block = (3 - self.chip) * 2 + self.core
        half = self.own.shape[0] // 2
        self.last = []
        for i, c in enumerate(self.late):
            c.wait_recv()
            piece = self.slots.at[block, pl.ds(i * half, half)]
            c = self.copy(self.ident + i, piece, piece, self.partner)
            c.start()
            self.last.append(c)
        self.started += self.last
        return block

    def final(self):
        if not self.late:
            return None
        for c in self.last:
            c.wait_recv()
        return (3 - self.chip) * 2 + 1 - self.core

    def drain(self):
        for c in self.started:
            c.wait_send()


def gather_copies(n):
    return 9 if n // 2 == 4 else 2 * (n // 2) - 1


def attention_kernel(
    n,
    heads,
    x_ref,
    wq_ref,
    wk_ref,
    wv_ref,
    wo_ref,
    mixed_ref,
    wo_all,
    x_all,
    q_all,
    k_all,
    v_all,
    stage,
    x_send,
    x_recv,
    o_send,
    o_recv,
    m_send,
    m_recv,
):
    me = lax.axis_index("ctx")
    rows = x_ref.shape[0]
    barrier = pltpu.get_barrier_semaphore()
    for d in range(1, n):
        pl.semaphore_signal(
            barrier, inc=1, device_id={"ctx": (me + d) % n}, device_id_type=MESH
        )
    pl.semaphore_wait(barrier, n - 1)

    def project(block, value):
        at = pl.ds(pl.multiple_of(block * rows, rows), rows)
        for h in range(heads):
            cols = pl.ds(h * HS, HS)
            q_all[h, at, :] = lax.dot_general(
                value, wq_ref[cols, :], LAST, preferred_element_type=jnp.float32
            ).astype(jnp.bfloat16)
            k_all[h, at, :] = lax.dot_general(
                value, wk_ref[cols, :], LAST, preferred_element_type=jnp.float32
            ).astype(jnp.bfloat16)
        v_all[:, at] = lax.dot_general(
            wv_ref[...], value, LAST, preferred_element_type=jnp.float32
        ).astype(jnp.bfloat16)

    g = Gather(n, me, x_ref, x_all, x_send, x_recv)
    o = Gather(n, me, wo_ref, wo_all, o_send, o_recv)
    g.begin()
    project(me, x_ref[...])
    wo_all[me] = wo_ref[...]
    g.twin.wait_recv()
    project(g.partner, x_all[g.partner])
    here = g.relay()
    o.begin()
    for block in here:
        project(block, x_all[block])
    for block, c in g.passed:
        c.wait_recv()
        project(block, x_all[block])
    block = g.diagonal()
    if block is not None:
        project(block, x_all[block])
    o.twin.wait_recv()
    o.relay()
    block = g.final()
    if block is not None:
        project(block, x_all[block])

    scale = score_gain / math.sqrt(HS) * math.log2(math.e)

    def send_block(step, target):
        return pltpu.make_async_remote_copy(
            src_ref=stage.at[step],
            dst_ref=mixed_ref.at[me],
            send_sem=m_send.at[step],
            recv_sem=m_recv.at[step],
            device_id={"ctx": target},
            device_id_type=MESH,
        )

    @pl.loop(0, n)
    def _(step):
        block = lax.rem(me + 1 + step, n)
        at = pl.ds(pl.multiple_of(block * rows, rows), rows)
        for h in range(heads):
            scores = lax.dot_general(
                k_all[h],
                q_all[h, at, :],
                LAST,
                preferred_element_type=jnp.float32,
            )
            top = jnp.max(scores, axis=0, keepdims=True)
            weights = jnp.exp2(scores * scale - top * scale)
            total = jnp.sum(weights, axis=0, keepdims=True)
            cols = pl.ds(h * HS, HS)
            mixed = jnp.dot(
                v_all[cols, :],
                weights.astype(jnp.bfloat16),
                preferred_element_type=jnp.float32,
            )
            stage[step, cols, :] = (mixed / total).astype(jnp.bfloat16)

        @pl.when(step < n - 1)
        def _():
            send_block(step, block).start()

    mixed_ref[me] = stage[n - 1]
    for _, c in o.passed:
        c.wait_recv()
    o.diagonal()
    o.final()

    @pl.loop(0, n - 1)
    def _(step):
        send_block(step, lax.rem(me + 1 + step, n)).wait()

    g.drain()
    o.drain()


def attention(normed, w_query, w_key, w_value, w_out):
    n = lax.axis_size("ctx")
    rows, width = normed.shape
    inner = w_query.shape[1]
    heads = inner // HS
    copies = gather_copies(n)
    vmem = pl.BlockSpec(memory_space=pltpu.VMEM)
    bf = jnp.bfloat16
    return pl.pallas_call(
        functools.partial(attention_kernel, n, heads),
        out_shape=(
            jax.ShapeDtypeStruct((n, inner, rows), bf),
            jax.ShapeDtypeStruct((n,) + w_out.shape, bf),
        ),
        in_specs=[vmem] * 5,
        out_specs=(vmem, vmem),
        scratch_shapes=[
            pltpu.VMEM((n, rows, width), bf),
            pltpu.VMEM((heads, n * rows, HS), bf),
            pltpu.VMEM((heads, n * rows, HS), bf),
            pltpu.VMEM((inner, n * rows), bf),
            pltpu.VMEM((n, inner, rows), bf),
            pltpu.SemaphoreType.DMA((copies,)),
            pltpu.SemaphoreType.DMA((copies,)),
            pltpu.SemaphoreType.DMA((copies,)),
            pltpu.SemaphoreType.DMA((copies,)),
            pltpu.SemaphoreType.DMA((n,)),
            pltpu.SemaphoreType.DMA((n,)),
        ],
        compiler_params=pltpu.CompilerParams(collective_id=0, has_side_effects=True),
        name="attention",
    )(normed, w_query.T, w_key.T, w_value.T, w_out)


def experts_plain(buffer, w_in, w_back, capacity):
    owners = lax.axis_size("dp") * lax.axis_size("ctx")
    expert_here, width = w_in.shape[0], buffer.shape[1]
    buffer = buffer.reshape(owners * expert_here, capacity, width)
    received = lax.all_to_all(buffer, ("dp", "ctx"), split_axis=0, concat_axis=0, tiled=True)
    grouped = received.reshape(owners, expert_here, capacity, width)
    hidden = jnp.einsum("sgid,gdf->sgif", grouped, w_in, preferred_element_type=jnp.float32)
    hidden = jnp.maximum(hidden, 0.0).astype(jnp.bfloat16)
    answer = jnp.einsum("sgif,gfd->sgid", hidden, w_back, preferred_element_type=jnp.float32)
    answered = answer.astype(jnp.bfloat16).reshape(owners * expert_here, capacity, width)
    back = lax.all_to_all(answered, ("dp", "ctx"), split_axis=0, concat_axis=0, tiled=True)
    return back.reshape(owners * expert_here * capacity, width)


def expert_kernel(
    planes,
    n,
    cap,
    buf_ref,
    w_in_hbm,
    w_back_hbm,
    back_ref,
    w_in_ref,
    w_back_ref,
    rows_ref,
    hidden_ref,
    answer_ref,
    w_sem,
    own_sem,
    d_send,
    d_recv,
    r_send,
    r_recv,
):
    dp, ctx = lax.axis_index("dp"), lax.axis_index("ctx")
    me = dp * n + ctx
    owners = planes * n
    loads = [
        pltpu.make_async_copy(w_in_hbm.at[0], w_in_ref, w_sem.at[0]),
        pltpu.make_async_copy(w_back_hbm.at[0], w_back_ref, w_sem.at[1]),
    ]
    for c in loads:
        c.start()
    barrier = pltpu.get_barrier_semaphore()

    @pl.loop(1, owners)
    def _(d):
        to = lax.rem(me + d, owners)
        pl.semaphore_signal(
            barrier, inc=1, device_id={"dp": to // n, "ctx": lax.rem(to, n)}, device_id_type=MESH
        )

    pl.semaphore_wait(barrier, owners - 1)

    def seat(index):
        return pl.ds(pl.multiple_of(index * cap, cap), cap)

    def at(shift):
        plane_shift, place_shift = shift // n, lax.rem(shift, n)
        half = planes // 2
        side = dp // half
        side = lax.rem(side + plane_shift // half, 2)
        plane = side * half + lax.rem(dp + plane_shift, half)
        return plane, lax.rem(ctx + place_shift, n)

    def dispatch(shift):
        plane, place = at(shift)
        return pltpu.make_async_remote_copy(
            src_ref=buf_ref.at[seat(plane * n + place)],
            dst_ref=rows_ref.at[seat(me)],
            send_sem=d_send.at[shift],
            recv_sem=d_recv.at[shift],
            device_id={"dp": plane, "ctx": place},
            device_id_type=MESH,
        )

    def give_back(shift):
        plane, place = at(shift)
        return pltpu.make_async_remote_copy(
            src_ref=answer_ref.at[seat(plane * n + place)],
            dst_ref=back_ref.at[seat(me)],
            send_sem=r_send.at[shift],
            recv_sem=r_recv.at[shift],
            device_id={"dp": plane, "ctx": place},
            device_id_type=MESH,
        )

    near = owners // 2

    @pl.loop(0, near)
    def _(shift):
        dispatch(near + shift).start()

        @pl.when(shift > 0)
        def _():
            dispatch(shift).start()

    own_in = pltpu.make_async_copy(buf_ref.at[seat(me)], rows_ref.at[seat(me)], own_sem.at[0])
    own_in.start()

    def run(first_row, count):
        inner = hidden_ref.shape[1]
        width = answer_ref.shape[1]
        take = pl.ds(pl.multiple_of(first_row, count), count)
        value = rows_ref[take, :]

        @pl.loop(0, inner // 256)
        def _(f):
            cols = pl.ds(pl.multiple_of(f * 256, 256), 256)
            hidden = jnp.dot(value, w_in_ref[:, cols], preferred_element_type=jnp.float32)
            hidden_ref[:, cols] = jnp.maximum(hidden, 0.0).astype(jnp.bfloat16)

        @pl.loop(0, width // 256)
        def _(f):
            cols = pl.ds(pl.multiple_of(f * 256, 256), 256)
            answer_ref[take, cols] = jnp.dot(
                hidden_ref[...], w_back_ref[:, cols], preferred_element_type=jnp.float32
            ).astype(jnp.bfloat16)

    half_rows = near * cap
    side = dp // (planes // 2)

    @pl.loop(1, near)
    def _(shift):
        dispatch(shift).wait_recv()

    own_in.wait()
    for c in loads:
        c.wait()

    @pl.loop(0, 2)
    def _(turn):
        @pl.when(turn == 1)
        def _():
            @pl.loop(near, owners)
            def _(shift):
                dispatch(shift).wait_recv()

        run(lax.rem(side + turn, 2) * half_rows, half_rows)

        @pl.loop(0, near)
        def _(shift):
            @pl.when(turn * near + shift > 0)
            def _():
                give_back(turn * near + shift).start()

    own_out = pltpu.make_async_copy(answer_ref.at[seat(me)], back_ref.at[seat(me)], own_sem.at[1])
    own_out.start()

    @pl.loop(1, owners)
    def _(shift):
        dispatch(shift).wait_send()
        give_back(shift).wait()

    own_out.wait()


def experts_fused(buffer, w_in, w_back, capacity):
    planes, n = lax.axis_size("dp"), lax.axis_size("ctx")
    owners = planes * n
    slots, width = buffer.shape
    inner = w_in.shape[2]
    bf = jnp.bfloat16
    vmem = pl.BlockSpec(memory_space=pltpu.VMEM)
    hbm = pl.BlockSpec(memory_space=pl.ANY)
    return pl.pallas_call(
        functools.partial(expert_kernel, planes, n, capacity),
        out_shape=jax.ShapeDtypeStruct((slots, width), bf),
        in_specs=[vmem, hbm, hbm],
        out_specs=vmem,
        scratch_shapes=[
            pltpu.VMEM(w_in.shape[1:], bf),
            pltpu.VMEM(w_back.shape[1:], bf),
            pltpu.VMEM((slots, width), bf),
            pltpu.VMEM((slots // 2, inner), bf),
            pltpu.VMEM((slots, width), bf),
            pltpu.SemaphoreType.DMA((2,)),
            pltpu.SemaphoreType.DMA((2,)),
            pltpu.SemaphoreType.DMA((owners,)),
            pltpu.SemaphoreType.DMA((owners,)),
            pltpu.SemaphoreType.DMA((owners,)),
            pltpu.SemaphoreType.DMA((owners,)),
        ],
        compiler_params=pltpu.CompilerParams(collective_id=1, has_side_effects=True),
        name="experts",
    )(buffer, w_in, w_back)


def experts(buffer, w_in, w_back, capacity):
    if capacity % 16 == 0 and w_in.shape[0] == 1:
        return experts_fused(buffer, w_in, w_back, capacity)
    return experts_plain(buffer, w_in, w_back, capacity)


def whole_kernel(
    planes,
    n,
    cap,
    kept_hbm,
    ids_hbm,
    gain_attn_hbm,
    gain_ffn_hbm,
    doc_hbm,
    wq_hbm,
    wk_hbm,
    wv_hbm,
    wo_hbm,
    w_in_hbm,
    w_back_hbm,
    out_ref,
    kept_ref,
    ids_ref,
    gain_attn_ref,
    gain_ffn_ref,
    doc_ref,
    w3_ref,
    wo_ref,
    w_in_ref,
    w_back_ref,
    place_all,
    x_all,
    q_all,
    k_all,
    v_all,
    mix_ref,
    m_out,
    m_in,
    wo_all,
    r_out,
    r_in,
    first_ref,
    ffn_ref,
    hidden_ref,
    second_ref,
    back_ref,
    picks_ref,
    acc_ref,
    w_sem,
    p_send,
    p_recv,
    x_send,
    x_recv,
    o_send,
    o_recv,
    r_send,
    r_recv,
    m_send,
    m_recv,
    b_send,
    b_recv,
    ready,
):
    f32, bf = jnp.float32, jnp.bfloat16
    dp, me = lax.axis_index("dp"), lax.axis_index("ctx")
    owners = planes * n
    rows, width = x_all.shape[1], x_all.shape[2]
    shard = doc_ref.shape[0]
    inner = hidden_ref.shape[1]
    wide = 2 * HS
    share = n * cap
    pairs = n // 2

    loads = [
        pltpu.make_async_copy(ids_hbm, ids_ref, w_sem.at[8]),
        pltpu.make_async_copy(kept_hbm, kept_ref, w_sem.at[9]),
        pltpu.make_async_copy(doc_hbm, doc_ref, w_sem.at[0]),
        pltpu.make_async_copy(gain_attn_hbm, gain_attn_ref, w_sem.at[10]),
        pltpu.make_async_copy(gain_ffn_hbm, gain_ffn_ref, w_sem.at[11]),
        pltpu.make_async_copy(wq_hbm, w3_ref.at[pl.ds(0, HS)], w_sem.at[1]),
        pltpu.make_async_copy(wk_hbm, w3_ref.at[pl.ds(2 * HS, HS)], w_sem.at[2]),
        pltpu.make_async_copy(wv_hbm, w3_ref.at[pl.ds(4 * HS, HS)], w_sem.at[3]),
        pltpu.make_async_copy(wv_hbm, w3_ref.at[pl.ds(7 * HS, HS)], w_sem.at[4]),
        pltpu.make_async_copy(wo_hbm, wo_ref, w_sem.at[5]),
        pltpu.make_async_copy(w_in_hbm.at[0], w_in_ref, w_sem.at[6]),
        pltpu.make_async_copy(w_back_hbm.at[0], w_back_ref, w_sem.at[7]),
    ]
    for c in loads:
        c.start()

    barrier = pltpu.get_barrier_semaphore()

    for d in range(1, n):
        pl.semaphore_signal(
            barrier, inc=1, device_id={"ctx": lax.rem(me + d, n)}, device_id_type=MESH
        )

    def column(sem):
        for d in range(1, planes):
            pl.semaphore_signal(
                sem, inc=1, device_id={"dp": lax.rem(dp + d, planes)}, device_id_type=MESH
            )

    column(barrier)

    def plane(g):
        high = lax.rem(dp // 2 + g // 2, 2)
        return high * 2 + lax.rem(dp + lax.rem(g, 2), 2)

    def one_hot(mask):
        return jnp.where(mask, 1.0, 0.0).astype(bf)

    def iota(shape, dim):
        return lax.broadcasted_iota(jnp.int32, shape, dim)

    blank = jnp.zeros((HS, width), bf)
    for i in (1, 3, 5, 6):
        w3_ref[pl.ds(i * HS, HS), :] = blank

    loads[0].wait()
    ids = ids_ref[...]
    named = one_hot(iota((owners, rows), 0) == ids)
    earlier = one_hot(iota((rows, rows), 0) < iota((rows, rows), 1))
    before = jnp.dot(named, earlier, preferred_element_type=f32)
    slot = jnp.sum(named.astype(f32) * before, axis=0, keepdims=True).astype(jnp.int32)
    place_own = ids * cap + slot
    place_all[me] = jnp.broadcast_to(place_own, place_all.shape[1:])

    loads[1].wait()
    local = kept_ref[...] - me * shard
    picks = one_hot(iota((shard, rows), 0) == local)
    for z in range(planes):
        cells = one_hot(iota((share, rows), 0) + z * share == place_own)
        picks_ref[z] = lax.dot_general(picks, cells, LAST, preferred_element_type=f32).astype(bf)
    loads[2].wait()
    x_all[me] = lax.dot_general(
        picks, doc_ref[...], (((0,), (0,)), ((), ())), preferred_element_type=f32
    ).astype(bf)

    for c in loads[3:10]:
        c.wait()
    pl.semaphore_wait(barrier, n + planes - 2)
    column(ready)

    def place_copy(d):
        return pltpu.make_async_remote_copy(
            src_ref=place_all.at[me],
            dst_ref=place_all.at[me],
            send_sem=p_send.at[d],
            recv_sem=p_recv.at[d],
            device_id={"ctx": lax.rem(me + d, n)},
            device_id_type=MESH,
        )

    for d in range(1, n):
        place_copy(d).start()

    o = Gather(n, me, wo_ref, wo_all, o_send, o_recv)
    core, chip, partner = o.core, o.chip, o.partner
    (near_x, _), (near_y, _) = o.peers()
    near_a = jnp.where(core == 0, near_x, near_y)
    near_b = jnp.where(core == 0, near_y, near_x)
    part = rows // 2

    def whole_block(ident, block, target):
        ref = x_all.at[block]
        return pltpu.make_async_remote_copy(
            src_ref=ref,
            dst_ref=ref,
            send_sem=x_send.at[ident],
            recv_sem=x_recv.at[ident],
            device_id={"ctx": target},
            device_id_type=MESH,
        )

    def half_block(ident, block, which, target):
        ref = x_all.at[block, pl.ds(pl.multiple_of(which * part, part), part)]
        return pltpu.make_async_remote_copy(
            src_ref=ref,
            dst_ref=ref,
            send_sem=x_send.at[ident],
            recv_sem=x_recv.at[ident],
            device_id={"ctx": target},
            device_id_type=MESH,
        )

    from_a, from_b, across = near_a * 2 + core, near_b * 2 + core, (3 - chip) * 2 + core
    own_a = whole_block(0, me, from_a)
    own_b = whole_block(1, me, from_b)
    twin = whole_block(2, me, partner)
    pass_a = whole_block(3, from_a, partner)
    pass_b = whole_block(4, from_b, partner)
    relay_a = half_block(5, from_a, core, from_b)
    relay_b = half_block(6, from_b, 1 - core, from_a)
    pass_c = half_block(7, across, core, partner)
    pass_d = half_block(8, across, 1 - core, partner)
    own_a.start()
    twin.start()

    def row_copy(turn, block):
        return pltpu.make_async_remote_copy(
            src_ref=r_out.at[turn - 1, block],
            dst_ref=r_in.at[dp, block],
            send_sem=r_send.at[turn * n + block],
            recv_sem=r_recv.at[turn * n + block],
            device_id={"dp": plane(turn)},
            device_id_type=MESH,
        )

    def route(block, value):
        index = iota((planes * cap, rows), 0)
        turn, s = index // cap, index % cap
        high = (dp // 2 + turn // 2) % 2
        to = high * 2 + (dp + turn % 2) % 2
        cell = (to * n + me) * cap + s
        taken = jnp.dot(
            one_hot(cell == place_all[block][0:1, :]), value, preferred_element_type=f32
        ).astype(bf)
        r_in[dp, block] = taken[0:cap]
        for turn in (2, 3, 1):
            r_out[turn - 1, block] = taken[turn * cap : (turn + 1) * cap]
            row_copy(turn, block).start()

    def project(block, value):
        at = pl.ds(pl.multiple_of(block * rows, rows), rows)
        normed = rms_scale(value, gain_attn_ref[...]).astype(bf)
        three = lax.dot_general(normed, w3_ref[...], LAST, preferred_element_type=f32)
        q_all[at, :] = three[:, 0:wide].astype(bf)
        k_all[at, :] = three[:, wide : 2 * wide].astype(bf)
        lane = iota((rows, wide), 1)
        v_all[0, at, :] = jnp.where(lane < HS, three[:, 2 * wide : 3 * wide], 1.0).astype(bf)
        v_all[1, at, :] = jnp.where(lane < HS, 1.0, three[:, 3 * wide : 4 * wide]).astype(bf)

    def take(block):
        value = x_all[block]
        route(block, value)
        project(block, value)

    take(me)
    wo_all[me] = wo_ref[...]
    for d in range(1, n):
        place_copy(d).wait_recv()
    twin.wait_recv()
    take(partner)
    own_a.wait_send()
    own_b.start()
    own_a.wait_recv()
    pass_a.start()
    relay_a.start()
    take(from_a)
    pass_a.wait_recv()
    take(near_b * 2 + 1 - core)
    own_b.wait_recv()
    pass_b.start()
    relay_b.start()
    take(from_b)
    pass_b.wait_recv()
    take(near_a * 2 + 1 - core)
    relay_a.wait_recv()
    pass_c.start()
    relay_b.wait_recv()
    pass_d.start()
    o.begin()
    take(across)
    pass_c.wait_recv()
    pass_d.wait_recv()
    take((3 - chip) * 2 + 1 - core)

    scale = score_gain / math.sqrt(HS) * math.log2(math.e)

    def mixed_copy(turn, d, j):
        to, c = plane(turn), lax.rem(me + d, n)
        lanes = pl.ds(pl.multiple_of(me * wide, wide), wide)
        return pltpu.make_async_remote_copy(
            src_ref=m_out.at[to * n + c, j],
            dst_ref=m_in.at[dp, j, :, lanes],
            send_sem=m_send.at[(turn * n + d) * pairs + j],
            recv_sem=m_recv.at[(turn * n + d) * pairs + j],
            device_id={"dp": to, "ctx": c},
            device_id_type=MESH,
        )

    def each(turn, act):
        @pl.loop(0, n)
        def _(d):
            @pl.when(turn + d > 0)
            def _():
                act(turn, d)

    def mixed_copies(turn, act):
        def some(turn, d):
            for j in range(pairs):
                act(mixed_copy(turn, d, j))

        each(turn, some)

    def attend(first, last):
        @pl.loop(first, last)
        def _(j):
            for side in (0, 1):
                block = 2 * j + side
                at = pl.ds(pl.multiple_of(block * rows, rows), rows)
                scores = lax.dot_general(
                    q_all[at, :], k_all[...], LAST, preferred_element_type=f32
                )
                top = jnp.max(scores, axis=1, keepdims=True)
                weights = jnp.exp2(scores * scale - top * scale)
                both = jnp.dot(weights.astype(bf), v_all[side], preferred_element_type=f32)
                total = pltpu.roll(both, HS, 1)
                mine = (iota((rows, wide), 1) // HS) == side
                mix_ref[pl.ds(side * rows, rows), :] = jnp.where(mine, both / total, 0.0).astype(bf)
            places = jnp.concatenate([place_all[2 * j][0:1, :], place_all[2 * j + 1][0:1, :]], axis=1)
            spots = one_hot(iota((owners * cap, 2 * rows), 0) == places)
            spread = jnp.dot(spots, mix_ref[...], preferred_element_type=f32).astype(bf)
            m_out[:, j] = spread.reshape(owners, cap, wide)
            each(2, lambda turn, d: mixed_copy(turn, d, j).start())
            each(0, lambda turn, d: mixed_copy(turn, d, j).start())

    pl.semaphore_wait(ready, planes - 1)
    attend(0, pairs - 1)
    o.twin.wait_recv()
    o.relay()
    attend(pairs - 1, pairs)
    o.diagonal()

    def seat(t):
        return lax.rem(t, 2) * 2 + t // 2

    def back_copy(turn, d):
        to, c = plane(turn), lax.rem(me + d, n)
        return pltpu.make_async_remote_copy(
            src_ref=second_ref.at[to, lax.rem(c, 2), c // 2],
            dst_ref=back_ref.at[dp, me],
            send_sem=b_send.at[turn * n + d],
            recv_sem=b_recv.at[turn * n + d],
            device_id={"dp": to, "ctx": c},
            device_id_type=MESH,
        )

    mixed_copies(1, lambda c: c.start())
    mixed_copies(3, lambda c: c.start())
    m_in[dp, :, :, pl.ds(pl.multiple_of(me * wide, wide), wide)] = m_out[dp * n + me]
    for _, c in o.passed:
        c.wait_recv()
    o.final()
    touched = jnp.zeros((shard, 1), f32)
    for z in range(planes):
        touched = touched + jnp.sum(picks_ref[z].astype(f32), axis=1, keepdims=True)
    acc_ref[...] = jnp.where(touched > 0.5, 0.0, doc_ref[...].astype(f32))
    for c in loads[10:]:
        c.wait()

    half = pairs * cap

    @pl.loop(0, planes)
    def _(t):
        turn = seat(t)
        source = plane(turn)
        mixed_copies(turn, lambda c: c.wait_recv())

        @pl.when(turn > 0)
        def _():
            @pl.loop(0, n)
            def _(block):
                row_copy(turn, block).wait_recv()

        mixed = m_in[source].reshape(half, n * wide)
        heads = [mixed[:, h * wide : (h + 1) * wide] for h in range(n)]
        low = jnp.concatenate([h[:, :HS] for h in heads], axis=1)
        high = jnp.concatenate([h[:, HS:] for h in heads], axis=1)
        base = [r_in[source, 2 * j + side] for side in (0, 1) for j in range(pairs)]
        first_ref[...] = jnp.concatenate(base, axis=0).astype(f32) + jnp.dot(
            jnp.concatenate([low, high], axis=0),
            wo_all[...].reshape(n * HS, width),
            preferred_element_type=f32,
        )
        ffn_ref[...] = rms_scale(first_ref[...], gain_ffn_ref[...]).astype(bf)
        for f in range(0, inner, 256):
            hidden = jnp.dot(ffn_ref[...], w_in_ref[:, f : f + 256], preferred_element_type=f32)
            hidden_ref[:, f : f + 256] = jnp.maximum(hidden, 0.0).astype(bf)
        for f in range(0, width, 256):
            answer = jnp.dot(
                hidden_ref[...], w_back_ref[:, f : f + 256], preferred_element_type=f32
            ).astype(bf)
            second = (first_ref[:, f : f + 256] + answer.astype(f32)).astype(bf)
            second_ref[source, :, :, :, f : f + 256] = second.reshape(2, pairs, cap, 256)
        each(turn, lambda turn, d: back_copy(turn, d).start())

    back_ref[dp, me] = second_ref[dp, lax.rem(me, 2), me // 2]

    @pl.loop(0, planes)
    def _(t):
        turn = seat(t)
        source = plane(turn)
        each(turn, lambda turn, d: back_copy(turn, d).wait_recv())
        acc_ref[...] += jnp.dot(
            picks_ref[source], back_ref[source].reshape(share, width), preferred_element_type=f32
        )

    out_ref[...] = acc_ref[...].astype(bf)

    for d in range(1, n):
        place_copy(d).wait_send()

    @pl.loop(0, planes)
    def _(turn):
        mixed_copies(turn, lambda c: c.wait_send())
        each(turn, lambda turn, d: back_copy(turn, d).wait_send())

        @pl.when(turn > 0)
        def _():
            @pl.loop(0, n)
            def _(block):
                row_copy(turn, block).wait_send()

    for c in (own_b, twin, pass_a, pass_b, relay_a, relay_b, pass_c, pass_d):
        c.wait_send()
    o.drain()


def whole(document, kept, ids, gain_attn, gain_ffn, w_query, w_key, w_value, w_out, w_in, w_back):
    planes, n = lax.axis_size("dp"), lax.axis_size("ctx")
    owners = planes * n
    shard, width = document.shape
    rows = kept.shape[1]
    cap = 2 * rows // owners
    inner = w_in.shape[2]
    pairs = n // 2
    wide = 2 * HS
    half = pairs * cap
    bf, f32 = jnp.bfloat16, jnp.float32
    vmem = pl.BlockSpec(memory_space=pltpu.VMEM)
    hbm = pl.BlockSpec(memory_space=pltpu.HBM)
    sems = pltpu.SemaphoreType.DMA
    copies = gather_copies(n)
    grant = 42 * 1024 * 1024
    operands = (
        kept,
        ids,
        gain_attn.reshape(1, width),
        gain_ffn.reshape(1, width),
        document,
        w_query.T,
        w_key.T,
        w_value.T,
        w_out,
        w_in,
        w_back,
    )
    return pl.pallas_call(
        functools.partial(whole_kernel, planes, n, cap),
        out_shape=jax.ShapeDtypeStruct((shard, width), bf),
        in_specs=[hbm] * 11,
        out_specs=vmem,
        scratch_shapes=[
            pltpu.VMEM((1, rows), jnp.int32),
            pltpu.VMEM((1, rows), jnp.int32),
            pltpu.VMEM((1, width), f32),
            pltpu.VMEM((1, width), f32),
            pltpu.VMEM((shard, width), bf),
            pltpu.VMEM((8 * HS, width), bf),
            pltpu.VMEM(w_out.shape, bf),
            pltpu.VMEM(w_in.shape[1:], bf),
            pltpu.VMEM(w_back.shape[1:], bf),
            pltpu.VMEM((n, 8, rows), jnp.int32),
            pltpu.VMEM((n, rows, width), bf),
            pltpu.VMEM((n * rows, wide), bf),
            pltpu.VMEM((n * rows, wide), bf),
            pltpu.VMEM((2, n * rows, wide), bf),
            pltpu.VMEM((2 * rows, wide), bf),
            pltpu.VMEM((owners, pairs, cap, wide), bf),
            pltpu.VMEM((planes, pairs, cap, n * wide), bf),
            pltpu.VMEM((n,) + w_out.shape, bf),
            pltpu.VMEM((planes - 1, n, cap, width), bf),
            pltpu.VMEM((planes, n, cap, width), bf),
            pltpu.VMEM((2 * half, width), f32),
            pltpu.VMEM((2 * half, width), bf),
            pltpu.VMEM((2 * half, inner), bf),
            pltpu.VMEM((planes, 2, pairs, cap, width), bf),
            pltpu.VMEM((planes, n, cap, width), bf),
            pltpu.VMEM((planes, shard, n * cap), bf),
            pltpu.VMEM((shard, width), f32),
            sems((12,)),
            sems((n,)),
            sems((n,)),
            sems((copies,)),
            sems((copies,)),
            sems((copies,)),
            sems((copies,)),
            sems((owners,)),
            sems((owners,)),
            sems((owners * pairs,)),
            sems((owners * pairs,)),
            sems((owners,)),
            sems((owners,)),
            pltpu.SemaphoreType.REGULAR,
        ],
        compiler_params=pltpu.CompilerParams(
            collective_id=2, has_side_effects=True, vmem_limit_bytes=grant
        ),
        name="whole",
    )(*[pltpu.with_memory_space_constraint(a, pltpu.HBM) for a in operands])


def fits_whole(planes, n, keep_here, w_query, w_out, w_in):
    cap = 2 * keep_here // (planes * n)
    return (
        planes == 4
        and n == 8
        and w_query.shape[1] == HS
        and w_out.shape[0] == HS
        and w_in.shape[0] == 1
        and cap % 16 == 0
        and w_in.shape[2] % 256 == 0
    )


def body(
    tokens, kept, gain_attn, gain_ffn, w_query, w_key, w_value, w_out, expert_ids, w_in, w_back
):
    document = tokens[0]
    shard_len, width_model = document.shape
    ctx_count = lax.axis_size("ctx")
    dp_count = lax.axis_size("dp")
    if fits_whole(dp_count, ctx_count, kept.shape[1], w_query, w_out, w_in):
        ids = expert_ids.reshape(1, kept.shape[1])
        weights = (w_query, w_key, w_value, w_out, w_in, w_back)
        return whole(document, kept, ids, gain_attn, gain_ffn, *weights)[None]
    local = kept[0] - lax.axis_index("ctx") * shard_len
    keep_here = local.shape[0]
    positions = jnp.arange(shard_len, dtype=jnp.int32)
    picks = (local[:, None] == positions[None, :]).astype(jnp.bfloat16)
    rows = jnp.dot(picks, document, preferred_element_type=jnp.float32).astype(jnp.bfloat16)
    normed = rms_scale(rows, gain_attn).astype(jnp.bfloat16)
    mixed, w_out_all = attention(normed, w_query, w_key, w_value, w_out)
    inner_all = w_out.shape[0] * ctx_count
    attn = lax.dot_general(
        mixed.reshape(inner_all, keep_here),
        w_out_all.reshape(inner_all, width_model),
        (((0,), (0,)), ((), ())),
        preferred_element_type=jnp.float32,
    )
    first = rows.astype(jnp.float32) + attn
    ffn_in = rms_scale(first, gain_ffn).astype(jnp.bfloat16)
    expert_here = w_in.shape[0]
    owners = dp_count * ctx_count
    experts_all = expert_here * owners
    capacity = 2 * keep_here // experts_all
    labels = expert_ids[0, :, 0]
    order = jnp.arange(keep_here, dtype=jnp.int32)
    same = (labels[:, None] == labels[None, :]) & (order[None, :] < order[:, None])
    slots = jnp.sum(same.astype(jnp.int32), axis=1)
    place = labels * capacity + slots
    cells = jnp.arange(experts_all * capacity, dtype=jnp.int32)
    spots = (place[None, :] == cells[:, None]).astype(jnp.bfloat16)
    buffer = jnp.dot(spots, ffn_in, preferred_element_type=jnp.float32).astype(jnp.bfloat16)
    answers = experts(buffer, w_in, w_back, capacity)
    seats = (place[:, None] == cells[None, :]).astype(jnp.bfloat16)
    taken = jnp.dot(seats, answers, preferred_element_type=jnp.float32)
    second = (first + taken).astype(jnp.bfloat16)
    hits = positions[:, None] == local[None, :]
    fresh = jnp.dot(hits.astype(jnp.bfloat16), second, preferred_element_type=jnp.float32)
    touched = jnp.any(hits, axis=1, keepdims=True)
    blended = jnp.where(touched, fresh.astype(jnp.bfloat16), document)
    return blended[None]


def solution(mesh):
    return jax.shard_map(
        body,
        mesh=mesh,
        in_specs=(
            P("dp", "ctx", None),
            P("dp", "ctx"),
            P(),
            P(),
            P(None, "ctx"),
            P(None, "ctx"),
            P(None, "ctx"),
            P("ctx", None),
            P("dp", "ctx", None),
            P(("dp", "ctx"), None, None),
            P(("dp", "ctx"), None, None),
        ),
        out_specs=P("dp", "ctx", None),
        check_vma=False,
    )
```

```python
import functools
import math

import jax
import jax.numpy as jnp
from jax import lax
from jax.experimental import pallas as pl
from jax.experimental.pallas import tpu as pltpu
from jax.sharding import PartitionSpec as P

HS = 64
MESH = pl.DeviceIdType.MESH
LAST = (((1,), (1,)), ((), ()))

eps_norm = 1e-06
score_gain = 2.5


def rms_scale(values, gain):
    values = values.astype(jnp.float32)
    power = jnp.mean(values * values, axis=-1, keepdims=True)
    return values * lax.rsqrt(power + eps_norm) * gain


class Gather:
    def __init__(self, n, me, own, slots, send, recv):
        self.n, self.me, self.own, self.slots = n, me, own, slots
        self.send, self.recv = send, recv
        self.core, self.chip = me % 2, me // 2
        self.partner = me + 1 - 2 * self.core
        self.started = []

    def copy(self, ident, src, dst, target):
        return pltpu.make_async_remote_copy(
            src_ref=src,
            dst_ref=dst,
            send_sem=self.send.at[ident],
            recv_sem=self.recv.at[ident],
            device_id={"ctx": target},
            device_id_type=MESH,
        )

    def peers(self):
        chips = self.n // 2
        if chips == 4:
            x, y = self.chip % 2, self.chip // 2
            nx, ny = y * 2 + (1 - x), (1 - y) * 2 + x
            return [(nx, nx), (ny, ny)]
        return [
            ((self.chip + d) % chips, (self.chip + chips - d) % chips) for d in range(1, chips)
        ]

    def begin(self):
        own_to = self.slots.at[self.me]
        self.first = [
            self.copy(i, self.own, own_to, to * 2 + self.core)
            for i, (to, _) in enumerate(self.peers())
        ]
        self.base = len(self.first)
        self.twin = self.copy(self.base, self.own, own_to, self.partner)
        for c in self.first:
            c.start()
        self.twin.start()
        self.started = self.first + [self.twin]

    def relay(self):
        here, self.passed, self.late = [], [], []
        ident = self.base + 1
        peers = self.peers()
        square = self.n // 2 == 4
        half = self.own.shape[0] // 2
        for i, (_, source) in enumerate(peers):
            self.first[i].wait_recv()
            block = source * 2 + self.core
            here.append(block)
            if square:
                piece = self.slots.at[block, pl.ds(i * half, half)]
                c = self.copy(ident, piece, piece, peers[1 - i][0] * 2 + self.core)
                c.start()
                self.late.append(c)
                ident += 1
            c = self.copy(ident, self.slots.at[block], self.slots.at[block], self.partner)
            c.start()
            self.passed.append((source * 2 + 1 - self.core, c))
            ident += 1
        self.ident = ident
        self.started += self.late + [c for _, c in self.passed]
        return here

    def diagonal(self):
        if not self.late:
            return None
        block = (3 - self.chip) * 2 + self.core
        half = self.own.shape[0] // 2
        self.last = []
        for i, c in enumerate(self.late):
            c.wait_recv()
            piece = self.slots.at[block, pl.ds(i * half, half)]
            c = self.copy(self.ident + i, piece, piece, self.partner)
            c.start()
            self.last.append(c)
        self.started += self.last
        return block

    def final(self):
        if not self.late:
            return None
        for c in self.last:
            c.wait_recv()
        return (3 - self.chip) * 2 + 1 - self.core

    def drain(self):
        for c in self.started:
            c.wait_send()


def gather_copies(n):
    return 9 if n // 2 == 4 else 2 * (n // 2) - 1


def attention_kernel(
    n,
    heads,
    x_ref,
    wq_ref,
    wk_ref,
    wv_ref,
    wo_ref,
    mixed_ref,
    wo_all,
    x_all,
    q_all,
    k_all,
    v_all,
    stage,
    x_send,
    x_recv,
    o_send,
    o_recv,
    m_send,
    m_recv,
):
    me = lax.axis_index("ctx")
    rows = x_ref.shape[0]
    barrier = pltpu.get_barrier_semaphore()
    for d in range(1, n):
        pl.semaphore_signal(
            barrier, inc=1, device_id={"ctx": (me + d) % n}, device_id_type=MESH
        )
    pl.semaphore_wait(barrier, n - 1)

    def project(block, value):
        at = pl.ds(pl.multiple_of(block * rows, rows), rows)
        for h in range(heads):
            cols = pl.ds(h * HS, HS)
            q_all[h, at, :] = lax.dot_general(
                value, wq_ref[cols, :], LAST, preferred_element_type=jnp.float32
            ).astype(jnp.bfloat16)
            k_all[h, at, :] = lax.dot_general(
                value, wk_ref[cols, :], LAST, preferred_element_type=jnp.float32
            ).astype(jnp.bfloat16)
        v_all[:, at] = lax.dot_general(
            wv_ref[...], value, LAST, preferred_element_type=jnp.float32
        ).astype(jnp.bfloat16)

    g = Gather(n, me, x_ref, x_all, x_send, x_recv)
    o = Gather(n, me, wo_ref, wo_all, o_send, o_recv)
    g.begin()
    project(me, x_ref[...])
    wo_all[me] = wo_ref[...]
    g.twin.wait_recv()
    project(g.partner, x_all[g.partner])
    here = g.relay()
    o.begin()
    for block in here:
        project(block, x_all[block])
    for block, c in g.passed:
        c.wait_recv()
        project(block, x_all[block])
    block = g.diagonal()
    if block is not None:
        project(block, x_all[block])
    o.twin.wait_recv()
    o.relay()
    block = g.final()
    if block is not None:
        project(block, x_all[block])

    scale = score_gain / math.sqrt(HS) * math.log2(math.e)

    def send_block(step, target):
        return pltpu.make_async_remote_copy(
            src_ref=stage.at[step],
            dst_ref=mixed_ref.at[me],
            send_sem=m_send.at[step],
            recv_sem=m_recv.at[step],
            device_id={"ctx": target},
            device_id_type=MESH,
        )

    @pl.loop(0, n)
    def _(step):
        block = lax.rem(me + 1 + step, n)
        at = pl.ds(pl.multiple_of(block * rows, rows), rows)
        for h in range(heads):
            scores = lax.dot_general(
                k_all[h],
                q_all[h, at, :],
                LAST,
                preferred_element_type=jnp.float32,
            )
            top = jnp.max(scores, axis=0, keepdims=True)
            weights = jnp.exp2(scores * scale - top * scale)
            total = jnp.sum(weights, axis=0, keepdims=True)
            cols = pl.ds(h * HS, HS)
            mixed = jnp.dot(
                v_all[cols, :],
                weights.astype(jnp.bfloat16),
                preferred_element_type=jnp.float32,
            )
            stage[step, cols, :] = (mixed / total).astype(jnp.bfloat16)

        @pl.when(step < n - 1)
        def _():
            send_block(step, block).start()

    mixed_ref[me] = stage[n - 1]
    for _, c in o.passed:
        c.wait_recv()
    o.diagonal()
    o.final()

    @pl.loop(0, n - 1)
    def _(step):
        send_block(step, lax.rem(me + 1 + step, n)).wait()

    g.drain()
    o.drain()


def attention(normed, w_query, w_key, w_value, w_out):
    n = lax.axis_size("ctx")
    rows, width = normed.shape
    inner = w_query.shape[1]
    heads = inner // HS
    copies = gather_copies(n)
    vmem = pl.BlockSpec(memory_space=pltpu.VMEM)
    bf = jnp.bfloat16
    return pl.pallas_call(
        functools.partial(attention_kernel, n, heads),
        out_shape=(
            jax.ShapeDtypeStruct((n, inner, rows), bf),
            jax.ShapeDtypeStruct((n,) + w_out.shape, bf),
        ),
        in_specs=[vmem] * 5,
        out_specs=(vmem, vmem),
        scratch_shapes=[
            pltpu.VMEM((n, rows, width), bf),
            pltpu.VMEM((heads, n * rows, HS), bf),
            pltpu.VMEM((heads, n * rows, HS), bf),
            pltpu.VMEM((inner, n * rows), bf),
            pltpu.VMEM((n, inner, rows), bf),
            pltpu.SemaphoreType.DMA((copies,)),
            pltpu.SemaphoreType.DMA((copies,)),
            pltpu.SemaphoreType.DMA((copies,)),
            pltpu.SemaphoreType.DMA((copies,)),
            pltpu.SemaphoreType.DMA((n,)),
            pltpu.SemaphoreType.DMA((n,)),
        ],
        compiler_params=pltpu.CompilerParams(collective_id=0, has_side_effects=True),
        name="attention",
    )(normed, w_query.T, w_key.T, w_value.T, w_out)


def experts_plain(buffer, w_in, w_back, capacity):
    owners = lax.axis_size("dp") * lax.axis_size("ctx")
    expert_here, width = w_in.shape[0], buffer.shape[1]
    buffer = buffer.reshape(owners * expert_here, capacity, width)
    received = lax.all_to_all(buffer, ("dp", "ctx"), split_axis=0, concat_axis=0, tiled=True)
    grouped = received.reshape(owners, expert_here, capacity, width)
    hidden = jnp.einsum("sgid,gdf->sgif", grouped, w_in, preferred_element_type=jnp.float32)
    hidden = jnp.maximum(hidden, 0.0).astype(jnp.bfloat16)
    answer = jnp.einsum("sgif,gfd->sgid", hidden, w_back, preferred_element_type=jnp.float32)
    answered = answer.astype(jnp.bfloat16).reshape(owners * expert_here, capacity, width)
    back = lax.all_to_all(answered, ("dp", "ctx"), split_axis=0, concat_axis=0, tiled=True)
    return back.reshape(owners * expert_here * capacity, width)


def expert_kernel(
    planes,
    n,
    cap,
    buf_ref,
    w_in_hbm,
    w_back_hbm,
    back_ref,
    w_in_ref,
    w_back_ref,
    rows_ref,
    hidden_ref,
    answer_ref,
    w_sem,
    own_sem,
    d_send,
    d_recv,
    r_send,
    r_recv,
):
    dp, ctx = lax.axis_index("dp"), lax.axis_index("ctx")
    me = dp * n + ctx
    owners = planes * n
    loads = [
        pltpu.make_async_copy(w_in_hbm.at[0], w_in_ref, w_sem.at[0]),
        pltpu.make_async_copy(w_back_hbm.at[0], w_back_ref, w_sem.at[1]),
    ]
    for c in loads:
        c.start()
    barrier = pltpu.get_barrier_semaphore()

    @pl.loop(1, owners)
    def _(d):
        to = lax.rem(me + d, owners)
        pl.semaphore_signal(
            barrier, inc=1, device_id={"dp": to // n, "ctx": lax.rem(to, n)}, device_id_type=MESH
        )

    pl.semaphore_wait(barrier, owners - 1)

    def seat(index):
        return pl.ds(pl.multiple_of(index * cap, cap), cap)

    def at(shift):
        plane_shift, place_shift = shift // n, lax.rem(shift, n)
        half = planes // 2
        side = dp // half
        side = lax.rem(side + plane_shift // half, 2)
        plane = side * half + lax.rem(dp + plane_shift, half)
        return plane, lax.rem(ctx + place_shift, n)

    def dispatch(shift):
        plane, place = at(shift)
        return pltpu.make_async_remote_copy(
            src_ref=buf_ref.at[seat(plane * n + place)],
            dst_ref=rows_ref.at[seat(me)],
            send_sem=d_send.at[shift],
            recv_sem=d_recv.at[shift],
            device_id={"dp": plane, "ctx": place},
            device_id_type=MESH,
        )

    def give_back(shift):
        plane, place = at(shift)
        return pltpu.make_async_remote_copy(
            src_ref=answer_ref.at[seat(plane * n + place)],
            dst_ref=back_ref.at[seat(me)],
            send_sem=r_send.at[shift],
            recv_sem=r_recv.at[shift],
            device_id={"dp": plane, "ctx": place},
            device_id_type=MESH,
        )

    near = owners // 2

    @pl.loop(0, near)
    def _(shift):
        dispatch(near + shift).start()

        @pl.when(shift > 0)
        def _():
            dispatch(shift).start()

    own_in = pltpu.make_async_copy(buf_ref.at[seat(me)], rows_ref.at[seat(me)], own_sem.at[0])
    own_in.start()

    def run(first_row, count):
        inner = hidden_ref.shape[1]
        width = answer_ref.shape[1]
        take = pl.ds(pl.multiple_of(first_row, count), count)
        value = rows_ref[take, :]

        @pl.loop(0, inner // 256)
        def _(f):
            cols = pl.ds(pl.multiple_of(f * 256, 256), 256)
            hidden = jnp.dot(value, w_in_ref[:, cols], preferred_element_type=jnp.float32)
            hidden_ref[:, cols] = jnp.maximum(hidden, 0.0).astype(jnp.bfloat16)

        @pl.loop(0, width // 256)
        def _(f):
            cols = pl.ds(pl.multiple_of(f * 256, 256), 256)
            answer_ref[take, cols] = jnp.dot(
                hidden_ref[...], w_back_ref[:, cols], preferred_element_type=jnp.float32
            ).astype(jnp.bfloat16)

    half_rows = near * cap
    side = dp // (planes // 2)

    @pl.loop(1, near)
    def _(shift):
        dispatch(shift).wait_recv()

    own_in.wait()
    for c in loads:
        c.wait()

    @pl.loop(0, 2)
    def _(turn):
        @pl.when(turn == 1)
        def _():
            @pl.loop(near, owners)
            def _(shift):
                dispatch(shift).wait_recv()

        run(lax.rem(side + turn, 2) * half_rows, half_rows)

        @pl.loop(0, near)
        def _(shift):
            @pl.when(turn * near + shift > 0)
            def _():
                give_back(turn * near + shift).start()

    own_out = pltpu.make_async_copy(answer_ref.at[seat(me)], back_ref.at[seat(me)], own_sem.at[1])
    own_out.start()

    @pl.loop(1, owners)
    def _(shift):
        dispatch(shift).wait_send()
        give_back(shift).wait()

    own_out.wait()


def experts_fused(buffer, w_in, w_back, capacity):
    planes, n = lax.axis_size("dp"), lax.axis_size("ctx")
    owners = planes * n
    slots, width = buffer.shape
    inner = w_in.shape[2]
    bf = jnp.bfloat16
    vmem = pl.BlockSpec(memory_space=pltpu.VMEM)
    hbm = pl.BlockSpec(memory_space=pl.ANY)
    return pl.pallas_call(
        functools.partial(expert_kernel, planes, n, capacity),
        out_shape=jax.ShapeDtypeStruct((slots, width), bf),
        in_specs=[vmem, hbm, hbm],
        out_specs=vmem,
        scratch_shapes=[
            pltpu.VMEM(w_in.shape[1:], bf),
            pltpu.VMEM(w_back.shape[1:], bf),
            pltpu.VMEM((slots, width), bf),
            pltpu.VMEM((slots // 2, inner), bf),
            pltpu.VMEM((slots, width), bf),
            pltpu.SemaphoreType.DMA((2,)),
            pltpu.SemaphoreType.DMA((2,)),
            pltpu.SemaphoreType.DMA((owners,)),
            pltpu.SemaphoreType.DMA((owners,)),
            pltpu.SemaphoreType.DMA((owners,)),
            pltpu.SemaphoreType.DMA((owners,)),
        ],
        compiler_params=pltpu.CompilerParams(collective_id=1, has_side_effects=True),
        name="experts",
    )(buffer, w_in, w_back)


def experts(buffer, w_in, w_back, capacity):
    if capacity % 16 == 0 and w_in.shape[0] == 1:
        return experts_fused(buffer, w_in, w_back, capacity)
    return experts_plain(buffer, w_in, w_back, capacity)


def whole_kernel(
    planes,
    n,
    cap,
    kept_hbm,
    ids_hbm,
    gain_attn_hbm,
    gain_ffn_hbm,
    doc_hbm,
    wq_hbm,
    wk_hbm,
    wv_hbm,
    wo_hbm,
    w_in_hbm,
    w_back_hbm,
    out_ref,
    kept_ref,
    ids_ref,
    gain_attn_ref,
    gain_ffn_ref,
    doc_ref,
    w3_ref,
    wo_ref,
    w_in_ref,
    w_back_ref,
    place_all,
    x_all,
    q_all,
    k_all,
    v_all,
    mix_ref,
    m_out,
    m_in,
    wo_all,
    r_out,
    r_in,
    first_ref,
    ffn_ref,
    hidden_ref,
    second_ref,
    back_ref,
    picks_ref,
    acc_ref,
    w_sem,
    p_send,
    p_recv,
    x_send,
    x_recv,
    o_send,
    o_recv,
    r_send,
    r_recv,
    m_send,
    m_recv,
    b_send,
    b_recv,
    ready,
):
    f32, bf = jnp.float32, jnp.bfloat16
    dp, me = lax.axis_index("dp"), lax.axis_index("ctx")
    owners = planes * n
    rows, width = x_all.shape[1], x_all.shape[2]
    shard = doc_ref.shape[0]
    inner = hidden_ref.shape[1]
    wide = 2 * HS
    share = n * cap
    pairs = n // 2

    loads = [
        pltpu.make_async_copy(ids_hbm, ids_ref, w_sem.at[8]),
        pltpu.make_async_copy(kept_hbm, kept_ref, w_sem.at[9]),
        pltpu.make_async_copy(doc_hbm, doc_ref, w_sem.at[0]),
        pltpu.make_async_copy(gain_attn_hbm, gain_attn_ref, w_sem.at[10]),
        pltpu.make_async_copy(gain_ffn_hbm, gain_ffn_ref, w_sem.at[11]),
        pltpu.make_async_copy(wq_hbm, w3_ref.at[pl.ds(0, HS)], w_sem.at[1]),
        pltpu.make_async_copy(wk_hbm, w3_ref.at[pl.ds(2 * HS, HS)], w_sem.at[2]),
        pltpu.make_async_copy(wv_hbm, w3_ref.at[pl.ds(4 * HS, HS)], w_sem.at[3]),
        pltpu.make_async_copy(wv_hbm, w3_ref.at[pl.ds(7 * HS, HS)], w_sem.at[4]),
        pltpu.make_async_copy(wo_hbm, wo_ref, w_sem.at[5]),
        pltpu.make_async_copy(w_in_hbm.at[0], w_in_ref, w_sem.at[6]),
        pltpu.make_async_copy(w_back_hbm.at[0], w_back_ref, w_sem.at[7]),
    ]
    for c in loads:
        c.start()

    barrier = pltpu.get_barrier_semaphore()

    for d in range(1, n):
        pl.semaphore_signal(
            barrier, inc=1, device_id={"ctx": lax.rem(me + d, n)}, device_id_type=MESH
        )

    def column(sem):
        for d in range(1, planes):
            pl.semaphore_signal(
                sem, inc=1, device_id={"dp": lax.rem(dp + d, planes)}, device_id_type=MESH
            )

    column(barrier)

    def plane(g):
        high = lax.rem(dp // 2 + g // 2, 2)
        return high * 2 + lax.rem(dp + lax.rem(g, 2), 2)

    def one_hot(mask):
        return jnp.where(mask, 1.0, 0.0).astype(bf)

    def iota(shape, dim):
        return lax.broadcasted_iota(jnp.int32, shape, dim)

    loads[0].wait()
    ids = ids_ref[...]
    named = one_hot(iota((owners, rows), 0) == ids)
    earlier = one_hot(iota((rows, rows), 0) < iota((rows, rows), 1))
    before = jnp.dot(named, earlier, preferred_element_type=f32)
    slot = jnp.sum(named.astype(f32) * before, axis=0, keepdims=True).astype(jnp.int32)
    place_own = ids * cap + slot
    place_all[me] = jnp.broadcast_to(place_own, place_all.shape[1:])
    loads[1].wait()
    local = kept_ref[...] - me * shard
    picks = one_hot(iota((shard, rows), 0) == local)
    loads[2].wait()
    x_all[me] = lax.dot_general(
        picks, doc_ref[...], (((0,), (0,)), ((), ())), preferred_element_type=f32
    ).astype(bf)

    pl.semaphore_wait(barrier, n + planes - 2)
    column(ready)

    o = Gather(n, me, wo_ref, wo_all, o_send, o_recv)

    def bulk(ref, sends, recvs):
        return pltpu.make_async_remote_copy(
            src_ref=ref,
            dst_ref=ref,
            send_sem=sends,
            recv_sem=recvs,
            device_id={"ctx": o.partner},
            device_id_type=MESH,
        )

    def place_copy(d):
        return pltpu.make_async_remote_copy(
            src_ref=place_all.at[me],
            dst_ref=place_all.at[me],
            send_sem=p_send,
            recv_sem=p_recv,
            device_id={"ctx": lax.rem(me + d, n)},
            device_id_type=MESH,
        )

    for d in range(1, n):
        place_copy(d).start()

    core, chip, partner = o.core, o.chip, o.partner
    (near_x, _), (near_y, _) = o.peers()
    part, piece = rows // 2, rows // 4

    def send(ident, block, first, count, target):
        ref = x_all.at[block, pl.ds(pl.multiple_of(first, count), count)]
        return pltpu.make_async_remote_copy(
            src_ref=ref,
            dst_ref=ref,
            send_sem=x_send.at[ident],
            recv_sem=x_recv.at[ident],
            device_id={"ctx": target},
            device_id_type=MESH,
        )

    to_x, to_y = near_x * 2 + core, near_y * 2 + core
    mine = core * part
    twin = send(0, me, 0, rows, partner)
    own, passed, relays, last = [], [], [], []
    for k in (0, 1):
        from_x, from_y, across = near_x * 2 + k, near_y * 2 + k, (3 - chip) * 2 + k
        own.append(
            (
                send(1 + k, chip * 2 + k, mine, part, to_x),
                send(3 + k, chip * 2 + k, mine, part, to_y),
            )
        )
        passed.append(
            (send(5 + k, from_x, mine, part, partner), send(7 + k, from_y, mine, part, partner))
        )
        relays.append(
            (
                send(9 + k, from_x, mine, piece, to_y),
                send(11 + k, from_y, mine + piece, piece, to_x),
            )
        )
        last.append(send(13 + k, across, mine, part, partner))
    twin.start()

    @pl.when(core == 0)
    def _():
        for c in own[0]:
            c.start()

    blank = jnp.zeros((HS, width), bf)
    for i in (1, 3, 5, 6):
        w3_ref[pl.ds(i * HS, HS), :] = blank
    for c in loads[3:10]:
        c.wait()

    def row_copy(turn, block):
        return pltpu.make_async_remote_copy(
            src_ref=r_out.at[turn - 1, block],
            dst_ref=r_in.at[dp, block],
            send_sem=r_send.at[turn],
            recv_sem=r_recv.at[turn],
            device_id={"dp": plane(turn)},
            device_id_type=MESH,
        )

    def route(block, value):
        index = iota((planes * cap, rows), 0)
        turn, s = index // cap, index % cap
        high = (dp // 2 + turn // 2) % 2
        to = high * 2 + (dp + turn % 2) % 2
        cell = (to * n + me) * cap + s
        taken = jnp.dot(
            one_hot(cell == place_all[block][0:1, :]), value, preferred_element_type=f32
        ).astype(bf)
        r_in[dp, block] = taken[0:cap]
        for turn in (2, 3, 1):
            r_out[turn - 1, block] = taken[turn * cap : (turn + 1) * cap]
            row_copy(turn, block).start()

    def project(block, value):
        at = pl.ds(pl.multiple_of(block * rows, rows), rows)
        normed = rms_scale(value, gain_attn_ref[...]).astype(bf)
        three = lax.dot_general(normed, w3_ref[...], LAST, preferred_element_type=f32)
        q_all[at, :] = three[:, 0:wide].astype(bf)
        k_all[at, :] = three[:, wide : 2 * wide].astype(bf)
        lane = iota((rows, wide), 1)
        v_all[0, at, :] = jnp.where(lane < HS, three[:, 2 * wide : 3 * wide], 1.0).astype(bf)
        v_all[1, at, :] = jnp.where(lane < HS, 1.0, three[:, 3 * wide : 4 * wide]).astype(bf)

    def take(block):
        value = x_all[block]
        route(block, value)
        project(block, value)

    take(me)
    twin.wait_recv()

    @pl.when(core == 1)
    def _():
        for c in own[0]:
            c.start()

    for c in own[1]:
        c.start()
    for z in range(planes):
        cells = one_hot(iota((share, rows), 0) + z * share == place_own)
        picks_ref[z] = lax.dot_general(picks, cells, LAST, preferred_element_type=f32).astype(bf)
    wo_all[me] = wo_ref[...]
    places = bulk(place_all.at[pl.ds(0, n - 1)], p_send, p_recv)
    places.wait_recv()
    take(partner)
    for k in (0, 1):
        for c, p, r in zip(own[k], passed[k], relays[k]):
            c.wait_recv()
            p.start()
            r.start()
        if k == 1:
            o.begin()
        for p, near in zip(passed[k], (near_x, near_y)):
            p.wait_recv()
            take(near * 2 + k)
    for k in (0, 1):
        for r in relays[k]:
            r.wait_recv()
        last[k].start()
    for k in (0, 1):
        last[k].wait_recv()
        take((3 - chip) * 2 + k)

    scale = score_gain / math.sqrt(HS) * math.log2(math.e)

    def mixed_copy(turn, d, j):
        to, c = plane(turn), lax.rem(me + d, n)
        lanes = pl.ds(pl.multiple_of(me * wide, wide), wide)
        return pltpu.make_async_remote_copy(
            src_ref=m_out.at[to * n + c, j],
            dst_ref=m_in.at[dp, j, :, lanes],
            send_sem=m_send.at[turn],
            recv_sem=m_recv.at[turn],
            device_id={"dp": to, "ctx": c},
            device_id_type=MESH,
        )

    def mixed_own(j):
        lanes = pl.ds(pl.multiple_of(me * wide, wide), wide)
        return pltpu.make_async_copy(
            m_out.at[dp * n + me, j], m_in.at[dp, j, :, lanes], m_recv.at[0]
        )

    def each(turn, act):
        @pl.loop(0, n)
        def _(d):
            @pl.when(turn + d > 0)
            def _():
                act(turn, d)

    def mixed_copies(turn, act):
        def some(turn, d):
            for j in range(pairs):
                act(mixed_copy(turn, d, j))

        each(turn, some)

    def attend(first, last):
        @pl.loop(first, last)
        def _(j):
            for side in (0, 1):
                block = 2 * j + side
                at = pl.ds(pl.multiple_of(block * rows, rows), rows)
                scores = lax.dot_general(
                    q_all[at, :], k_all[...], LAST, preferred_element_type=f32
                )
                top = jnp.max(scores, axis=1, keepdims=True)
                weights = jnp.exp2(scores * scale - top * scale)
                both = jnp.dot(weights.astype(bf), v_all[side], preferred_element_type=f32)
                total = pltpu.roll(both, HS, 1)
                mine = (iota((rows, wide), 1) // HS) == side
                mix_ref[pl.ds(side * rows, rows), :] = jnp.where(mine, both / total, 0.0).astype(bf)
            places = jnp.concatenate([place_all[2 * j][0:1, :], place_all[2 * j + 1][0:1, :]], axis=1)
            spots = one_hot(iota((owners * cap, 2 * rows), 0) == places)
            spread = jnp.dot(spots, mix_ref[...], preferred_element_type=f32).astype(bf)
            m_out[:, j] = spread.reshape(owners, cap, wide)
            each(2, lambda turn, d: mixed_copy(turn, d, j).start())
            each(0, lambda turn, d: mixed_copy(turn, d, j).start())
            mixed_own(j).start()

    pl.semaphore_wait(ready, planes - 1)
    attend(0, pairs - 1)
    o.twin.wait_recv()
    o.relay()
    attend(pairs - 1, pairs)
    o.diagonal()

    def seat(t):
        return lax.rem(t + planes // 2, planes)

    def back_copy(turn, d):
        to, c = plane(turn), lax.rem(me + d, n)
        return pltpu.make_async_remote_copy(
            src_ref=second_ref.at[to, lax.rem(c, 2), c // 2],
            dst_ref=back_ref.at[dp, me],
            send_sem=b_send.at[turn],
            recv_sem=b_recv.at[turn],
            device_id={"dp": to, "ctx": c},
            device_id_type=MESH,
        )

    mixed_copies(3, lambda c: c.start())
    mixed_copies(1, lambda c: c.start())
    touched = jnp.zeros((shard, 1), f32)
    for z in range(planes):
        touched = touched + jnp.sum(picks_ref[z].astype(f32), axis=1, keepdims=True)
    acc_ref[...] = jnp.where(touched > 0.5, 0.0, doc_ref[...].astype(f32))
    for c in loads[10:]:
        c.wait()
    for _, c in o.passed:
        c.wait_recv()
    o.final()

    half = pairs * cap

    @pl.loop(0, planes)
    def _(t):
        turn = seat(t)
        source = plane(turn)
        bulk(m_in.at[source], m_send.at[turn], m_recv.at[turn]).wait_recv()

        @pl.when(turn > 0)
        def _():
            bulk(r_in.at[source], r_send.at[turn], r_recv.at[turn]).wait_recv()

        mixed = m_in[source].reshape(half, n * wide)
        heads = [mixed[:, h * wide : (h + 1) * wide] for h in range(n)]
        low = jnp.concatenate([h[:, :HS] for h in heads], axis=1)
        high = jnp.concatenate([h[:, HS:] for h in heads], axis=1)
        base = [r_in[source, 2 * j + side] for side in (0, 1) for j in range(pairs)]
        first_ref[...] = jnp.concatenate(base, axis=0).astype(f32) + jnp.dot(
            jnp.concatenate([low, high], axis=0),
            wo_all[...].reshape(n * HS, width),
            preferred_element_type=f32,
        )
        ffn_ref[...] = rms_scale(first_ref[...], gain_ffn_ref[...]).astype(bf)
        for f in range(0, inner, 256):
            hidden = jnp.dot(ffn_ref[...], w_in_ref[:, f : f + 256], preferred_element_type=f32)
            hidden_ref[:, f : f + 256] = jnp.maximum(hidden, 0.0).astype(bf)
        for f in range(0, width, 256):
            answer = jnp.dot(
                hidden_ref[...], w_back_ref[:, f : f + 256], preferred_element_type=f32
            ).astype(bf)
            second = (first_ref[:, f : f + 256] + answer.astype(f32)).astype(bf)
            second_ref[source, :, :, :, f : f + 256] = second.reshape(2, pairs, cap, 256)
        each(turn, lambda turn, d: back_copy(turn, d).start())

    pltpu.make_async_copy(
        second_ref.at[dp, lax.rem(me, 2), me // 2], back_ref.at[dp, me], b_recv.at[0]
    ).start()

    def returned(turn):
        source = plane(turn)
        bulk(back_ref.at[source], b_send.at[turn], b_recv.at[turn]).wait_recv()
        return acc_ref[...] + jnp.dot(
            picks_ref[source], back_ref[source].reshape(share, width), preferred_element_type=f32
        )

    for turn in (0, 1, 2):
        acc_ref[...] = returned(turn)

    out_ref[...] = returned(3).astype(bf)

    places.wait_send()

    for turn in range(planes):
        count = n - (turn == 0)
        bulk(m_out.at[pl.ds(0, count)], m_send.at[turn], m_recv.at[turn]).wait_send()
        bulk(back_ref.at[0, pl.ds(0, count)], b_send.at[turn], b_recv.at[turn]).wait_send()
        if turn:
            bulk(r_in.at[0], r_send.at[turn], r_recv.at[turn]).wait_send()
    for c in (twin, *last):
        c.wait_send()
    for c in own + passed + relays:
        c[0].wait_send()
        c[1].wait_send()
    o.drain()


def whole(document, kept, ids, gain_attn, gain_ffn, w_query, w_key, w_value, w_out, w_in, w_back):
    planes, n = lax.axis_size("dp"), lax.axis_size("ctx")
    owners = planes * n
    shard, width = document.shape
    rows = kept.shape[1]
    cap = 2 * rows // owners
    inner = w_in.shape[2]
    pairs = n // 2
    wide = 2 * HS
    half = pairs * cap
    bf, f32 = jnp.bfloat16, jnp.float32
    vmem = pl.BlockSpec(memory_space=pltpu.VMEM)
    hbm = pl.BlockSpec(memory_space=pltpu.HBM)
    sems = pltpu.SemaphoreType.DMA
    copies = gather_copies(n)
    grant = 42 * 1024 * 1024
    operands = (
        kept,
        ids,
        gain_attn.reshape(1, width),
        gain_ffn.reshape(1, width),
        document,
        w_query.T,
        w_key.T,
        w_value.T,
        w_out,
        w_in,
        w_back,
    )
    return pl.pallas_call(
        functools.partial(whole_kernel, planes, n, cap),
        out_shape=jax.ShapeDtypeStruct((shard, width), bf),
        in_specs=[hbm] * 11,
        out_specs=vmem,
        scratch_shapes=[
            pltpu.VMEM((1, rows), jnp.int32),
            pltpu.VMEM((1, rows), jnp.int32),
            pltpu.VMEM((1, width), f32),
            pltpu.VMEM((1, width), f32),
            pltpu.VMEM((shard, width), bf),
            pltpu.VMEM((8 * HS, width), bf),
            pltpu.VMEM(w_out.shape, bf),
            pltpu.VMEM(w_in.shape[1:], bf),
            pltpu.VMEM(w_back.shape[1:], bf),
            pltpu.VMEM((n, 8, rows), jnp.int32),
            pltpu.VMEM((n, rows, width), bf),
            pltpu.VMEM((n * rows, wide), bf),
            pltpu.VMEM((n * rows, wide), bf),
            pltpu.VMEM((2, n * rows, wide), bf),
            pltpu.VMEM((2 * rows, wide), bf),
            pltpu.VMEM((owners, pairs, cap, wide), bf),
            pltpu.VMEM((planes, pairs, cap, n * wide), bf),
            pltpu.VMEM((n,) + w_out.shape, bf),
            pltpu.VMEM((planes - 1, n, cap, width), bf),
            pltpu.VMEM((planes, n, cap, width), bf),
            pltpu.VMEM((2 * half, width), f32),
            pltpu.VMEM((2 * half, width), bf),
            pltpu.VMEM((2 * half, inner), bf),
            pltpu.VMEM((planes, 2, pairs, cap, width), bf),
            pltpu.VMEM((planes, n, cap, width), bf),
            pltpu.VMEM((planes, shard, n * cap), bf),
            pltpu.VMEM((shard, width), f32),
            sems((12,)),
            sems(()),
            sems(()),
            sems((15,)),
            sems((15,)),
            sems((copies,)),
            sems((copies,)),
            sems((planes,)),
            sems((planes,)),
            sems((planes,)),
            sems((planes,)),
            sems((planes,)),
            sems((planes,)),
            pltpu.SemaphoreType.REGULAR,
        ],
        compiler_params=pltpu.CompilerParams(
            collective_id=2, has_side_effects=True, vmem_limit_bytes=grant
        ),
        name="whole",
    )(*[pltpu.with_memory_space_constraint(a, pltpu.HBM) for a in operands])


def fits_whole(planes, n, keep_here, w_query, w_out, w_in):
    cap = 2 * keep_here // (planes * n)
    return (
        planes == 4
        and n == 8
        and w_query.shape[1] == HS
        and w_out.shape[0] == HS
        and w_in.shape[0] == 1
        and cap % 16 == 0
        and w_in.shape[2] % 256 == 0
    )


def body(
    tokens, kept, gain_attn, gain_ffn, w_query, w_key, w_value, w_out, expert_ids, w_in, w_back
):
    document = tokens[0]
    shard_len, width_model = document.shape
    ctx_count = lax.axis_size("ctx")
    dp_count = lax.axis_size("dp")
    if fits_whole(dp_count, ctx_count, kept.shape[1], w_query, w_out, w_in):
        ids = expert_ids.reshape(1, kept.shape[1])
        weights = (w_query, w_key, w_value, w_out, w_in, w_back)
        return whole(document, kept, ids, gain_attn, gain_ffn, *weights)[None]
    local = kept[0] - lax.axis_index("ctx") * shard_len
    keep_here = local.shape[0]
    positions = jnp.arange(shard_len, dtype=jnp.int32)
    picks = (local[:, None] == positions[None, :]).astype(jnp.bfloat16)
    rows = jnp.dot(picks, document, preferred_element_type=jnp.float32).astype(jnp.bfloat16)
    normed = rms_scale(rows, gain_attn).astype(jnp.bfloat16)
    mixed, w_out_all = attention(normed, w_query, w_key, w_value, w_out)
    inner_all = w_out.shape[0] * ctx_count
    attn = lax.dot_general(
        mixed.reshape(inner_all, keep_here),
        w_out_all.reshape(inner_all, width_model),
        (((0,), (0,)), ((), ())),
        preferred_element_type=jnp.float32,
    )
    first = rows.astype(jnp.float32) + attn
    ffn_in = rms_scale(first, gain_ffn).astype(jnp.bfloat16)
    expert_here = w_in.shape[0]
    owners = dp_count * ctx_count
    experts_all = expert_here * owners
    capacity = 2 * keep_here // experts_all
    labels = expert_ids[0, :, 0]
    order = jnp.arange(keep_here, dtype=jnp.int32)
    same = (labels[:, None] == labels[None, :]) & (order[None, :] < order[:, None])
    slots = jnp.sum(same.astype(jnp.int32), axis=1)
    place = labels * capacity + slots
    cells = jnp.arange(experts_all * capacity, dtype=jnp.int32)
    spots = (place[None, :] == cells[:, None]).astype(jnp.bfloat16)
    buffer = jnp.dot(spots, ffn_in, preferred_element_type=jnp.float32).astype(jnp.bfloat16)
    answers = experts(buffer, w_in, w_back, capacity)
    seats = (place[:, None] == cells[None, :]).astype(jnp.bfloat16)
    taken = jnp.dot(seats, answers, preferred_element_type=jnp.float32)
    second = (first + taken).astype(jnp.bfloat16)
    hits = positions[:, None] == local[None, :]
    fresh = jnp.dot(hits.astype(jnp.bfloat16), second, preferred_element_type=jnp.float32)
    touched = jnp.any(hits, axis=1, keepdims=True)
    blended = jnp.where(touched, fresh.astype(jnp.bfloat16), document)
    return blended[None]


def solution(mesh):
    return jax.shard_map(
        body,
        mesh=mesh,
        in_specs=(
            P("dp", "ctx", None),
            P("dp", "ctx"),
            P(),
            P(),
            P(None, "ctx"),
            P(None, "ctx"),
            P(None, "ctx"),
            P("ctx", None),
            P("dp", "ctx", None),
            P(("dp", "ctx"), None, None),
            P(("dp", "ctx"), None, None),
        ),
        out_specs=P("dp", "ctx", None),
        check_vma=False,
    )
```

```python
import functools
import math

import jax
import jax.numpy as jnp
from jax import lax
from jax.experimental import pallas as pl
from jax.experimental.pallas import tpu as pltpu
from jax.sharding import PartitionSpec as P

HS = 64
MESH = pl.DeviceIdType.MESH
LAST = (((1,), (1,)), ((), ()))

eps_norm = 1e-06
score_gain = 2.5


def rms_scale(values, gain):
    values = values.astype(jnp.float32)
    power = jnp.mean(values * values, axis=-1, keepdims=True)
    return values * lax.rsqrt(power + eps_norm) * gain


class Gather:
    def __init__(self, n, me, own, slots, send, recv):
        self.n, self.me, self.own, self.slots = n, me, own, slots
        self.send, self.recv = send, recv
        self.core, self.chip = me % 2, me // 2
        self.partner = me + 1 - 2 * self.core
        self.started = []

    def copy(self, ident, src, dst, target):
        return pltpu.make_async_remote_copy(
            src_ref=src,
            dst_ref=dst,
            send_sem=self.send.at[ident],
            recv_sem=self.recv.at[ident],
            device_id={"ctx": target},
            device_id_type=MESH,
        )

    def peers(self):
        chips = self.n // 2
        if chips == 4:
            x, y = self.chip % 2, self.chip // 2
            nx, ny = y * 2 + (1 - x), (1 - y) * 2 + x
            return [(nx, nx), (ny, ny)]
        return [
            ((self.chip + d) % chips, (self.chip + chips - d) % chips) for d in range(1, chips)
        ]

    def begin(self):
        own_to = self.slots.at[self.me]
        self.first = [
            self.copy(i, self.own, own_to, to * 2 + self.core)
            for i, (to, _) in enumerate(self.peers())
        ]
        self.base = len(self.first)
        self.twin = self.copy(self.base, self.own, own_to, self.partner)
        for c in self.first:
            c.start()
        self.twin.start()
        self.started = self.first + [self.twin]

    def relay(self):
        here, self.passed, self.late = [], [], []
        ident = self.base + 1
        peers = self.peers()
        square = self.n // 2 == 4
        half = self.own.shape[0] // 2
        for i, (_, source) in enumerate(peers):
            self.first[i].wait_recv()
            block = source * 2 + self.core
            here.append(block)
            if square:
                piece = self.slots.at[block, pl.ds(i * half, half)]
                c = self.copy(ident, piece, piece, peers[1 - i][0] * 2 + self.core)
                c.start()
                self.late.append(c)
                ident += 1
            c = self.copy(ident, self.slots.at[block], self.slots.at[block], self.partner)
            c.start()
            self.passed.append((source * 2 + 1 - self.core, c))
            ident += 1
        self.ident = ident
        self.started += self.late + [c for _, c in self.passed]
        return here

    def diagonal(self):
        if not self.late:
            return None
        block = (3 - self.chip) * 2 + self.core
        half = self.own.shape[0] // 2
        self.last = []
        for i, c in enumerate(self.late):
            c.wait_recv()
            piece = self.slots.at[block, pl.ds(i * half, half)]
            c = self.copy(self.ident + i, piece, piece, self.partner)
            c.start()
            self.last.append(c)
        self.started += self.last
        return block

    def final(self):
        if not self.late:
            return None
        for c in self.last:
            c.wait_recv()
        return (3 - self.chip) * 2 + 1 - self.core

    def drain(self):
        for c in self.started:
            c.wait_send()


def gather_copies(n):
    return 9 if n // 2 == 4 else 2 * (n // 2) - 1


def attention_kernel(
    n,
    heads,
    x_ref,
    wq_ref,
    wk_ref,
    wv_ref,
    wo_ref,
    mixed_ref,
    wo_all,
    x_all,
    q_all,
    k_all,
    v_all,
    stage,
    x_send,
    x_recv,
    o_send,
    o_recv,
    m_send,
    m_recv,
):
    me = lax.axis_index("ctx")
    rows = x_ref.shape[0]
    barrier = pltpu.get_barrier_semaphore()
    for d in range(1, n):
        pl.semaphore_signal(
            barrier, inc=1, device_id={"ctx": (me + d) % n}, device_id_type=MESH
        )
    pl.semaphore_wait(barrier, n - 1)

    def project(block, value):
        at = pl.ds(pl.multiple_of(block * rows, rows), rows)
        for h in range(heads):
            cols = pl.ds(h * HS, HS)
            q_all[h, at, :] = lax.dot_general(
                value, wq_ref[cols, :], LAST, preferred_element_type=jnp.float32
            ).astype(jnp.bfloat16)
            k_all[h, at, :] = lax.dot_general(
                value, wk_ref[cols, :], LAST, preferred_element_type=jnp.float32
            ).astype(jnp.bfloat16)
        v_all[:, at] = lax.dot_general(
            wv_ref[...], value, LAST, preferred_element_type=jnp.float32
        ).astype(jnp.bfloat16)

    g = Gather(n, me, x_ref, x_all, x_send, x_recv)
    o = Gather(n, me, wo_ref, wo_all, o_send, o_recv)
    g.begin()
    project(me, x_ref[...])
    wo_all[me] = wo_ref[...]
    g.twin.wait_recv()
    project(g.partner, x_all[g.partner])
    here = g.relay()
    o.begin()
    for block in here:
        project(block, x_all[block])
    for block, c in g.passed:
        c.wait_recv()
        project(block, x_all[block])
    block = g.diagonal()
    if block is not None:
        project(block, x_all[block])
    o.twin.wait_recv()
    o.relay()
    block = g.final()
    if block is not None:
        project(block, x_all[block])

    scale = score_gain / math.sqrt(HS) * math.log2(math.e)

    def send_block(step, target):
        return pltpu.make_async_remote_copy(
            src_ref=stage.at[step],
            dst_ref=mixed_ref.at[me],
            send_sem=m_send.at[step],
            recv_sem=m_recv.at[step],
            device_id={"ctx": target},
            device_id_type=MESH,
        )

    @pl.loop(0, n)
    def _(step):
        block = lax.rem(me + 1 + step, n)
        at = pl.ds(pl.multiple_of(block * rows, rows), rows)
        for h in range(heads):
            scores = lax.dot_general(
                k_all[h],
                q_all[h, at, :],
                LAST,
                preferred_element_type=jnp.float32,
            )
            top = jnp.max(scores, axis=0, keepdims=True)
            weights = jnp.exp2(scores * scale - top * scale)
            total = jnp.sum(weights, axis=0, keepdims=True)
            cols = pl.ds(h * HS, HS)
            mixed = jnp.dot(
                v_all[cols, :],
                weights.astype(jnp.bfloat16),
                preferred_element_type=jnp.float32,
            )
            stage[step, cols, :] = (mixed / total).astype(jnp.bfloat16)

        @pl.when(step < n - 1)
        def _():
            send_block(step, block).start()

    mixed_ref[me] = stage[n - 1]
    for _, c in o.passed:
        c.wait_recv()
    o.diagonal()
    o.final()

    @pl.loop(0, n - 1)
    def _(step):
        send_block(step, lax.rem(me + 1 + step, n)).wait()

    g.drain()
    o.drain()


def attention(normed, w_query, w_key, w_value, w_out):
    n = lax.axis_size("ctx")
    rows, width = normed.shape
    inner = w_query.shape[1]
    heads = inner // HS
    copies = gather_copies(n)
    vmem = pl.BlockSpec(memory_space=pltpu.VMEM)
    bf = jnp.bfloat16
    return pl.pallas_call(
        functools.partial(attention_kernel, n, heads),
        out_shape=(
            jax.ShapeDtypeStruct((n, inner, rows), bf),
            jax.ShapeDtypeStruct((n,) + w_out.shape, bf),
        ),
        in_specs=[vmem] * 5,
        out_specs=(vmem, vmem),
        scratch_shapes=[
            pltpu.VMEM((n, rows, width), bf),
            pltpu.VMEM((heads, n * rows, HS), bf),
            pltpu.VMEM((heads, n * rows, HS), bf),
            pltpu.VMEM((inner, n * rows), bf),
            pltpu.VMEM((n, inner, rows), bf),
            pltpu.SemaphoreType.DMA((copies,)),
            pltpu.SemaphoreType.DMA((copies,)),
            pltpu.SemaphoreType.DMA((copies,)),
            pltpu.SemaphoreType.DMA((copies,)),
            pltpu.SemaphoreType.DMA((n,)),
            pltpu.SemaphoreType.DMA((n,)),
        ],
        compiler_params=pltpu.CompilerParams(collective_id=0, has_side_effects=True),
        name="attention",
    )(normed, w_query.T, w_key.T, w_value.T, w_out)


def experts_plain(buffer, w_in, w_back, capacity):
    owners = lax.axis_size("dp") * lax.axis_size("ctx")
    expert_here, width = w_in.shape[0], buffer.shape[1]
    buffer = buffer.reshape(owners * expert_here, capacity, width)
    received = lax.all_to_all(buffer, ("dp", "ctx"), split_axis=0, concat_axis=0, tiled=True)
    grouped = received.reshape(owners, expert_here, capacity, width)
    hidden = jnp.einsum("sgid,gdf->sgif", grouped, w_in, preferred_element_type=jnp.float32)
    hidden = jnp.maximum(hidden, 0.0).astype(jnp.bfloat16)
    answer = jnp.einsum("sgif,gfd->sgid", hidden, w_back, preferred_element_type=jnp.float32)
    answered = answer.astype(jnp.bfloat16).reshape(owners * expert_here, capacity, width)
    back = lax.all_to_all(answered, ("dp", "ctx"), split_axis=0, concat_axis=0, tiled=True)
    return back.reshape(owners * expert_here * capacity, width)


def expert_kernel(
    planes,
    n,
    cap,
    buf_ref,
    w_in_hbm,
    w_back_hbm,
    back_ref,
    w_in_ref,
    w_back_ref,
    rows_ref,
    hidden_ref,
    answer_ref,
    w_sem,
    own_sem,
    d_send,
    d_recv,
    r_send,
    r_recv,
):
    dp, ctx = lax.axis_index("dp"), lax.axis_index("ctx")
    me = dp * n + ctx
    owners = planes * n
    loads = [
        pltpu.make_async_copy(w_in_hbm.at[0], w_in_ref, w_sem.at[0]),
        pltpu.make_async_copy(w_back_hbm.at[0], w_back_ref, w_sem.at[1]),
    ]
    for c in loads:
        c.start()
    barrier = pltpu.get_barrier_semaphore()

    @pl.loop(1, owners)
    def _(d):
        to = lax.rem(me + d, owners)
        pl.semaphore_signal(
            barrier, inc=1, device_id={"dp": to // n, "ctx": lax.rem(to, n)}, device_id_type=MESH
        )

    pl.semaphore_wait(barrier, owners - 1)

    def seat(index):
        return pl.ds(pl.multiple_of(index * cap, cap), cap)

    def at(shift):
        plane_shift, place_shift = shift // n, lax.rem(shift, n)
        half = planes // 2
        side = dp // half
        side = lax.rem(side + plane_shift // half, 2)
        plane = side * half + lax.rem(dp + plane_shift, half)
        return plane, lax.rem(ctx + place_shift, n)

    def dispatch(shift):
        plane, place = at(shift)
        return pltpu.make_async_remote_copy(
            src_ref=buf_ref.at[seat(plane * n + place)],
            dst_ref=rows_ref.at[seat(me)],
            send_sem=d_send.at[shift],
            recv_sem=d_recv.at[shift],
            device_id={"dp": plane, "ctx": place},
            device_id_type=MESH,
        )

    def give_back(shift):
        plane, place = at(shift)
        return pltpu.make_async_remote_copy(
            src_ref=answer_ref.at[seat(plane * n + place)],
            dst_ref=back_ref.at[seat(me)],
            send_sem=r_send.at[shift],
            recv_sem=r_recv.at[shift],
            device_id={"dp": plane, "ctx": place},
            device_id_type=MESH,
        )

    near = owners // 2

    @pl.loop(0, near)
    def _(shift):
        dispatch(near + shift).start()

        @pl.when(shift > 0)
        def _():
            dispatch(shift).start()

    own_in = pltpu.make_async_copy(buf_ref.at[seat(me)], rows_ref.at[seat(me)], own_sem.at[0])
    own_in.start()

    def run(first_row, count):
        inner = hidden_ref.shape[1]
        width = answer_ref.shape[1]
        take = pl.ds(pl.multiple_of(first_row, count), count)
        value = rows_ref[take, :]

        @pl.loop(0, inner // 256)
        def _(f):
            cols = pl.ds(pl.multiple_of(f * 256, 256), 256)
            hidden = jnp.dot(value, w_in_ref[:, cols], preferred_element_type=jnp.float32)
            hidden_ref[:, cols] = jnp.maximum(hidden, 0.0).astype(jnp.bfloat16)

        @pl.loop(0, width // 256)
        def _(f):
            cols = pl.ds(pl.multiple_of(f * 256, 256), 256)
            answer_ref[take, cols] = jnp.dot(
                hidden_ref[...], w_back_ref[:, cols], preferred_element_type=jnp.float32
            ).astype(jnp.bfloat16)

    half_rows = near * cap
    side = dp // (planes // 2)

    @pl.loop(1, near)
    def _(shift):
        dispatch(shift).wait_recv()

    own_in.wait()
    for c in loads:
        c.wait()

    @pl.loop(0, 2)
    def _(turn):
        @pl.when(turn == 1)
        def _():
            @pl.loop(near, owners)
            def _(shift):
                dispatch(shift).wait_recv()

        run(lax.rem(side + turn, 2) * half_rows, half_rows)

        @pl.loop(0, near)
        def _(shift):
            @pl.when(turn * near + shift > 0)
            def _():
                give_back(turn * near + shift).start()

    own_out = pltpu.make_async_copy(answer_ref.at[seat(me)], back_ref.at[seat(me)], own_sem.at[1])
    own_out.start()

    @pl.loop(1, owners)
    def _(shift):
        dispatch(shift).wait_send()
        give_back(shift).wait()

    own_out.wait()


def experts_fused(buffer, w_in, w_back, capacity):
    planes, n = lax.axis_size("dp"), lax.axis_size("ctx")
    owners = planes * n
    slots, width = buffer.shape
    inner = w_in.shape[2]
    bf = jnp.bfloat16
    vmem = pl.BlockSpec(memory_space=pltpu.VMEM)
    hbm = pl.BlockSpec(memory_space=pl.ANY)
    return pl.pallas_call(
        functools.partial(expert_kernel, planes, n, capacity),
        out_shape=jax.ShapeDtypeStruct((slots, width), bf),
        in_specs=[vmem, hbm, hbm],
        out_specs=vmem,
        scratch_shapes=[
            pltpu.VMEM(w_in.shape[1:], bf),
            pltpu.VMEM(w_back.shape[1:], bf),
            pltpu.VMEM((slots, width), bf),
            pltpu.VMEM((slots // 2, inner), bf),
            pltpu.VMEM((slots, width), bf),
            pltpu.SemaphoreType.DMA((2,)),
            pltpu.SemaphoreType.DMA((2,)),
            pltpu.SemaphoreType.DMA((owners,)),
            pltpu.SemaphoreType.DMA((owners,)),
            pltpu.SemaphoreType.DMA((owners,)),
            pltpu.SemaphoreType.DMA((owners,)),
        ],
        compiler_params=pltpu.CompilerParams(collective_id=1, has_side_effects=True),
        name="experts",
    )(buffer, w_in, w_back)


def experts(buffer, w_in, w_back, capacity):
    if capacity % 16 == 0 and w_in.shape[0] == 1:
        return experts_fused(buffer, w_in, w_back, capacity)
    return experts_plain(buffer, w_in, w_back, capacity)


def whole_kernel(
    planes,
    n,
    cap,
    kept_hbm,
    ids_hbm,
    gain_attn_hbm,
    gain_ffn_hbm,
    doc_hbm,
    wq_hbm,
    wk_hbm,
    wv_hbm,
    wo_hbm,
    w_in_hbm,
    w_back_hbm,
    out_ref,
    kept_ref,
    ids_ref,
    gain_attn_ref,
    gain_ffn_ref,
    doc_ref,
    w3_ref,
    wo_ref,
    w_in_ref,
    w_back_ref,
    place_all,
    x_all,
    q_all,
    k_all,
    v_all,
    sum_ref,
    top_ref,
    mix_ref,
    cells_ref,
    m_out,
    m_in,
    wo_all,
    r_out,
    r_in,
    first_ref,
    ffn_ref,
    hidden_ref,
    second_ref,
    back_ref,
    picks_ref,
    acc_ref,
    w_sem,
    p_send,
    p_recv,
    x_send,
    x_recv,
    o_send,
    o_recv,
    r_send,
    r_recv,
    m_send,
    m_recv,
    b_send,
    b_recv,
    ready,
):
    f32, bf = jnp.float32, jnp.bfloat16
    dp, me = lax.axis_index("dp"), lax.axis_index("ctx")
    owners = planes * n
    rows, width = x_all.shape[1], x_all.shape[2]
    shard = doc_ref.shape[0]
    inner = hidden_ref.shape[1]
    wide = 2 * HS
    share = n * cap
    pairs = n // 2

    loads = [
        pltpu.make_async_copy(ids_hbm, ids_ref, w_sem.at[8]),
        pltpu.make_async_copy(kept_hbm, kept_ref, w_sem.at[9]),
        pltpu.make_async_copy(doc_hbm, doc_ref, w_sem.at[0]),
        pltpu.make_async_copy(gain_attn_hbm, gain_attn_ref, w_sem.at[10]),
        pltpu.make_async_copy(gain_ffn_hbm, gain_ffn_ref, w_sem.at[11]),
        pltpu.make_async_copy(wq_hbm, w3_ref.at[pl.ds(0, HS)], w_sem.at[1]),
        pltpu.make_async_copy(wk_hbm, w3_ref.at[pl.ds(2 * HS, HS)], w_sem.at[2]),
        pltpu.make_async_copy(wv_hbm, w3_ref.at[pl.ds(4 * HS, HS)], w_sem.at[3]),
        pltpu.make_async_copy(wo_hbm, wo_ref, w_sem.at[5]),
        pltpu.make_async_copy(w_in_hbm.at[0], w_in_ref, w_sem.at[6]),
        pltpu.make_async_copy(w_back_hbm.at[0], w_back_ref, w_sem.at[7]),
    ]
    for c in loads:
        c.start()

    barrier = pltpu.get_barrier_semaphore()

    for d in range(1, n):
        pl.semaphore_signal(
            barrier, inc=1, device_id={"ctx": lax.rem(me + d, n)}, device_id_type=MESH
        )

    def column(sem):
        for d in range(1, planes):
            pl.semaphore_signal(
                sem, inc=1, device_id={"dp": lax.rem(dp + d, planes)}, device_id_type=MESH
            )

    column(barrier)

    def plane(g):
        high = lax.rem(dp // 2 + g // 2, 2)
        return high * 2 + lax.rem(dp + lax.rem(g, 2), 2)

    def one_hot(mask):
        return jnp.where(mask, 1.0, 0.0).astype(bf)

    def iota(shape, dim):
        return lax.broadcasted_iota(jnp.int32, shape, dim)

    loads[0].wait()
    ids = ids_ref[...]
    named = one_hot(iota((owners, rows), 0) == ids)
    earlier = one_hot(iota((rows, rows), 0) < iota((rows, rows), 1))
    before = jnp.dot(named, earlier, preferred_element_type=f32)
    slot = jnp.sum(named.astype(f32) * before, axis=0, keepdims=True).astype(jnp.int32)
    place_own = ids * cap + slot
    place_all[me] = jnp.broadcast_to(place_own, place_all.shape[1:])
    loads[1].wait()
    local = kept_ref[...] - me * shard
    picks = one_hot(iota((shard, rows), 0) == local)
    loads[2].wait()
    x_all[me] = lax.dot_general(
        picks, doc_ref[...], (((0,), (0,)), ((), ())), preferred_element_type=f32
    ).astype(bf)

    pl.semaphore_wait(barrier, n + planes - 2)
    column(ready)

    o = Gather(n, me, wo_ref, wo_all, o_send, o_recv)

    def bulk(ref, sends, recvs):
        return pltpu.make_async_remote_copy(
            src_ref=ref,
            dst_ref=ref,
            send_sem=sends,
            recv_sem=recvs,
            device_id={"ctx": o.partner},
            device_id_type=MESH,
        )

    def place_copy(d):
        return pltpu.make_async_remote_copy(
            src_ref=place_all.at[me],
            dst_ref=place_all.at[me],
            send_sem=p_send,
            recv_sem=p_recv,
            device_id={"ctx": lax.rem(me + d, n)},
            device_id_type=MESH,
        )

    for d in range(1, n):
        place_copy(d).start()

    core, chip, partner = o.core, o.chip, o.partner
    (near_x, _), (near_y, _) = o.peers()
    part, piece = rows // 2, rows // 4

    def send(ident, block, first, count, target):
        ref = x_all.at[block, pl.ds(pl.multiple_of(first, count), count)]
        return pltpu.make_async_remote_copy(
            src_ref=ref,
            dst_ref=ref,
            send_sem=x_send.at[ident],
            recv_sem=x_recv.at[ident],
            device_id={"ctx": target},
            device_id_type=MESH,
        )

    to_x, to_y = near_x * 2 + core, near_y * 2 + core
    mine = core * part
    twin = send(0, me, (1 - core) * part, part, partner)
    rest = send(15, me, mine, part, partner)
    own, passed, relays, last = [], [], [], []
    for k in (0, 1):
        from_x, from_y, across = near_x * 2 + k, near_y * 2 + k, (3 - chip) * 2 + k
        own.append(
            (
                send(1 + k, chip * 2 + k, mine, part, to_x),
                send(3 + k, chip * 2 + k, mine, part, to_y),
            )
        )
        passed.append(
            (send(5 + k, from_x, mine, part, partner), send(7 + k, from_y, mine, part, partner))
        )
        relays.append(
            (
                send(9 + k, from_x, mine, piece, to_y),
                send(11 + k, from_y, mine + piece, piece, to_x),
            )
        )
        last.append(send(13 + k, across, mine, part, partner))
    twin.start()
    rest.start()

    @pl.when(core == 0)
    def _():
        for c in own[0]:
            c.start()

    blank = jnp.zeros((HS, width), bf)
    for i in (1, 3, 5):
        w3_ref[pl.ds(i * HS, HS), :] = blank
    for c in loads[3:9]:
        c.wait()

    def row_copy(turn, block):
        return pltpu.make_async_remote_copy(
            src_ref=r_out.at[turn - 1, block],
            dst_ref=r_in.at[dp, block],
            send_sem=r_send.at[turn],
            recv_sem=r_recv.at[turn],
            device_id={"dp": plane(turn)},
            device_id_type=MESH,
        )

    def route(block, value):
        index = iota((planes * cap, rows), 0)
        turn, s = index // cap, index % cap
        high = (dp // 2 + turn // 2) % 2
        to = high * 2 + (dp + turn % 2) % 2
        cell = (to * n + me) * cap + s
        taken = jnp.dot(
            one_hot(cell == place_all[block][0:1, :]), value, preferred_element_type=f32
        ).astype(bf)
        r_in[dp, block] = taken[0:cap]
        for turn in (2, 3, 1):
            r_out[turn - 1, block] = taken[turn * cap : (turn + 1) * cap]
            row_copy(turn, block).start()

    def project(spot, value):
        at = pl.ds(pl.multiple_of(spot * rows, rows), rows)
        normed = rms_scale(value, gain_attn_ref[...]).astype(bf)
        three = lax.dot_general(normed, w3_ref[...], LAST, preferred_element_type=f32)
        q_all[at, :] = three[:, 0:wide].astype(bf)
        k_all[at, :] = three[:, wide : 2 * wide].astype(bf)
        lane = iota((rows, wide), 1)
        v_all[at, :] = jnp.where(lane < HS, three[:, 2 * wide : 3 * wide], 1.0).astype(bf)

    def take(block, spot):
        value = x_all[block]
        route(block, value)
        project(spot, value)

    scale = score_gain / math.sqrt(HS) * math.log2(math.e)

    def update(spot, spots, first, count, fresh):
        at = pl.ds(spot * rows, spots * rows)
        keys = pl.ds(first * rows, count * rows)
        scores = lax.dot_general(q_all[at, :], k_all[keys, :], LAST, preferred_element_type=f32)
        top = jnp.broadcast_to(
            jnp.max(scores, axis=1, keepdims=True), (spots * rows, wide)
        )
        if not fresh:
            known = top_ref[at, :]
            top = jnp.maximum(top, known)
        shift = jnp.concatenate([top * scale] * (count * rows // wide), axis=1)
        weights = jnp.exp2(scores * scale - shift)
        both = jnp.dot(weights.astype(bf), v_all[keys, :], preferred_element_type=f32)
        if not fresh:
            both = both + sum_ref[at, :] * jnp.exp2(known * scale - top * scale)
        sum_ref[at, :] = both
        top_ref[at, :] = top

    def match(chip):
        places = [place_all[2 * chip + side][0:1, :] for side in (0, 1)]
        cells_ref[chip] = one_hot(
            iota((owners * cap, 2 * rows), 0) == jnp.concatenate(places, axis=1)
        )

    take(me, core)
    twin.wait_recv()

    @pl.when(core == 1)
    def _():
        for c in own[0]:
            c.start()

    for c in own[1]:
        c.start()
    for z in range(planes):
        cells = one_hot(iota((share, rows), 0) + z * share == place_own)
        picks_ref[z] = lax.dot_general(picks, cells, LAST, preferred_element_type=f32).astype(bf)
    wo_all[me] = wo_ref[...]
    places = bulk(place_all.at[pl.ds(0, n - 1)], p_send, p_recv)
    places.wait_recv()
    def mixed_copy(turn, d, j):
        to, c = plane(turn), lax.rem(me + d, n)
        lanes = pl.ds(pl.multiple_of(me * wide, wide), wide)
        return pltpu.make_async_remote_copy(
            src_ref=m_out.at[to * n + c, j],
            dst_ref=m_in.at[dp, j, :, lanes],
            send_sem=m_send.at[turn],
            recv_sem=m_recv.at[turn],
            device_id={"dp": to, "ctx": c},
            device_id_type=MESH,
        )

    def mixed_own(j):
        lanes = pl.ds(pl.multiple_of(me * wide, wide), wide)
        return pltpu.make_async_copy(
            m_out.at[dp * n + me, j], m_in.at[dp, j, :, lanes], m_recv.at[0]
        )

    def each(turn, act):
        @pl.loop(0, n)
        def _(d):
            @pl.when(turn + d > 0)
            def _():
                act(turn, d)

    def mixed_copies(turn, act):
        def some(turn, d):
            for j in range(pairs):
                act(mixed_copy(turn, d, j))

        each(turn, some)

    def finish(chip, spots):
        for side, spot in enumerate(spots):
            both = sum_ref[pl.ds(spot * rows, rows), :]
            mixed = jnp.where(iota((rows, wide), 1) < HS, both / pltpu.roll(both, HS, 1), 0.0)
            if side:
                mixed = pltpu.roll(mixed, HS, 1)
            mix_ref[pl.ds(side * rows, rows), :] = mixed.astype(bf)
        spread = jnp.dot(cells_ref[chip], mix_ref[...], preferred_element_type=f32).astype(bf)
        m_out[:, chip] = spread.reshape(owners, cap, wide)
        each(2, lambda turn, d: mixed_copy(turn, d, chip).start())
        each(0, lambda turn, d: mixed_copy(turn, d, chip).start())
        mixed_own(chip).start()

    rest.wait_recv()
    take(partner, 1 - core)
    update(0, 2, 0, 2, True)
    for at in range(pairs):
        match(at)
    for c, p, r in zip(own[0], passed[0], relays[0]):
        c.wait_recv()
        p.start()
        r.start()
    for i, near in enumerate((near_x, near_y)):
        passed[0][i].wait_recv()
        take(near * 2, 2 + i)
    update(0, 2, 2, 2, False)
    update(2, 2, 0, 4, True)
    for c, p, r in zip(own[1], passed[1], relays[1]):
        c.wait_recv()
        p.start()
        r.start()
    for i, near in enumerate((near_x, near_y)):
        passed[1][i].wait_recv()
        take(near * 2 + 1, 4 + i)
    update(0, 4, 4, 2, False)
    for r in relays[0]:
        r.wait_recv()
    last[0].start()
    o.begin()
    update(4, 2, 0, 6, True)
    for r in relays[1]:
        r.wait_recv()
    last[1].start()
    for k in (0, 1):
        last[k].wait_recv()
        take((3 - chip) * 2 + k, 6 + k)
    update(0, 6, 6, 2, False)
    o.twin.wait_recv()
    o.relay()
    pl.semaphore_wait(ready, planes - 1)
    finish(chip, (0, 1))
    finish(near_x, (2, 4))
    finish(near_y, (3, 5))
    update(6, 2, 0, 8, True)
    finish(3 - chip, (6, 7))
    o.diagonal()

    def seat(t):
        return lax.rem(t + planes // 2, planes)

    def back_copy(turn, d):
        to, c = plane(turn), lax.rem(me + d, n)
        return pltpu.make_async_remote_copy(
            src_ref=second_ref.at[to, lax.rem(c, 2), c // 2],
            dst_ref=back_ref.at[dp, me],
            send_sem=b_send.at[turn],
            recv_sem=b_recv.at[turn],
            device_id={"dp": to, "ctx": c},
            device_id_type=MESH,
        )

    mixed_copies(3, lambda c: c.start())
    mixed_copies(1, lambda c: c.start())
    touched = jnp.zeros((shard, 1), f32)
    for z in range(planes):
        touched = touched + jnp.sum(picks_ref[z].astype(f32), axis=1, keepdims=True)
    acc_ref[...] = jnp.where(touched > 0.5, 0.0, doc_ref[...].astype(f32))
    for c in loads[9:]:
        c.wait()
    for _, c in o.passed:
        c.wait_recv()
    o.final()

    half = pairs * cap

    @pl.loop(0, planes)
    def _(t):
        turn = seat(t)
        source = plane(turn)
        bulk(m_in.at[source], m_send.at[turn], m_recv.at[turn]).wait_recv()

        @pl.when(turn > 0)
        def _():
            bulk(r_in.at[source], r_send.at[turn], r_recv.at[turn]).wait_recv()

        mixed = m_in[source].reshape(half, n * wide)
        heads = [mixed[:, h * wide : (h + 1) * wide] for h in range(n)]
        low = jnp.concatenate([h[:, :HS] for h in heads], axis=1)
        high = jnp.concatenate([h[:, HS:] for h in heads], axis=1)
        base = [r_in[source, 2 * j + side] for side in (0, 1) for j in range(pairs)]
        first_ref[...] = jnp.concatenate(base, axis=0).astype(f32) + jnp.dot(
            jnp.concatenate([low, high], axis=0),
            wo_all[...].reshape(n * HS, width),
            preferred_element_type=f32,
        )
        ffn_ref[...] = rms_scale(first_ref[...], gain_ffn_ref[...]).astype(bf)
        for f in range(0, inner, 256):
            hidden = jnp.dot(ffn_ref[...], w_in_ref[:, f : f + 256], preferred_element_type=f32)
            hidden_ref[:, f : f + 256] = jnp.maximum(hidden, 0.0).astype(bf)
        for f in range(0, width, 256):
            answer = jnp.dot(
                hidden_ref[...], w_back_ref[:, f : f + 256], preferred_element_type=f32
            ).astype(bf)
            second = (first_ref[:, f : f + 256] + answer.astype(f32)).astype(bf)
            second_ref[source, :, :, :, f : f + 256] = second.reshape(2, pairs, cap, 256)
        each(turn, lambda turn, d: back_copy(turn, d).start())

    pltpu.make_async_copy(
        second_ref.at[dp, lax.rem(me, 2), me // 2], back_ref.at[dp, me], b_recv.at[0]
    ).start()

    def returned(turn):
        source = plane(turn)
        bulk(back_ref.at[source], b_send.at[turn], b_recv.at[turn]).wait_recv()
        return acc_ref[...] + jnp.dot(
            picks_ref[source], back_ref[source].reshape(share, width), preferred_element_type=f32
        )

    for turn in (0, 1, 2):
        acc_ref[...] = returned(turn)

    out_ref[...] = returned(3).astype(bf)

    places.wait_send()

    for turn in range(planes):
        count = n - (turn == 0)
        bulk(m_out.at[pl.ds(0, count)], m_send.at[turn], m_recv.at[turn]).wait_send()
        bulk(back_ref.at[0, pl.ds(0, count)], b_send.at[turn], b_recv.at[turn]).wait_send()
        if turn:
            bulk(r_in.at[0], r_send.at[turn], r_recv.at[turn]).wait_send()
    for c in (twin, rest, *last):
        c.wait_send()
    for c in own + passed + relays:
        c[0].wait_send()
        c[1].wait_send()
    o.drain()


def whole(document, kept, ids, gain_attn, gain_ffn, w_query, w_key, w_value, w_out, w_in, w_back):
    planes, n = lax.axis_size("dp"), lax.axis_size("ctx")
    owners = planes * n
    shard, width = document.shape
    rows = kept.shape[1]
    cap = 2 * rows // owners
    inner = w_in.shape[2]
    pairs = n // 2
    wide = 2 * HS
    half = pairs * cap
    bf, f32 = jnp.bfloat16, jnp.float32
    vmem = pl.BlockSpec(memory_space=pltpu.VMEM)
    hbm = pl.BlockSpec(memory_space=pltpu.HBM)
    sems = pltpu.SemaphoreType.DMA
    copies = gather_copies(n)
    grant = 42 * 1024 * 1024
    operands = (
        kept,
        ids,
        gain_attn.reshape(1, width),
        gain_ffn.reshape(1, width),
        document,
        w_query.T,
        w_key.T,
        w_value.T,
        w_out,
        w_in,
        w_back,
    )
    return pl.pallas_call(
        functools.partial(whole_kernel, planes, n, cap),
        out_shape=jax.ShapeDtypeStruct((shard, width), bf),
        in_specs=[hbm] * 11,
        out_specs=vmem,
        scratch_shapes=[
            pltpu.VMEM((1, rows), jnp.int32),
            pltpu.VMEM((1, rows), jnp.int32),
            pltpu.VMEM((1, width), f32),
            pltpu.VMEM((1, width), f32),
            pltpu.VMEM((shard, width), bf),
            pltpu.VMEM((6 * HS, width), bf),
            pltpu.VMEM(w_out.shape, bf),
            pltpu.VMEM(w_in.shape[1:], bf),
            pltpu.VMEM(w_back.shape[1:], bf),
            pltpu.VMEM((n, 8, rows), jnp.int32),
            pltpu.VMEM((n, rows, width), bf),
            pltpu.VMEM((n * rows, wide), bf),
            pltpu.VMEM((n * rows, wide), bf),
            pltpu.VMEM((n * rows, wide), bf),
            pltpu.VMEM((n * rows, wide), f32),
            pltpu.VMEM((n * rows, wide), f32),
            pltpu.VMEM((2 * rows, wide), bf),
            pltpu.VMEM((n // 2, owners * cap, 2 * rows), bf),
            pltpu.VMEM((owners, pairs, cap, wide), bf),
            pltpu.VMEM((planes, pairs, cap, n * wide), bf),
            pltpu.VMEM((n,) + w_out.shape, bf),
            pltpu.VMEM((planes - 1, n, cap, width), bf),
            pltpu.VMEM((planes, n, cap, width), bf),
            pltpu.VMEM((2 * half, width), f32),
            pltpu.VMEM((2 * half, width), bf),
            pltpu.VMEM((2 * half, inner), bf),
            pltpu.VMEM((planes, 2, pairs, cap, width), bf),
            pltpu.VMEM((planes, n, cap, width), bf),
            pltpu.VMEM((planes, shard, n * cap), bf),
            pltpu.VMEM((shard, width), f32),
            sems((12,)),
            sems(()),
            sems(()),
            sems((16,)),
            sems((16,)),
            sems((copies,)),
            sems((copies,)),
            sems((planes,)),
            sems((planes,)),
            sems((planes,)),
            sems((planes,)),
            sems((planes,)),
            sems((planes,)),
            pltpu.SemaphoreType.REGULAR,
        ],
        compiler_params=pltpu.CompilerParams(
            collective_id=2, has_side_effects=True, vmem_limit_bytes=grant
        ),
        name="whole",
    )(*[pltpu.with_memory_space_constraint(a, pltpu.HBM) for a in operands])


def fits_whole(planes, n, keep_here, w_query, w_out, w_in):
    cap = 2 * keep_here // (planes * n)
    return (
        planes == 4
        and n == 8
        and w_query.shape[1] == HS
        and w_out.shape[0] == HS
        and w_in.shape[0] == 1
        and cap % 16 == 0
        and w_in.shape[2] % 256 == 0
    )


def body(
    tokens, kept, gain_attn, gain_ffn, w_query, w_key, w_value, w_out, expert_ids, w_in, w_back
):
    document = tokens[0]
    shard_len, width_model = document.shape
    ctx_count = lax.axis_size("ctx")
    dp_count = lax.axis_size("dp")
    if fits_whole(dp_count, ctx_count, kept.shape[1], w_query, w_out, w_in):
        ids = expert_ids.reshape(1, kept.shape[1])
        weights = (w_query, w_key, w_value, w_out, w_in, w_back)
        return whole(document, kept, ids, gain_attn, gain_ffn, *weights)[None]
    local = kept[0] - lax.axis_index("ctx") * shard_len
    keep_here = local.shape[0]
    positions = jnp.arange(shard_len, dtype=jnp.int32)
    picks = (local[:, None] == positions[None, :]).astype(jnp.bfloat16)
    rows = jnp.dot(picks, document, preferred_element_type=jnp.float32).astype(jnp.bfloat16)
    normed = rms_scale(rows, gain_attn).astype(jnp.bfloat16)
    mixed, w_out_all = attention(normed, w_query, w_key, w_value, w_out)
    inner_all = w_out.shape[0] * ctx_count
    attn = lax.dot_general(
        mixed.reshape(inner_all, keep_here),
        w_out_all.reshape(inner_all, width_model),
        (((0,), (0,)), ((), ())),
        preferred_element_type=jnp.float32,
    )
    first = rows.astype(jnp.float32) + attn
    ffn_in = rms_scale(first, gain_ffn).astype(jnp.bfloat16)
    expert_here = w_in.shape[0]
    owners = dp_count * ctx_count
    experts_all = expert_here * owners
    capacity = 2 * keep_here // experts_all
    labels = expert_ids[0, :, 0]
    order = jnp.arange(keep_here, dtype=jnp.int32)
    same = (labels[:, None] == labels[None, :]) & (order[None, :] < order[:, None])
    slots = jnp.sum(same.astype(jnp.int32), axis=1)
    place = labels * capacity + slots
    cells = jnp.arange(experts_all * capacity, dtype=jnp.int32)
    spots = (place[None, :] == cells[:, None]).astype(jnp.bfloat16)
    buffer = jnp.dot(spots, ffn_in, preferred_element_type=jnp.float32).astype(jnp.bfloat16)
    answers = experts(buffer, w_in, w_back, capacity)
    seats = (place[:, None] == cells[None, :]).astype(jnp.bfloat16)
    taken = jnp.dot(seats, answers, preferred_element_type=jnp.float32)
    second = (first + taken).astype(jnp.bfloat16)
    hits = positions[:, None] == local[None, :]
    fresh = jnp.dot(hits.astype(jnp.bfloat16), second, preferred_element_type=jnp.float32)
    touched = jnp.any(hits, axis=1, keepdims=True)
    blended = jnp.where(touched, fresh.astype(jnp.bfloat16), document)
    return blended[None]


def solution(mesh):
    return jax.shard_map(
        body,
        mesh=mesh,
        in_specs=(
            P("dp", "ctx", None),
            P("dp", "ctx"),
            P(),
            P(),
            P(None, "ctx"),
            P(None, "ctx"),
            P(None, "ctx"),
            P("ctx", None),
            P("dp", "ctx", None),
            P(("dp", "ctx"), None, None),
            P(("dp", "ctx"), None, None),
        ),
        out_specs=P("dp", "ctx", None),
        check_vma=False,
    )
```

```python
import functools
import math

import jax
import jax.numpy as jnp
from jax import lax
from jax.experimental import pallas as pl
from jax.experimental.pallas import tpu as pltpu
from jax.sharding import PartitionSpec as P

HS = 64
MESH = pl.DeviceIdType.MESH
LAST = (((1,), (1,)), ((), ()))

eps_norm = 1e-06
score_gain = 2.5


def rms_scale(values, gain):
    values = values.astype(jnp.float32)
    power = jnp.mean(values * values, axis=-1, keepdims=True)
    return values * lax.rsqrt(power + eps_norm) * gain


class Gather:
    def __init__(self, n, me, own, slots, send, recv):
        self.n, self.me, self.own, self.slots = n, me, own, slots
        self.send, self.recv = send, recv
        self.core, self.chip = me % 2, me // 2
        self.partner = me + 1 - 2 * self.core
        self.started = []

    def copy(self, ident, src, dst, target):
        return pltpu.make_async_remote_copy(
            src_ref=src,
            dst_ref=dst,
            send_sem=self.send.at[ident],
            recv_sem=self.recv.at[ident],
            device_id={"ctx": target},
            device_id_type=MESH,
        )

    def peers(self):
        chips = self.n // 2
        if chips == 4:
            x, y = self.chip % 2, self.chip // 2
            nx, ny = y * 2 + (1 - x), (1 - y) * 2 + x
            return [(nx, nx), (ny, ny)]
        return [
            ((self.chip + d) % chips, (self.chip + chips - d) % chips) for d in range(1, chips)
        ]

    def begin(self):
        own_to = self.slots.at[self.me]
        self.first = [
            self.copy(i, self.own, own_to, to * 2 + self.core)
            for i, (to, _) in enumerate(self.peers())
        ]
        self.base = len(self.first)
        self.twin = self.copy(self.base, self.own, own_to, self.partner)
        for c in self.first:
            c.start()
        self.twin.start()
        self.started = self.first + [self.twin]

    def relay(self):
        here, self.passed, self.late = [], [], []
        ident = self.base + 1
        peers = self.peers()
        square = self.n // 2 == 4
        half = self.own.shape[0] // 2
        for i, (_, source) in enumerate(peers):
            self.first[i].wait_recv()
            block = source * 2 + self.core
            here.append(block)
            if square:
                piece = self.slots.at[block, pl.ds(i * half, half)]
                c = self.copy(ident, piece, piece, peers[1 - i][0] * 2 + self.core)
                c.start()
                self.late.append(c)
                ident += 1
            c = self.copy(ident, self.slots.at[block], self.slots.at[block], self.partner)
            c.start()
            self.passed.append((source * 2 + 1 - self.core, c))
            ident += 1
        self.ident = ident
        self.started += self.late + [c for _, c in self.passed]
        return here

    def diagonal(self):
        if not self.late:
            return None
        block = (3 - self.chip) * 2 + self.core
        half = self.own.shape[0] // 2
        self.last = []
        for i, c in enumerate(self.late):
            c.wait_recv()
            piece = self.slots.at[block, pl.ds(i * half, half)]
            c = self.copy(self.ident + i, piece, piece, self.partner)
            c.start()
            self.last.append(c)
        self.started += self.last
        return block

    def final(self):
        if not self.late:
            return None
        for c in self.last:
            c.wait_recv()
        return (3 - self.chip) * 2 + 1 - self.core

    def drain(self):
        for c in self.started:
            c.wait_send()


def gather_copies(n):
    return 9 if n // 2 == 4 else 2 * (n // 2) - 1


def attention_kernel(
    n,
    heads,
    x_ref,
    wq_ref,
    wk_ref,
    wv_ref,
    wo_ref,
    mixed_ref,
    wo_all,
    x_all,
    q_all,
    k_all,
    v_all,
    stage,
    x_send,
    x_recv,
    o_send,
    o_recv,
    m_send,
    m_recv,
):
    me = lax.axis_index("ctx")
    rows = x_ref.shape[0]
    barrier = pltpu.get_barrier_semaphore()
    for d in range(1, n):
        pl.semaphore_signal(
            barrier, inc=1, device_id={"ctx": (me + d) % n}, device_id_type=MESH
        )
    pl.semaphore_wait(barrier, n - 1)

    def project(block, value):
        at = pl.ds(pl.multiple_of(block * rows, rows), rows)
        for h in range(heads):
            cols = pl.ds(h * HS, HS)
            q_all[h, at, :] = lax.dot_general(
                value, wq_ref[cols, :], LAST, preferred_element_type=jnp.float32
            ).astype(jnp.bfloat16)
            k_all[h, at, :] = lax.dot_general(
                value, wk_ref[cols, :], LAST, preferred_element_type=jnp.float32
            ).astype(jnp.bfloat16)
        v_all[:, at] = lax.dot_general(
            wv_ref[...], value, LAST, preferred_element_type=jnp.float32
        ).astype(jnp.bfloat16)

    g = Gather(n, me, x_ref, x_all, x_send, x_recv)
    o = Gather(n, me, wo_ref, wo_all, o_send, o_recv)
    g.begin()
    project(me, x_ref[...])
    wo_all[me] = wo_ref[...]
    g.twin.wait_recv()
    project(g.partner, x_all[g.partner])
    here = g.relay()
    o.begin()
    for block in here:
        project(block, x_all[block])
    for block, c in g.passed:
        c.wait_recv()
        project(block, x_all[block])
    block = g.diagonal()
    if block is not None:
        project(block, x_all[block])
    o.twin.wait_recv()
    o.relay()
    block = g.final()
    if block is not None:
        project(block, x_all[block])

    scale = score_gain / math.sqrt(HS) * math.log2(math.e)

    def send_block(step, target):
        return pltpu.make_async_remote_copy(
            src_ref=stage.at[step],
            dst_ref=mixed_ref.at[me],
            send_sem=m_send.at[step],
            recv_sem=m_recv.at[step],
            device_id={"ctx": target},
            device_id_type=MESH,
        )

    @pl.loop(0, n)
    def _(step):
        block = lax.rem(me + 1 + step, n)
        at = pl.ds(pl.multiple_of(block * rows, rows), rows)
        for h in range(heads):
            scores = lax.dot_general(
                k_all[h],
                q_all[h, at, :],
                LAST,
                preferred_element_type=jnp.float32,
            )
            top = jnp.max(scores, axis=0, keepdims=True)
            weights = jnp.exp2(scores * scale - top * scale)
            total = jnp.sum(weights, axis=0, keepdims=True)
            cols = pl.ds(h * HS, HS)
            mixed = jnp.dot(
                v_all[cols, :],
                weights.astype(jnp.bfloat16),
                preferred_element_type=jnp.float32,
            )
            stage[step, cols, :] = (mixed / total).astype(jnp.bfloat16)

        @pl.when(step < n - 1)
        def _():
            send_block(step, block).start()

    mixed_ref[me] = stage[n - 1]
    for _, c in o.passed:
        c.wait_recv()
    o.diagonal()
    o.final()

    @pl.loop(0, n - 1)
    def _(step):
        send_block(step, lax.rem(me + 1 + step, n)).wait()

    g.drain()
    o.drain()


def attention(normed, w_query, w_key, w_value, w_out):
    n = lax.axis_size("ctx")
    rows, width = normed.shape
    inner = w_query.shape[1]
    heads = inner // HS
    copies = gather_copies(n)
    vmem = pl.BlockSpec(memory_space=pltpu.VMEM)
    bf = jnp.bfloat16
    return pl.pallas_call(
        functools.partial(attention_kernel, n, heads),
        out_shape=(
            jax.ShapeDtypeStruct((n, inner, rows), bf),
            jax.ShapeDtypeStruct((n,) + w_out.shape, bf),
        ),
        in_specs=[vmem] * 5,
        out_specs=(vmem, vmem),
        scratch_shapes=[
            pltpu.VMEM((n, rows, width), bf),
            pltpu.VMEM((heads, n * rows, HS), bf),
            pltpu.VMEM((heads, n * rows, HS), bf),
            pltpu.VMEM((inner, n * rows), bf),
            pltpu.VMEM((n, inner, rows), bf),
            pltpu.SemaphoreType.DMA((copies,)),
            pltpu.SemaphoreType.DMA((copies,)),
            pltpu.SemaphoreType.DMA((copies,)),
            pltpu.SemaphoreType.DMA((copies,)),
            pltpu.SemaphoreType.DMA((n,)),
            pltpu.SemaphoreType.DMA((n,)),
        ],
        compiler_params=pltpu.CompilerParams(collective_id=0, has_side_effects=True),
        name="attention",
    )(normed, w_query.T, w_key.T, w_value.T, w_out)


def experts_plain(buffer, w_in, w_back, capacity):
    owners = lax.axis_size("dp") * lax.axis_size("ctx")
    expert_here, width = w_in.shape[0], buffer.shape[1]
    buffer = buffer.reshape(owners * expert_here, capacity, width)
    received = lax.all_to_all(buffer, ("dp", "ctx"), split_axis=0, concat_axis=0, tiled=True)
    grouped = received.reshape(owners, expert_here, capacity, width)
    hidden = jnp.einsum("sgid,gdf->sgif", grouped, w_in, preferred_element_type=jnp.float32)
    hidden = jnp.maximum(hidden, 0.0).astype(jnp.bfloat16)
    answer = jnp.einsum("sgif,gfd->sgid", hidden, w_back, preferred_element_type=jnp.float32)
    answered = answer.astype(jnp.bfloat16).reshape(owners * expert_here, capacity, width)
    back = lax.all_to_all(answered, ("dp", "ctx"), split_axis=0, concat_axis=0, tiled=True)
    return back.reshape(owners * expert_here * capacity, width)


def expert_kernel(
    planes,
    n,
    cap,
    buf_ref,
    w_in_hbm,
    w_back_hbm,
    back_ref,
    w_in_ref,
    w_back_ref,
    rows_ref,
    hidden_ref,
    answer_ref,
    w_sem,
    own_sem,
    d_send,
    d_recv,
    r_send,
    r_recv,
):
    dp, ctx = lax.axis_index("dp"), lax.axis_index("ctx")
    me = dp * n + ctx
    owners = planes * n
    loads = [
        pltpu.make_async_copy(w_in_hbm.at[0], w_in_ref, w_sem.at[0]),
        pltpu.make_async_copy(w_back_hbm.at[0], w_back_ref, w_sem.at[1]),
    ]
    for c in loads:
        c.start()
    barrier = pltpu.get_barrier_semaphore()

    @pl.loop(1, owners)
    def _(d):
        to = lax.rem(me + d, owners)
        pl.semaphore_signal(
            barrier, inc=1, device_id={"dp": to // n, "ctx": lax.rem(to, n)}, device_id_type=MESH
        )

    pl.semaphore_wait(barrier, owners - 1)

    def seat(index):
        return pl.ds(pl.multiple_of(index * cap, cap), cap)

    def at(shift):
        plane_shift, place_shift = shift // n, lax.rem(shift, n)
        half = planes // 2
        side = dp // half
        side = lax.rem(side + plane_shift // half, 2)
        plane = side * half + lax.rem(dp + plane_shift, half)
        return plane, lax.rem(ctx + place_shift, n)

    def dispatch(shift):
        plane, place = at(shift)
        return pltpu.make_async_remote_copy(
            src_ref=buf_ref.at[seat(plane * n + place)],
            dst_ref=rows_ref.at[seat(me)],
            send_sem=d_send.at[shift],
            recv_sem=d_recv.at[shift],
            device_id={"dp": plane, "ctx": place},
            device_id_type=MESH,
        )

    def give_back(shift):
        plane, place = at(shift)
        return pltpu.make_async_remote_copy(
            src_ref=answer_ref.at[seat(plane * n + place)],
            dst_ref=back_ref.at[seat(me)],
            send_sem=r_send.at[shift],
            recv_sem=r_recv.at[shift],
            device_id={"dp": plane, "ctx": place},
            device_id_type=MESH,
        )

    near = owners // 2

    @pl.loop(0, near)
    def _(shift):
        dispatch(near + shift).start()

        @pl.when(shift > 0)
        def _():
            dispatch(shift).start()

    own_in = pltpu.make_async_copy(buf_ref.at[seat(me)], rows_ref.at[seat(me)], own_sem.at[0])
    own_in.start()

    def run(first_row, count):
        inner = hidden_ref.shape[1]
        width = answer_ref.shape[1]
        take = pl.ds(pl.multiple_of(first_row, count), count)
        value = rows_ref[take, :]

        @pl.loop(0, inner // 256)
        def _(f):
            cols = pl.ds(pl.multiple_of(f * 256, 256), 256)
            hidden = jnp.dot(value, w_in_ref[:, cols], preferred_element_type=jnp.float32)
            hidden_ref[:, cols] = jnp.maximum(hidden, 0.0).astype(jnp.bfloat16)

        @pl.loop(0, width // 256)
        def _(f):
            cols = pl.ds(pl.multiple_of(f * 256, 256), 256)
            answer_ref[take, cols] = jnp.dot(
                hidden_ref[...], w_back_ref[:, cols], preferred_element_type=jnp.float32
            ).astype(jnp.bfloat16)

    half_rows = near * cap
    side = dp // (planes // 2)

    @pl.loop(1, near)
    def _(shift):
        dispatch(shift).wait_recv()

    own_in.wait()
    for c in loads:
        c.wait()

    @pl.loop(0, 2)
    def _(turn):
        @pl.when(turn == 1)
        def _():
            @pl.loop(near, owners)
            def _(shift):
                dispatch(shift).wait_recv()

        run(lax.rem(side + turn, 2) * half_rows, half_rows)

        @pl.loop(0, near)
        def _(shift):
            @pl.when(turn * near + shift > 0)
            def _():
                give_back(turn * near + shift).start()

    own_out = pltpu.make_async_copy(answer_ref.at[seat(me)], back_ref.at[seat(me)], own_sem.at[1])
    own_out.start()

    @pl.loop(1, owners)
    def _(shift):
        dispatch(shift).wait_send()
        give_back(shift).wait()

    own_out.wait()


def experts_fused(buffer, w_in, w_back, capacity):
    planes, n = lax.axis_size("dp"), lax.axis_size("ctx")
    owners = planes * n
    slots, width = buffer.shape
    inner = w_in.shape[2]
    bf = jnp.bfloat16
    vmem = pl.BlockSpec(memory_space=pltpu.VMEM)
    hbm = pl.BlockSpec(memory_space=pl.ANY)
    return pl.pallas_call(
        functools.partial(expert_kernel, planes, n, capacity),
        out_shape=jax.ShapeDtypeStruct((slots, width), bf),
        in_specs=[vmem, hbm, hbm],
        out_specs=vmem,
        scratch_shapes=[
            pltpu.VMEM(w_in.shape[1:], bf),
            pltpu.VMEM(w_back.shape[1:], bf),
            pltpu.VMEM((slots, width), bf),
            pltpu.VMEM((slots // 2, inner), bf),
            pltpu.VMEM((slots, width), bf),
            pltpu.SemaphoreType.DMA((2,)),
            pltpu.SemaphoreType.DMA((2,)),
            pltpu.SemaphoreType.DMA((owners,)),
            pltpu.SemaphoreType.DMA((owners,)),
            pltpu.SemaphoreType.DMA((owners,)),
            pltpu.SemaphoreType.DMA((owners,)),
        ],
        compiler_params=pltpu.CompilerParams(collective_id=1, has_side_effects=True),
        name="experts",
    )(buffer, w_in, w_back)


def experts(buffer, w_in, w_back, capacity):
    if capacity % 16 == 0 and w_in.shape[0] == 1:
        return experts_fused(buffer, w_in, w_back, capacity)
    return experts_plain(buffer, w_in, w_back, capacity)


def whole_kernel(
    planes,
    n,
    cap,
    kept_hbm,
    ids_hbm,
    gain_attn_hbm,
    gain_ffn_hbm,
    doc_hbm,
    wq_hbm,
    wk_hbm,
    wv_hbm,
    wo_hbm,
    w_in_hbm,
    w_back_hbm,
    out_ref,
    kept_ref,
    ids_ref,
    gain_attn_ref,
    gain_ffn_ref,
    doc_ref,
    w3_ref,
    wo_ref,
    w_in_ref,
    w_back_ref,
    place_all,
    x_all,
    q_all,
    k_all,
    v_all,
    sum_ref,
    top_ref,
    mix_ref,
    cells_ref,
    m_out,
    m_in,
    wo_all,
    r_out,
    r_in,
    first_ref,
    ffn_ref,
    hidden_ref,
    second_ref,
    back_ref,
    picks_ref,
    acc_ref,
    w_sem,
    p_send,
    p_recv,
    x_send,
    x_recv,
    o_send,
    o_recv,
    r_send,
    r_recv,
    m_send,
    m_recv,
    b_send,
    b_recv,
    ready,
):
    f32, bf = jnp.float32, jnp.bfloat16
    dp, me = lax.axis_index("dp"), lax.axis_index("ctx")
    owners = planes * n
    rows, width = x_all.shape[1], x_all.shape[2]
    shard = doc_ref.shape[0]
    inner = hidden_ref.shape[1]
    wide = 2 * HS
    share = n * cap
    pairs = n // 2

    loads = [
        pltpu.make_async_copy(ids_hbm, ids_ref, w_sem.at[8]),
        pltpu.make_async_copy(kept_hbm, kept_ref, w_sem.at[9]),
        pltpu.make_async_copy(doc_hbm, doc_ref, w_sem.at[0]),
        pltpu.make_async_copy(gain_attn_hbm, gain_attn_ref, w_sem.at[10]),
        pltpu.make_async_copy(gain_ffn_hbm, gain_ffn_ref, w_sem.at[11]),
        pltpu.make_async_copy(wq_hbm, w3_ref.at[pl.ds(0, HS)], w_sem.at[1]),
        pltpu.make_async_copy(wk_hbm, w3_ref.at[pl.ds(2 * HS, HS)], w_sem.at[2]),
        pltpu.make_async_copy(wv_hbm, w3_ref.at[pl.ds(4 * HS, HS)], w_sem.at[3]),
        pltpu.make_async_copy(wo_hbm, wo_ref, w_sem.at[5]),
        pltpu.make_async_copy(w_in_hbm.at[0], w_in_ref, w_sem.at[6]),
        pltpu.make_async_copy(w_back_hbm.at[0], w_back_ref, w_sem.at[7]),
    ]

    barrier = pltpu.get_barrier_semaphore()

    for d in range(1, n):
        pl.semaphore_signal(
            barrier, inc=1, device_id={"ctx": lax.rem(me + d, n)}, device_id_type=MESH
        )

    def column(sem):
        for d in range(1, planes):
            pl.semaphore_signal(
                sem, inc=1, device_id={"dp": lax.rem(dp + d, planes)}, device_id_type=MESH
            )

    column(barrier)
    for c in loads:
        c.start()

    def plane(g):
        high = lax.rem(dp // 2 + g // 2, 2)
        return high * 2 + lax.rem(dp + lax.rem(g, 2), 2)

    def one_hot(mask):
        return jnp.where(mask, 1.0, 0.0).astype(bf)

    def iota(shape, dim):
        return lax.broadcasted_iota(jnp.int32, shape, dim)

    loads[0].wait()
    ids = ids_ref[...]
    named = one_hot(iota((owners, rows), 0) == ids)
    earlier = one_hot(iota((rows, rows), 0) < iota((rows, rows), 1))
    before = jnp.dot(named, earlier, preferred_element_type=f32)
    slot = jnp.sum(named.astype(f32) * before, axis=0, keepdims=True).astype(jnp.int32)
    place_own = ids * cap + slot
    place_all[me] = jnp.broadcast_to(place_own, place_all.shape[1:])
    loads[1].wait()
    local = kept_ref[...] - me * shard
    picks = one_hot(iota((shard, rows), 0) == local)
    loads[2].wait()
    x_all[me] = lax.dot_general(
        picks, doc_ref[...], (((0,), (0,)), ((), ())), preferred_element_type=f32
    ).astype(bf)

    pl.semaphore_wait(barrier, n + planes - 2)
    column(ready)

    o = Gather(n, me, wo_ref, wo_all, o_send, o_recv)

    def bulk(ref, sends, recvs):
        return pltpu.make_async_remote_copy(
            src_ref=ref,
            dst_ref=ref,
            send_sem=sends,
            recv_sem=recvs,
            device_id={"ctx": o.partner},
            device_id_type=MESH,
        )

    def place_copy(d):
        return pltpu.make_async_remote_copy(
            src_ref=place_all.at[me],
            dst_ref=place_all.at[me],
            send_sem=p_send,
            recv_sem=p_recv,
            device_id={"ctx": lax.rem(me + d, n)},
            device_id_type=MESH,
        )

    for d in range(1, n):
        place_copy(d).start()

    core, chip, partner = o.core, o.chip, o.partner
    (near_x, _), (near_y, _) = o.peers()
    part, piece = rows // 2, rows // 4

    def send(ident, block, first, count, target):
        ref = x_all.at[block, pl.ds(pl.multiple_of(first, count), count)]
        return pltpu.make_async_remote_copy(
            src_ref=ref,
            dst_ref=ref,
            send_sem=x_send,
            recv_sem=x_recv.at[ident],
            device_id={"ctx": target},
            device_id_type=MESH,
        )

    to_x, to_y = near_x * 2 + core, near_y * 2 + core
    mine = core * part
    twin = send(0, me, (1 - core) * part, part, partner)
    rest = send(15, me, mine, part, partner)
    own, passed, relays, last = [], [], [], []
    for k in (0, 1):
        from_x, from_y, across = near_x * 2 + k, near_y * 2 + k, (3 - chip) * 2 + k
        own.append(
            (
                send(1 + k, chip * 2 + k, mine, part, to_x),
                send(3 + k, chip * 2 + k, mine, part, to_y),
            )
        )
        passed.append(
            (send(5 + k, from_x, mine, part, partner), send(7 + k, from_y, mine, part, partner))
        )
        relays.append(
            (
                send(9 + k, from_x, mine, piece, to_y),
                send(11 + k, from_y, mine + piece, piece, to_x),
            )
        )
        last.append(send(13 + k, across, mine, part, partner))
    twin.start()

    @pl.when(core == 0)
    def _():
        for c in own[0]:
            c.start()

    blank = jnp.zeros((HS, width), bf)
    for i in (1, 3, 5):
        w3_ref[pl.ds(i * HS, HS), :] = blank
    for c in loads[3:9]:
        c.wait()

    def row_copy(turn, block):
        return pltpu.make_async_remote_copy(
            src_ref=r_out.at[turn - 1, block],
            dst_ref=r_in.at[dp, block],
            send_sem=r_send.at[turn],
            recv_sem=r_recv.at[turn],
            device_id={"dp": plane(turn)},
            device_id_type=MESH,
        )

    def route(block, value):
        index = iota((planes * cap, rows), 0)
        turn, s = index // cap, index % cap
        high = (dp // 2 + turn // 2) % 2
        to = high * 2 + (dp + turn % 2) % 2
        cell = (to * n + me) * cap + s
        taken = jnp.dot(
            one_hot(cell == place_all[block][0:1, :]), value, preferred_element_type=f32
        ).astype(bf)
        r_in[dp, block] = taken[0:cap]
        for turn in (2, 3, 1):
            r_out[turn - 1, block] = taken[turn * cap : (turn + 1) * cap]
            row_copy(turn, block).start()

    def project(spot, value):
        at = pl.ds(pl.multiple_of(spot * rows, rows), rows)
        normed = rms_scale(value, gain_attn_ref[...]).astype(bf)
        three = lax.dot_general(normed, w3_ref[...], LAST, preferred_element_type=f32)
        q_all[at, :] = three[:, 0:wide].astype(bf)
        k_all[at, :] = three[:, wide : 2 * wide].astype(bf)
        lane = iota((rows, wide), 1)
        v_all[at, :] = jnp.where(lane < HS, three[:, 2 * wide : 3 * wide], 1.0).astype(bf)

    def take(block, spot):
        value = x_all[block]
        route(block, value)
        project(spot, value)

    scale = score_gain / math.sqrt(HS) * math.log2(math.e)

    def update(spot, spots, first, count, fresh):
        at = pl.ds(spot * rows, spots * rows)
        keys = pl.ds(first * rows, count * rows)
        scores = lax.dot_general(q_all[at, :], k_all[keys, :], LAST, preferred_element_type=f32)
        top = jnp.broadcast_to(
            jnp.max(scores, axis=1, keepdims=True), (spots * rows, wide)
        )
        if not fresh:
            known = top_ref[at, :]
            top = jnp.maximum(top, known)
        shift = jnp.concatenate([top * scale] * (count * rows // wide), axis=1)
        weights = jnp.exp2(scores * scale - shift)
        both = jnp.dot(weights.astype(bf), v_all[keys, :], preferred_element_type=f32)
        if not fresh:
            both = both + sum_ref[at, :] * jnp.exp2(known * scale - top * scale)
        sum_ref[at, :] = both
        top_ref[at, :] = top

    def match(chip):
        places = [place_all[2 * chip + side][0:1, :] for side in (0, 1)]
        cells_ref[chip] = one_hot(
            iota((owners * cap, 2 * rows), 0) == jnp.concatenate(places, axis=1)
        )

    twin.wait_recv()

    @pl.when(core == 1)
    def _():
        for c in own[0]:
            c.start()

    rest.start()
    for c in own[1]:
        c.start()
    take(me, core)
    for z in range(planes):
        cells = one_hot(iota((share, rows), 0) + z * share == place_own)
        picks_ref[z] = lax.dot_general(picks, cells, LAST, preferred_element_type=f32).astype(bf)
    wo_all[me] = wo_ref[...]
    places = bulk(place_all.at[pl.ds(0, n - 1)], p_send, p_recv)
    places.wait_recv()
    def mixed_copy(turn, d, j):
        to, c = plane(turn), lax.rem(me + d, n)
        lanes = pl.ds(pl.multiple_of(me * wide, wide), wide)
        return pltpu.make_async_remote_copy(
            src_ref=m_out.at[to * n + c, j],
            dst_ref=m_in.at[dp, j, :, lanes],
            send_sem=m_send.at[turn],
            recv_sem=m_recv.at[turn],
            device_id={"dp": to, "ctx": c},
            device_id_type=MESH,
        )

    def mixed_own(j):
        lanes = pl.ds(pl.multiple_of(me * wide, wide), wide)
        return pltpu.make_async_copy(
            m_out.at[dp * n + me, j], m_in.at[dp, j, :, lanes], m_recv.at[0]
        )

    def each(turn, act):
        @pl.loop(0, n)
        def _(d):
            @pl.when(turn + d > 0)
            def _():
                act(turn, d)

    def mixed_copies(turn, act):
        def some(turn, d):
            for j in range(pairs):
                act(mixed_copy(turn, d, j))

        each(turn, some)

    def finish(chip, spots):
        for side, spot in enumerate(spots):
            both = sum_ref[pl.ds(spot * rows, rows), :]
            mixed = jnp.where(iota((rows, wide), 1) < HS, both / pltpu.roll(both, HS, 1), 0.0)
            if side:
                mixed = pltpu.roll(mixed, HS, 1)
            mix_ref[pl.ds(side * rows, rows), :] = mixed.astype(bf)
        spread = jnp.dot(cells_ref[chip], mix_ref[...], preferred_element_type=f32).astype(bf)
        m_out[:, chip] = spread.reshape(owners, cap, wide)
        each(2, lambda turn, d: mixed_copy(turn, d, chip).start())
        each(3, lambda turn, d: mixed_copy(turn, d, chip).start())

    rest.wait_recv()
    take(partner, 1 - core)
    update(0, 2, 0, 2, True)
    for at in range(pairs):
        match(at)
    for c, p, r in zip(own[0], passed[0], relays[0]):
        c.wait_recv()
        p.start()
        r.start()
    for i, near in enumerate((near_x, near_y)):
        passed[0][i].wait_recv()
        take(near * 2, 2 + i)
    update(0, 2, 2, 2, False)
    update(2, 2, 0, 4, True)
    for c, p, r in zip(own[1], passed[1], relays[1]):
        c.wait_recv()
        p.start()
        r.start()
    for i, near in enumerate((near_x, near_y)):
        passed[1][i].wait_recv()
        take(near * 2 + 1, 4 + i)
    update(0, 4, 4, 2, False)
    for r in relays[0]:
        r.wait_recv()
    last[0].start()
    o.begin()
    update(4, 2, 0, 6, True)
    for r in relays[1]:
        r.wait_recv()
    last[1].start()
    for k in (0, 1):
        last[k].wait_recv()
        take((3 - chip) * 2 + k, 6 + k)
    update(0, 6, 6, 2, False)
    o.twin.wait_recv()
    o.relay()
    pl.semaphore_wait(ready, planes - 1)
    finish(chip, (0, 1))
    finish(near_x, (2, 4))
    finish(near_y, (3, 5))
    update(6, 2, 0, 8, True)
    finish(3 - chip, (6, 7))
    o.diagonal()

    def seat(t):
        return lax.rem(t + planes // 2, planes)

    def back_copy(turn, d):
        to, c = plane(turn), lax.rem(me + d, n)
        return pltpu.make_async_remote_copy(
            src_ref=second_ref.at[to, lax.rem(c, 2), c // 2],
            dst_ref=back_ref.at[dp, me],
            send_sem=b_send.at[turn],
            recv_sem=b_recv.at[turn],
            device_id={"dp": to, "ctx": c},
            device_id_type=MESH,
        )

    mixed_copies(0, lambda c: c.start())
    mixed_copies(1, lambda c: c.start())
    for j in range(pairs):
        mixed_own(j).start()
    touched = jnp.zeros((shard, 1), f32)
    for z in range(planes):
        touched = touched + jnp.sum(picks_ref[z].astype(f32), axis=1, keepdims=True)
    acc_ref[...] = jnp.where(touched > 0.5, 0.0, doc_ref[...].astype(f32))
    for c in loads[9:]:
        c.wait()
    for _, c in o.passed:
        c.wait_recv()
    o.final()

    half = pairs * cap

    @pl.loop(0, planes)
    def _(t):
        turn = seat(t)
        source = plane(turn)
        bulk(m_in.at[source], m_send.at[turn], m_recv.at[turn]).wait_recv()

        @pl.when(turn > 0)
        def _():
            bulk(r_in.at[source], r_send.at[turn], r_recv.at[turn]).wait_recv()

        mixed = m_in[source].reshape(half, n * wide)
        heads = [mixed[:, h * wide : (h + 1) * wide] for h in range(n)]
        low = jnp.concatenate([h[:, :HS] for h in heads], axis=1)
        high = jnp.concatenate([h[:, HS:] for h in heads], axis=1)
        base = [r_in[source, 2 * j + side] for side in (0, 1) for j in range(pairs)]
        first_ref[...] = jnp.concatenate(base, axis=0).astype(f32) + jnp.dot(
            jnp.concatenate([low, high], axis=0),
            wo_all[...].reshape(n * HS, width),
            preferred_element_type=f32,
        )
        ffn_ref[...] = rms_scale(first_ref[...], gain_ffn_ref[...]).astype(bf)
        for f in range(0, inner, 256):
            hidden = jnp.dot(ffn_ref[...], w_in_ref[:, f : f + 256], preferred_element_type=f32)
            hidden_ref[:, f : f + 256] = jnp.maximum(hidden, 0.0).astype(bf)
        for f in range(0, width, 256):
            answer = jnp.dot(
                hidden_ref[...], w_back_ref[:, f : f + 256], preferred_element_type=f32
            ).astype(bf)
            second = (first_ref[:, f : f + 256] + answer.astype(f32)).astype(bf)
            second_ref[source, :, :, :, f : f + 256] = second.reshape(2, pairs, cap, 256)
        each(turn, lambda turn, d: back_copy(turn, d).start())

    pltpu.make_async_copy(
        second_ref.at[dp, lax.rem(me, 2), me // 2], back_ref.at[dp, me], b_recv.at[0]
    ).start()

    def returned(turn):
        source = plane(turn)
        bulk(back_ref.at[source], b_send.at[turn], b_recv.at[turn]).wait_recv()
        return acc_ref[...] + jnp.dot(
            picks_ref[source], back_ref[source].reshape(share, width), preferred_element_type=f32
        )

    for turn in (0, 1, 2):
        acc_ref[...] = returned(turn)

    out_ref[...] = returned(3).astype(bf)

    places.wait_send()

    for turn in range(planes):
        count = n - (turn == 0)
        bulk(m_out.at[pl.ds(0, count)], m_send.at[turn], m_recv.at[turn]).wait_send()
        bulk(back_ref.at[0, pl.ds(0, count)], b_send.at[turn], b_recv.at[turn]).wait_send()
        if turn:
            bulk(r_in.at[0], r_send.at[turn], r_recv.at[turn]).wait_send()
    bulk(x_all.at[pl.ds(0, n - 1)], x_send, x_recv.at[0]).wait_send()
    o.drain()


def whole(document, kept, ids, gain_attn, gain_ffn, w_query, w_key, w_value, w_out, w_in, w_back):
    planes, n = lax.axis_size("dp"), lax.axis_size("ctx")
    owners = planes * n
    shard, width = document.shape
    rows = kept.shape[1]
    cap = 2 * rows // owners
    inner = w_in.shape[2]
    pairs = n // 2
    wide = 2 * HS
    half = pairs * cap
    bf, f32 = jnp.bfloat16, jnp.float32
    vmem = pl.BlockSpec(memory_space=pltpu.VMEM)
    hbm = pl.BlockSpec(memory_space=pltpu.HBM)
    sems = pltpu.SemaphoreType.DMA
    copies = gather_copies(n)
    grant = 42 * 1024 * 1024
    operands = (
        kept,
        ids,
        gain_attn.reshape(1, width),
        gain_ffn.reshape(1, width),
        document,
        w_query.T,
        w_key.T,
        w_value.T,
        w_out,
        w_in,
        w_back,
    )
    return pl.pallas_call(
        functools.partial(whole_kernel, planes, n, cap),
        out_shape=jax.ShapeDtypeStruct((shard, width), bf),
        in_specs=[hbm] * 11,
        out_specs=vmem,
        scratch_shapes=[
            pltpu.VMEM((1, rows), jnp.int32),
            pltpu.VMEM((1, rows), jnp.int32),
            pltpu.VMEM((1, width), f32),
            pltpu.VMEM((1, width), f32),
            pltpu.VMEM((shard, width), bf),
            pltpu.VMEM((6 * HS, width), bf),
            pltpu.VMEM(w_out.shape, bf),
            pltpu.VMEM(w_in.shape[1:], bf),
            pltpu.VMEM(w_back.shape[1:], bf),
            pltpu.VMEM((n, 8, rows), jnp.int32),
            pltpu.VMEM((n, rows, width), bf),
            pltpu.VMEM((n * rows, wide), bf),
            pltpu.VMEM((n * rows, wide), bf),
            pltpu.VMEM((n * rows, wide), bf),
            pltpu.VMEM((n * rows, wide), f32),
            pltpu.VMEM((n * rows, wide), f32),
            pltpu.VMEM((2 * rows, wide), bf),
            pltpu.VMEM((n // 2, owners * cap, 2 * rows), bf),
            pltpu.VMEM((owners, pairs, cap, wide), bf),
            pltpu.VMEM((planes, pairs, cap, n * wide), bf),
            pltpu.VMEM((n,) + w_out.shape, bf),
            pltpu.VMEM((planes - 1, n, cap, width), bf),
            pltpu.VMEM((planes, n, cap, width), bf),
            pltpu.VMEM((2 * half, width), f32),
            pltpu.VMEM((2 * half, width), bf),
            pltpu.VMEM((2 * half, inner), bf),
            pltpu.VMEM((planes, 2, pairs, cap, width), bf),
            pltpu.VMEM((planes, n, cap, width), bf),
            pltpu.VMEM((planes, shard, n * cap), bf),
            pltpu.VMEM((shard, width), f32),
            sems((12,)),
            sems(()),
            sems(()),
            sems(()),
            sems((16,)),
            sems((copies,)),
            sems((copies,)),
            sems((planes,)),
            sems((planes,)),
            sems((planes,)),
            sems((planes,)),
            sems((planes,)),
            sems((planes,)),
            pltpu.SemaphoreType.REGULAR,
        ],
        compiler_params=pltpu.CompilerParams(
            collective_id=2, has_side_effects=True, vmem_limit_bytes=grant
        ),
        name="whole",
    )(*[pltpu.with_memory_space_constraint(a, pltpu.HBM) for a in operands])


def fits_whole(planes, n, keep_here, w_query, w_out, w_in):
    cap = 2 * keep_here // (planes * n)
    return (
        planes == 4
        and n == 8
        and w_query.shape[1] == HS
        and w_out.shape[0] == HS
        and w_in.shape[0] == 1
        and cap % 16 == 0
        and w_in.shape[2] % 256 == 0
    )


def body(
    tokens, kept, gain_attn, gain_ffn, w_query, w_key, w_value, w_out, expert_ids, w_in, w_back
):
    document = tokens[0]
    shard_len, width_model = document.shape
    ctx_count = lax.axis_size("ctx")
    dp_count = lax.axis_size("dp")
    if fits_whole(dp_count, ctx_count, kept.shape[1], w_query, w_out, w_in):
        ids = expert_ids.reshape(1, kept.shape[1])
        weights = (w_query, w_key, w_value, w_out, w_in, w_back)
        return whole(document, kept, ids, gain_attn, gain_ffn, *weights)[None]
    local = kept[0] - lax.axis_index("ctx") * shard_len
    keep_here = local.shape[0]
    positions = jnp.arange(shard_len, dtype=jnp.int32)
    picks = (local[:, None] == positions[None, :]).astype(jnp.bfloat16)
    rows = jnp.dot(picks, document, preferred_element_type=jnp.float32).astype(jnp.bfloat16)
    normed = rms_scale(rows, gain_attn).astype(jnp.bfloat16)
    mixed, w_out_all = attention(normed, w_query, w_key, w_value, w_out)
    inner_all = w_out.shape[0] * ctx_count
    attn = lax.dot_general(
        mixed.reshape(inner_all, keep_here),
        w_out_all.reshape(inner_all, width_model),
        (((0,), (0,)), ((), ())),
        preferred_element_type=jnp.float32,
    )
    first = rows.astype(jnp.float32) + attn
    ffn_in = rms_scale(first, gain_ffn).astype(jnp.bfloat16)
    expert_here = w_in.shape[0]
    owners = dp_count * ctx_count
    experts_all = expert_here * owners
    capacity = 2 * keep_here // experts_all
    labels = expert_ids[0, :, 0]
    order = jnp.arange(keep_here, dtype=jnp.int32)
    same = (labels[:, None] == labels[None, :]) & (order[None, :] < order[:, None])
    slots = jnp.sum(same.astype(jnp.int32), axis=1)
    place = labels * capacity + slots
    cells = jnp.arange(experts_all * capacity, dtype=jnp.int32)
    spots = (place[None, :] == cells[:, None]).astype(jnp.bfloat16)
    buffer = jnp.dot(spots, ffn_in, preferred_element_type=jnp.float32).astype(jnp.bfloat16)
    answers = experts(buffer, w_in, w_back, capacity)
    seats = (place[:, None] == cells[None, :]).astype(jnp.bfloat16)
    taken = jnp.dot(seats, answers, preferred_element_type=jnp.float32)
    second = (first + taken).astype(jnp.bfloat16)
    hits = positions[:, None] == local[None, :]
    fresh = jnp.dot(hits.astype(jnp.bfloat16), second, preferred_element_type=jnp.float32)
    touched = jnp.any(hits, axis=1, keepdims=True)
    blended = jnp.where(touched, fresh.astype(jnp.bfloat16), document)
    return blended[None]


def solution(mesh):
    return jax.shard_map(
        body,
        mesh=mesh,
        in_specs=(
            P("dp", "ctx", None),
            P("dp", "ctx"),
            P(),
            P(),
            P(None, "ctx"),
            P(None, "ctx"),
            P(None, "ctx"),
            P("ctx", None),
            P("dp", "ctx", None),
            P(("dp", "ctx"), None, None),
            P(("dp", "ctx"), None, None),
        ),
        out_specs=P("dp", "ctx", None),
        check_vma=False,
    )
```

```python
import functools
import math

import jax
import jax.numpy as jnp
from jax import lax
from jax.experimental import pallas as pl
from jax.experimental.pallas import tpu as pltpu
from jax.sharding import PartitionSpec as P

HS = 64
MESH = pl.DeviceIdType.MESH
LAST = (((1,), (1,)), ((), ()))

eps_norm = 1e-06
score_gain = 2.5


def rms_scale(values, gain):
    values = values.astype(jnp.float32)
    power = jnp.mean(values * values, axis=-1, keepdims=True)
    return values * lax.rsqrt(power + eps_norm) * gain


class Gather:
    def __init__(self, n, me, own, slots, send, recv):
        self.n, self.me, self.own, self.slots = n, me, own, slots
        self.send, self.recv = send, recv
        self.core, self.chip = me % 2, me // 2
        self.partner = me + 1 - 2 * self.core
        self.started = []

    def copy(self, ident, src, dst, target):
        return pltpu.make_async_remote_copy(
            src_ref=src,
            dst_ref=dst,
            send_sem=self.send.at[ident],
            recv_sem=self.recv.at[ident],
            device_id={"ctx": target},
            device_id_type=MESH,
        )

    def peers(self):
        chips = self.n // 2
        if chips == 4:
            x, y = self.chip % 2, self.chip // 2
            nx, ny = y * 2 + (1 - x), (1 - y) * 2 + x
            return [(nx, nx), (ny, ny)]
        return [
            ((self.chip + d) % chips, (self.chip + chips - d) % chips) for d in range(1, chips)
        ]

    def begin(self):
        own_to = self.slots.at[self.me]
        self.first = [
            self.copy(i, self.own, own_to, to * 2 + self.core)
            for i, (to, _) in enumerate(self.peers())
        ]
        self.base = len(self.first)
        self.twin = self.copy(self.base, self.own, own_to, self.partner)
        for c in self.first:
            c.start()
        self.twin.start()
        self.started = self.first + [self.twin]

    def relay(self):
        here, self.passed, self.late = [], [], []
        ident = self.base + 1
        peers = self.peers()
        square = self.n // 2 == 4
        half = self.own.shape[0] // 2
        for i, (_, source) in enumerate(peers):
            self.first[i].wait_recv()
            block = source * 2 + self.core
            here.append(block)
            if square:
                piece = self.slots.at[block, pl.ds(i * half, half)]
                c = self.copy(ident, piece, piece, peers[1 - i][0] * 2 + self.core)
                c.start()
                self.late.append(c)
                ident += 1
            c = self.copy(ident, self.slots.at[block], self.slots.at[block], self.partner)
            c.start()
            self.passed.append((source * 2 + 1 - self.core, c))
            ident += 1
        self.ident = ident
        self.started += self.late + [c for _, c in self.passed]
        return here

    def diagonal(self):
        if not self.late:
            return None
        block = (3 - self.chip) * 2 + self.core
        half = self.own.shape[0] // 2
        self.last = []
        for i, c in enumerate(self.late):
            c.wait_recv()
            piece = self.slots.at[block, pl.ds(i * half, half)]
            c = self.copy(self.ident + i, piece, piece, self.partner)
            c.start()
            self.last.append(c)
        self.started += self.last
        return block

    def final(self):
        if not self.late:
            return None
        for c in self.last:
            c.wait_recv()
        return (3 - self.chip) * 2 + 1 - self.core

    def drain(self):
        for c in self.started:
            c.wait_send()


def gather_copies(n):
    return 9 if n // 2 == 4 else 2 * (n // 2) - 1


def attention_kernel(
    n,
    heads,
    x_ref,
    wq_ref,
    wk_ref,
    wv_ref,
    wo_ref,
    mixed_ref,
    wo_all,
    x_all,
    q_all,
    k_all,
    v_all,
    stage,
    x_send,
    x_recv,
    o_send,
    o_recv,
    m_send,
    m_recv,
):
    me = lax.axis_index("ctx")
    rows = x_ref.shape[0]
    barrier = pltpu.get_barrier_semaphore()
    for d in range(1, n):
        pl.semaphore_signal(
            barrier, inc=1, device_id={"ctx": (me + d) % n}, device_id_type=MESH
        )
    pl.semaphore_wait(barrier, n - 1)

    def project(block, value):
        at = pl.ds(pl.multiple_of(block * rows, rows), rows)
        for h in range(heads):
            cols = pl.ds(h * HS, HS)
            q_all[h, at, :] = lax.dot_general(
                value, wq_ref[cols, :], LAST, preferred_element_type=jnp.float32
            ).astype(jnp.bfloat16)
            k_all[h, at, :] = lax.dot_general(
                value, wk_ref[cols, :], LAST, preferred_element_type=jnp.float32
            ).astype(jnp.bfloat16)
        v_all[:, at] = lax.dot_general(
            wv_ref[...], value, LAST, preferred_element_type=jnp.float32
        ).astype(jnp.bfloat16)

    g = Gather(n, me, x_ref, x_all, x_send, x_recv)
    o = Gather(n, me, wo_ref, wo_all, o_send, o_recv)
    g.begin()
    project(me, x_ref[...])
    wo_all[me] = wo_ref[...]
    g.twin.wait_recv()
    project(g.partner, x_all[g.partner])
    here = g.relay()
    o.begin()
    for block in here:
        project(block, x_all[block])
    for block, c in g.passed:
        c.wait_recv()
        project(block, x_all[block])
    block = g.diagonal()
    if block is not None:
        project(block, x_all[block])
    o.twin.wait_recv()
    o.relay()
    block = g.final()
    if block is not None:
        project(block, x_all[block])

    scale = score_gain / math.sqrt(HS) * math.log2(math.e)

    def send_block(step, target):
        return pltpu.make_async_remote_copy(
            src_ref=stage.at[step],
            dst_ref=mixed_ref.at[me],
            send_sem=m_send.at[step],
            recv_sem=m_recv.at[step],
            device_id={"ctx": target},
            device_id_type=MESH,
        )

    @pl.loop(0, n)
    def _(step):
        block = lax.rem(me + 1 + step, n)
        at = pl.ds(pl.multiple_of(block * rows, rows), rows)
        for h in range(heads):
            scores = lax.dot_general(
                k_all[h],
                q_all[h, at, :],
                LAST,
                preferred_element_type=jnp.float32,
            )
            top = jnp.max(scores, axis=0, keepdims=True)
            weights = jnp.exp2(scores * scale - top * scale)
            total = jnp.sum(weights, axis=0, keepdims=True)
            cols = pl.ds(h * HS, HS)
            mixed = jnp.dot(
                v_all[cols, :],
                weights.astype(jnp.bfloat16),
                preferred_element_type=jnp.float32,
            )
            stage[step, cols, :] = (mixed / total).astype(jnp.bfloat16)

        @pl.when(step < n - 1)
        def _():
            send_block(step, block).start()

    mixed_ref[me] = stage[n - 1]
    for _, c in o.passed:
        c.wait_recv()
    o.diagonal()
    o.final()

    @pl.loop(0, n - 1)
    def _(step):
        send_block(step, lax.rem(me + 1 + step, n)).wait()

    g.drain()
    o.drain()


def attention(normed, w_query, w_key, w_value, w_out):
    n = lax.axis_size("ctx")
    rows, width = normed.shape
    inner = w_query.shape[1]
    heads = inner // HS
    copies = gather_copies(n)
    vmem = pl.BlockSpec(memory_space=pltpu.VMEM)
    bf = jnp.bfloat16
    return pl.pallas_call(
        functools.partial(attention_kernel, n, heads),
        out_shape=(
            jax.ShapeDtypeStruct((n, inner, rows), bf),
            jax.ShapeDtypeStruct((n,) + w_out.shape, bf),
        ),
        in_specs=[vmem] * 5,
        out_specs=(vmem, vmem),
        scratch_shapes=[
            pltpu.VMEM((n, rows, width), bf),
            pltpu.VMEM((heads, n * rows, HS), bf),
            pltpu.VMEM((heads, n * rows, HS), bf),
            pltpu.VMEM((inner, n * rows), bf),
            pltpu.VMEM((n, inner, rows), bf),
            pltpu.SemaphoreType.DMA((copies,)),
            pltpu.SemaphoreType.DMA((copies,)),
            pltpu.SemaphoreType.DMA((copies,)),
            pltpu.SemaphoreType.DMA((copies,)),
            pltpu.SemaphoreType.DMA((n,)),
            pltpu.SemaphoreType.DMA((n,)),
        ],
        compiler_params=pltpu.CompilerParams(collective_id=0, has_side_effects=True),
        name="attention",
    )(normed, w_query.T, w_key.T, w_value.T, w_out)


def experts_plain(buffer, w_in, w_back, capacity):
    owners = lax.axis_size("dp") * lax.axis_size("ctx")
    expert_here, width = w_in.shape[0], buffer.shape[1]
    buffer = buffer.reshape(owners * expert_here, capacity, width)
    received = lax.all_to_all(buffer, ("dp", "ctx"), split_axis=0, concat_axis=0, tiled=True)
    grouped = received.reshape(owners, expert_here, capacity, width)
    hidden = jnp.einsum("sgid,gdf->sgif", grouped, w_in, preferred_element_type=jnp.float32)
    hidden = jnp.maximum(hidden, 0.0).astype(jnp.bfloat16)
    answer = jnp.einsum("sgif,gfd->sgid", hidden, w_back, preferred_element_type=jnp.float32)
    answered = answer.astype(jnp.bfloat16).reshape(owners * expert_here, capacity, width)
    back = lax.all_to_all(answered, ("dp", "ctx"), split_axis=0, concat_axis=0, tiled=True)
    return back.reshape(owners * expert_here * capacity, width)


def expert_kernel(
    planes,
    n,
    cap,
    buf_ref,
    w_in_hbm,
    w_back_hbm,
    back_ref,
    w_in_ref,
    w_back_ref,
    rows_ref,
    hidden_ref,
    answer_ref,
    w_sem,
    own_sem,
    d_send,
    d_recv,
    r_send,
    r_recv,
):
    dp, ctx = lax.axis_index("dp"), lax.axis_index("ctx")
    me = dp * n + ctx
    owners = planes * n
    loads = [
        pltpu.make_async_copy(w_in_hbm.at[0], w_in_ref, w_sem.at[0]),
        pltpu.make_async_copy(w_back_hbm.at[0], w_back_ref, w_sem.at[1]),
    ]
    for c in loads:
        c.start()
    barrier = pltpu.get_barrier_semaphore()

    @pl.loop(1, owners)
    def _(d):
        to = lax.rem(me + d, owners)
        pl.semaphore_signal(
            barrier, inc=1, device_id={"dp": to // n, "ctx": lax.rem(to, n)}, device_id_type=MESH
        )

    pl.semaphore_wait(barrier, owners - 1)

    def seat(index):
        return pl.ds(pl.multiple_of(index * cap, cap), cap)

    def at(shift):
        plane_shift, place_shift = shift // n, lax.rem(shift, n)
        half = planes // 2
        side = dp // half
        side = lax.rem(side + plane_shift // half, 2)
        plane = side * half + lax.rem(dp + plane_shift, half)
        return plane, lax.rem(ctx + place_shift, n)

    def dispatch(shift):
        plane, place = at(shift)
        return pltpu.make_async_remote_copy(
            src_ref=buf_ref.at[seat(plane * n + place)],
            dst_ref=rows_ref.at[seat(me)],
            send_sem=d_send.at[shift],
            recv_sem=d_recv.at[shift],
            device_id={"dp": plane, "ctx": place},
            device_id_type=MESH,
        )

    def give_back(shift):
        plane, place = at(shift)
        return pltpu.make_async_remote_copy(
            src_ref=answer_ref.at[seat(plane * n + place)],
            dst_ref=back_ref.at[seat(me)],
            send_sem=r_send.at[shift],
            recv_sem=r_recv.at[shift],
            device_id={"dp": plane, "ctx": place},
            device_id_type=MESH,
        )

    near = owners // 2

    @pl.loop(0, near)
    def _(shift):
        dispatch(near + shift).start()

        @pl.when(shift > 0)
        def _():
            dispatch(shift).start()

    own_in = pltpu.make_async_copy(buf_ref.at[seat(me)], rows_ref.at[seat(me)], own_sem.at[0])
    own_in.start()

    def run(first_row, count):
        inner = hidden_ref.shape[1]
        width = answer_ref.shape[1]
        take = pl.ds(pl.multiple_of(first_row, count), count)
        value = rows_ref[take, :]

        @pl.loop(0, inner // 256)
        def _(f):
            cols = pl.ds(pl.multiple_of(f * 256, 256), 256)
            hidden = jnp.dot(value, w_in_ref[:, cols], preferred_element_type=jnp.float32)
            hidden_ref[:, cols] = jnp.maximum(hidden, 0.0).astype(jnp.bfloat16)

        @pl.loop(0, width // 256)
        def _(f):
            cols = pl.ds(pl.multiple_of(f * 256, 256), 256)
            answer_ref[take, cols] = jnp.dot(
                hidden_ref[...], w_back_ref[:, cols], preferred_element_type=jnp.float32
            ).astype(jnp.bfloat16)

    half_rows = near * cap
    side = dp // (planes // 2)

    @pl.loop(1, near)
    def _(shift):
        dispatch(shift).wait_recv()

    own_in.wait()
    for c in loads:
        c.wait()

    @pl.loop(0, 2)
    def _(turn):
        @pl.when(turn == 1)
        def _():
            @pl.loop(near, owners)
            def _(shift):
                dispatch(shift).wait_recv()

        run(lax.rem(side + turn, 2) * half_rows, half_rows)

        @pl.loop(0, near)
        def _(shift):
            @pl.when(turn * near + shift > 0)
            def _():
                give_back(turn * near + shift).start()

    own_out = pltpu.make_async_copy(answer_ref.at[seat(me)], back_ref.at[seat(me)], own_sem.at[1])
    own_out.start()

    @pl.loop(1, owners)
    def _(shift):
        dispatch(shift).wait_send()
        give_back(shift).wait()

    own_out.wait()


def experts_fused(buffer, w_in, w_back, capacity):
    planes, n = lax.axis_size("dp"), lax.axis_size("ctx")
    owners = planes * n
    slots, width = buffer.shape
    inner = w_in.shape[2]
    bf = jnp.bfloat16
    vmem = pl.BlockSpec(memory_space=pltpu.VMEM)
    hbm = pl.BlockSpec(memory_space=pl.ANY)
    return pl.pallas_call(
        functools.partial(expert_kernel, planes, n, capacity),
        out_shape=jax.ShapeDtypeStruct((slots, width), bf),
        in_specs=[vmem, hbm, hbm],
        out_specs=vmem,
        scratch_shapes=[
            pltpu.VMEM(w_in.shape[1:], bf),
            pltpu.VMEM(w_back.shape[1:], bf),
            pltpu.VMEM((slots, width), bf),
            pltpu.VMEM((slots // 2, inner), bf),
            pltpu.VMEM((slots, width), bf),
            pltpu.SemaphoreType.DMA((2,)),
            pltpu.SemaphoreType.DMA((2,)),
            pltpu.SemaphoreType.DMA((owners,)),
            pltpu.SemaphoreType.DMA((owners,)),
            pltpu.SemaphoreType.DMA((owners,)),
            pltpu.SemaphoreType.DMA((owners,)),
        ],
        compiler_params=pltpu.CompilerParams(collective_id=1, has_side_effects=True),
        name="experts",
    )(buffer, w_in, w_back)


def experts(buffer, w_in, w_back, capacity):
    if capacity % 16 == 0 and w_in.shape[0] == 1:
        return experts_fused(buffer, w_in, w_back, capacity)
    return experts_plain(buffer, w_in, w_back, capacity)


def whole_kernel(
    planes,
    n,
    cap,
    kept_hbm,
    ids_hbm,
    gain_attn_hbm,
    gain_ffn_hbm,
    doc_hbm,
    wq_hbm,
    wk_hbm,
    wv_hbm,
    wo_hbm,
    w_in_hbm,
    w_back_hbm,
    out_ref,
    kept_ref,
    ids_ref,
    gain_attn_ref,
    gain_ffn_ref,
    doc_ref,
    w3_ref,
    wo_ref,
    w_in_ref,
    w_back_ref,
    place_all,
    x_all,
    q_all,
    k_all,
    v_all,
    sum_ref,
    top_ref,
    mix_ref,
    cells_ref,
    m_out,
    m_in,
    wo_all,
    r_out,
    r_in,
    first_ref,
    ffn_ref,
    hidden_ref,
    second_ref,
    back_ref,
    picks_ref,
    acc_ref,
    w_sem,
    p_send,
    p_recv,
    x_send,
    x_recv,
    o_send,
    o_recv,
    r_send,
    r_recv,
    m_send,
    m_recv,
    b_send,
    b_recv,
    ready,
):
    f32, bf = jnp.float32, jnp.bfloat16
    dp, me = lax.axis_index("dp"), lax.axis_index("ctx")
    owners = planes * n
    rows, width = x_all.shape[1], x_all.shape[2]
    shard = doc_ref.shape[0]
    inner = hidden_ref.shape[1]
    wide = 2 * HS
    share = n * cap
    pairs = n // 2

    loads = [
        pltpu.make_async_copy(ids_hbm, ids_ref, w_sem.at[8]),
        pltpu.make_async_copy(kept_hbm, kept_ref, w_sem.at[9]),
        pltpu.make_async_copy(doc_hbm, doc_ref, w_sem.at[0]),
        pltpu.make_async_copy(gain_attn_hbm, gain_attn_ref, w_sem.at[10]),
        pltpu.make_async_copy(gain_ffn_hbm, gain_ffn_ref, w_sem.at[11]),
        pltpu.make_async_copy(wq_hbm, w3_ref.at[pl.ds(0, HS)], w_sem.at[1]),
        pltpu.make_async_copy(wk_hbm, w3_ref.at[pl.ds(2 * HS, HS)], w_sem.at[2]),
        pltpu.make_async_copy(wv_hbm, w3_ref.at[pl.ds(4 * HS, HS)], w_sem.at[3]),
        pltpu.make_async_copy(wo_hbm, wo_ref, w_sem.at[5]),
        pltpu.make_async_copy(w_in_hbm.at[0], w_in_ref, w_sem.at[6]),
        pltpu.make_async_copy(w_back_hbm.at[0], w_back_ref, w_sem.at[7]),
    ]

    barrier = pltpu.get_barrier_semaphore()

    for d in range(1, n):
        pl.semaphore_signal(
            barrier, inc=1, device_id={"ctx": lax.rem(me + d, n)}, device_id_type=MESH
        )

    def column(sem):
        for d in range(1, planes):
            pl.semaphore_signal(
                sem, inc=1, device_id={"dp": lax.rem(dp + d, planes)}, device_id_type=MESH
            )

    column(barrier)
    for c in loads:
        c.start()

    def plane(g):
        high = lax.rem(dp // 2 + g // 2, 2)
        return high * 2 + lax.rem(dp + lax.rem(g, 2), 2)

    def one_hot(mask):
        return jnp.where(mask, 1.0, 0.0).astype(bf)

    def iota(shape, dim):
        return lax.broadcasted_iota(jnp.int32, shape, dim)

    loads[0].wait()
    ids = ids_ref[...]
    named = one_hot(iota((owners, rows), 0) == ids)
    earlier = one_hot(iota((rows, rows), 0) < iota((rows, rows), 1))
    before = jnp.dot(named, earlier, preferred_element_type=f32)
    slot = jnp.sum(named.astype(f32) * before, axis=0, keepdims=True).astype(jnp.int32)
    place_own = ids * cap + slot
    place_all[me] = jnp.broadcast_to(place_own, place_all.shape[1:])
    loads[1].wait()
    local = kept_ref[...] - me * shard
    picks = one_hot(iota((shard, rows), 0) == local)
    loads[2].wait()
    x_all[me] = lax.dot_general(
        picks, doc_ref[...], (((0,), (0,)), ((), ())), preferred_element_type=f32
    ).astype(bf)

    pl.semaphore_wait(barrier, n + planes - 2)
    column(ready)

    o = Gather(n, me, wo_ref, wo_all, o_send, o_recv)

    def bulk(ref, sends, recvs):
        return pltpu.make_async_remote_copy(
            src_ref=ref,
            dst_ref=ref,
            send_sem=sends,
            recv_sem=recvs,
            device_id={"ctx": o.partner},
            device_id_type=MESH,
        )

    def place_copy(d):
        return pltpu.make_async_remote_copy(
            src_ref=place_all.at[me],
            dst_ref=place_all.at[me],
            send_sem=p_send,
            recv_sem=p_recv,
            device_id={"ctx": lax.rem(me + d, n)},
            device_id_type=MESH,
        )

    for d in range(1, n):
        place_copy(d).start()

    core, chip, partner = o.core, o.chip, o.partner
    (near_x, _), (near_y, _) = o.peers()
    part, piece = rows // 2, rows // 4

    def send(ident, block, first, count, target):
        ref = x_all.at[block, pl.ds(pl.multiple_of(first, count), count)]
        return pltpu.make_async_remote_copy(
            src_ref=ref,
            dst_ref=ref,
            send_sem=x_send,
            recv_sem=x_recv.at[ident],
            device_id={"ctx": target},
            device_id_type=MESH,
        )

    to_x, to_y = near_x * 2 + core, near_y * 2 + core
    mine = core * part
    twin = send(0, me, (1 - core) * part, part, partner)
    rest = send(15, me, mine, part, partner)
    own, passed, relays, last = [], [], [], []
    for k in (0, 1):
        from_x, from_y, across = near_x * 2 + k, near_y * 2 + k, (3 - chip) * 2 + k
        own.append(
            (
                send(1 + k, chip * 2 + k, mine, part, to_x),
                send(3 + k, chip * 2 + k, mine, part, to_y),
            )
        )
        passed.append(
            (send(5 + k, from_x, mine, part, partner), send(7 + k, from_y, mine, part, partner))
        )
        relays.append(
            (
                send(9 + k, from_x, mine, piece, to_y),
                send(11 + k, from_y, mine + piece, piece, to_x),
            )
        )
        last.append(send(13 + k, across, mine, part, partner))
    twin.start()

    @pl.when(core == 0)
    def _():
        for c in own[0]:
            c.start()

    blank = jnp.zeros((HS, width), bf)
    for i in (1, 3, 5):
        w3_ref[pl.ds(i * HS, HS), :] = blank
    for c in loads[3:9]:
        c.wait()

    def row_copy(turn, block):
        return pltpu.make_async_remote_copy(
            src_ref=r_out.at[turn - 1, block],
            dst_ref=r_in.at[dp, block],
            send_sem=r_send.at[turn],
            recv_sem=r_recv.at[turn],
            device_id={"dp": plane(turn)},
            device_id_type=MESH,
        )

    def route(block, value):
        index = iota((planes * cap, rows), 0)
        turn, s = index // cap, index % cap
        high = (dp // 2 + turn // 2) % 2
        to = high * 2 + (dp + turn % 2) % 2
        cell = (to * n + me) * cap + s
        taken = jnp.dot(
            one_hot(cell == place_all[block][0:1, :]), value, preferred_element_type=f32
        ).astype(bf)
        r_in[dp, block] = taken[0:cap]
        for turn in (2, 3, 1):
            r_out[turn - 1, block] = taken[turn * cap : (turn + 1) * cap]
            row_copy(turn, block).start()

    def project(spot, value):
        at = pl.ds(pl.multiple_of(spot * rows, rows), rows)
        normed = rms_scale(value, gain_attn_ref[...]).astype(bf)
        three = lax.dot_general(normed, w3_ref[...], LAST, preferred_element_type=f32)
        q_all[at, :] = three[:, 0:wide].astype(bf)
        k_all[at, :] = three[:, wide : 2 * wide].astype(bf)
        lane = iota((rows, wide), 1)
        v_all[at, :] = jnp.where(lane < HS, three[:, 2 * wide : 3 * wide], 1.0).astype(bf)

    def take(block, spot):
        value = x_all[block]
        route(block, value)
        project(spot, value)

    scale = score_gain / math.sqrt(HS) * math.log2(math.e)

    def update(spot, spots, first, count, fresh):
        at = pl.ds(spot * rows, spots * rows)
        keys = pl.ds(first * rows, count * rows)
        scores = lax.dot_general(q_all[at, :], k_all[keys, :], LAST, preferred_element_type=f32)
        top = jnp.broadcast_to(
            jnp.max(scores, axis=1, keepdims=True), (spots * rows, wide)
        )
        if not fresh:
            known = top_ref[at, :]
            top = jnp.maximum(top, known)
        shift = jnp.concatenate([top * scale] * (count * rows // wide), axis=1)
        weights = jnp.exp2(scores * scale - shift)
        both = jnp.dot(weights.astype(bf), v_all[keys, :], preferred_element_type=f32)
        if not fresh:
            both = both + sum_ref[at, :] * jnp.exp2(known * scale - top * scale)
        sum_ref[at, :] = both
        top_ref[at, :] = top

    def match(chip):
        places = [place_all[2 * chip + side][0:1, :] for side in (0, 1)]
        cells_ref[chip] = one_hot(
            iota((owners * cap, 2 * rows), 0) == jnp.concatenate(places, axis=1)
        )

    twin.wait_recv()

    @pl.when(core == 1)
    def _():
        for c in own[0]:
            c.start()

    rest.start()
    for c in own[1]:
        c.start()
    take(me, core)
    for z in range(planes):
        cells = one_hot(iota((share, rows), 0) + z * share == place_own)
        picks_ref[z] = lax.dot_general(picks, cells, LAST, preferred_element_type=f32).astype(bf)
    wo_all[me] = wo_ref[...]
    places = bulk(place_all.at[pl.ds(0, n - 1)], p_send, p_recv)
    places.wait_recv()
    def mixed_copy(turn, d, j):
        to, c = plane(turn), lax.rem(me + d, n)
        lanes = pl.ds(pl.multiple_of(me * wide, wide), wide)
        return pltpu.make_async_remote_copy(
            src_ref=m_out.at[to * n + c, j],
            dst_ref=m_in.at[dp, j, :, lanes],
            send_sem=m_send.at[turn],
            recv_sem=m_recv.at[turn],
            device_id={"dp": to, "ctx": c},
            device_id_type=MESH,
        )

    def mixed_own(j):
        lanes = pl.ds(pl.multiple_of(me * wide, wide), wide)
        return pltpu.make_async_copy(
            m_out.at[dp * n + me, j], m_in.at[dp, j, :, lanes], m_recv.at[0]
        )

    def each(turn, act):
        @pl.loop(0, n)
        def _(d):
            @pl.when(turn + d > 0)
            def _():
                act(turn, d)

    def mixed_copies(turn, act):
        def some(turn, d):
            for j in range(pairs):
                act(mixed_copy(turn, d, j))

        each(turn, some)

    def finish(chip, spots):
        for side, spot in enumerate(spots):
            both = sum_ref[pl.ds(spot * rows, rows), :]
            mixed = jnp.where(iota((rows, wide), 1) < HS, both / pltpu.roll(both, HS, 1), 0.0)
            if side:
                mixed = pltpu.roll(mixed, HS, 1)
            mix_ref[pl.ds(side * rows, rows), :] = mixed.astype(bf)
        spread = jnp.dot(cells_ref[chip], mix_ref[...], preferred_element_type=f32).astype(bf)
        m_out[:, chip] = spread.reshape(owners, cap, wide)
        each(2, lambda turn, d: mixed_copy(turn, d, chip).start())
        each(3, lambda turn, d: mixed_copy(turn, d, chip).start())

    rest.wait_recv()
    take(partner, 1 - core)
    update(0, 2, 0, 2, True)
    for at in range(pairs):
        match(at)
    for c, p, r in zip(own[0], passed[0], relays[0]):
        c.wait_recv()
        p.start()
        r.start()
    for i, near in enumerate((near_x, near_y)):
        passed[0][i].wait_recv()
        take(near * 2, 2 + i)
    update(0, 2, 2, 2, False)
    update(2, 2, 0, 4, True)
    for c, p, r in zip(own[1], passed[1], relays[1]):
        c.wait_recv()
        p.start()
        r.start()
    for i, near in enumerate((near_x, near_y)):
        passed[1][i].wait_recv()
        take(near * 2 + 1, 4 + i)
    update(0, 4, 4, 2, False)
    for r in relays[0]:
        r.wait_recv()
    last[0].start()
    o.begin()
    update(4, 2, 0, 6, True)
    for r in relays[1]:
        r.wait_recv()
    last[1].start()
    for k in (0, 1):
        last[k].wait_recv()
        take((3 - chip) * 2 + k, 6 + k)
    update(0, 6, 6, 2, False)
    o.twin.wait_recv()
    o.relay()
    pl.semaphore_wait(ready, planes - 1)
    finish(chip, (0, 1))
    finish(near_x, (2, 4))
    finish(near_y, (3, 5))
    update(6, 2, 0, 8, True)
    finish(3 - chip, (6, 7))
    o.diagonal()

    inside = lax.rem((dp + 1) // 2, 2)

    def seat(t):
        return lax.rem(t + 2 * inside, planes)

    def back_copy(turn, d):
        to, c = plane(turn), lax.rem(me + d, n)
        return pltpu.make_async_remote_copy(
            src_ref=second_ref.at[to, lax.rem(c, 2), c // 2],
            dst_ref=back_ref.at[dp, me],
            send_sem=b_send.at[turn],
            recv_sem=b_recv.at[turn],
            device_id={"dp": to, "ctx": c},
            device_id_type=MESH,
        )

    mixed_copies(0, lambda c: c.start())
    mixed_copies(1, lambda c: c.start())
    for j in range(pairs):
        mixed_own(j).start()
    touched = jnp.zeros((shard, 1), f32)
    for z in range(planes):
        touched = touched + jnp.sum(picks_ref[z].astype(f32), axis=1, keepdims=True)
    acc_ref[...] = jnp.where(touched > 0.5, 0.0, doc_ref[...].astype(f32))
    for c in loads[9:]:
        c.wait()
    for _, c in o.passed:
        c.wait_recv()
    o.final()

    half = pairs * cap

    @pl.loop(0, planes)
    def _(t):
        turn = seat(t)
        source = plane(turn)
        bulk(m_in.at[source], m_send.at[turn], m_recv.at[turn]).wait_recv()

        @pl.when(turn > 0)
        def _():
            bulk(r_in.at[source], r_send.at[turn], r_recv.at[turn]).wait_recv()

        mixed = m_in[source].reshape(half, n * wide)
        heads = [mixed[:, h * wide : (h + 1) * wide] for h in range(n)]
        low = jnp.concatenate([h[:, :HS] for h in heads], axis=1)
        high = jnp.concatenate([h[:, HS:] for h in heads], axis=1)
        base = [r_in[source, 2 * j + side] for side in (0, 1) for j in range(pairs)]
        first_ref[...] = jnp.concatenate(base, axis=0).astype(f32) + jnp.dot(
            jnp.concatenate([low, high], axis=0),
            wo_all[...].reshape(n * HS, width),
            preferred_element_type=f32,
        )
        ffn_ref[...] = rms_scale(first_ref[...], gain_ffn_ref[...]).astype(bf)
        for f in range(0, inner, 256):
            hidden = jnp.dot(ffn_ref[...], w_in_ref[:, f : f + 256], preferred_element_type=f32)
            hidden_ref[:, f : f + 256] = jnp.maximum(hidden, 0.0).astype(bf)
        for f in range(0, width, 256):
            answer = jnp.dot(
                hidden_ref[...], w_back_ref[:, f : f + 256], preferred_element_type=f32
            ).astype(bf)
            second = (first_ref[:, f : f + 256] + answer.astype(f32)).astype(bf)
            second_ref[source, :, :, :, f : f + 256] = second.reshape(2, pairs, cap, 256)
        each(turn, lambda turn, d: back_copy(turn, d).start())

    pltpu.make_async_copy(
        second_ref.at[dp, lax.rem(me, 2), me // 2], back_ref.at[dp, me], b_recv.at[0]
    ).start()

    def returned(turn):
        source = plane(turn)
        bulk(back_ref.at[source], b_send.at[turn], b_recv.at[turn]).wait_recv()
        return acc_ref[...] + jnp.dot(
            picks_ref[source], back_ref[source].reshape(share, width), preferred_element_type=f32
        )

    for turn in (0, 1, 2):
        acc_ref[...] = returned(turn)

    out_ref[...] = returned(3).astype(bf)

    places.wait_send()

    for turn in range(planes):
        count = n - (turn == 0)
        bulk(m_out.at[pl.ds(0, count)], m_send.at[turn], m_recv.at[turn]).wait_send()
        bulk(back_ref.at[0, pl.ds(0, count)], b_send.at[turn], b_recv.at[turn]).wait_send()
        if turn:
            bulk(r_in.at[0], r_send.at[turn], r_recv.at[turn]).wait_send()
    bulk(x_all.at[pl.ds(0, n - 1)], x_send, x_recv.at[0]).wait_send()
    o.drain()


def whole(document, kept, ids, gain_attn, gain_ffn, w_query, w_key, w_value, w_out, w_in, w_back):
    planes, n = lax.axis_size("dp"), lax.axis_size("ctx")
    owners = planes * n
    shard, width = document.shape
    rows = kept.shape[1]
    cap = 2 * rows // owners
    inner = w_in.shape[2]
    pairs = n // 2
    wide = 2 * HS
    half = pairs * cap
    bf, f32 = jnp.bfloat16, jnp.float32
    vmem = pl.BlockSpec(memory_space=pltpu.VMEM)
    hbm = pl.BlockSpec(memory_space=pltpu.HBM)
    sems = pltpu.SemaphoreType.DMA
    copies = gather_copies(n)
    grant = 42 * 1024 * 1024
    operands = (
        kept,
        ids,
        gain_attn.reshape(1, width),
        gain_ffn.reshape(1, width),
        document,
        w_query.T,
        w_key.T,
        w_value.T,
        w_out,
        w_in,
        w_back,
    )
    return pl.pallas_call(
        functools.partial(whole_kernel, planes, n, cap),
        out_shape=jax.ShapeDtypeStruct((shard, width), bf),
        in_specs=[hbm] * 11,
        out_specs=vmem,
        scratch_shapes=[
            pltpu.VMEM((1, rows), jnp.int32),
            pltpu.VMEM((1, rows), jnp.int32),
            pltpu.VMEM((1, width), f32),
            pltpu.VMEM((1, width), f32),
            pltpu.VMEM((shard, width), bf),
            pltpu.VMEM((6 * HS, width), bf),
            pltpu.VMEM(w_out.shape, bf),
            pltpu.VMEM(w_in.shape[1:], bf),
            pltpu.VMEM(w_back.shape[1:], bf),
            pltpu.VMEM((n, 8, rows), jnp.int32),
            pltpu.VMEM((n, rows, width), bf),
            pltpu.VMEM((n * rows, wide), bf),
            pltpu.VMEM((n * rows, wide), bf),
            pltpu.VMEM((n * rows, wide), bf),
            pltpu.VMEM((n * rows, wide), f32),
            pltpu.VMEM((n * rows, wide), f32),
            pltpu.VMEM((2 * rows, wide), bf),
            pltpu.VMEM((n // 2, owners * cap, 2 * rows), bf),
            pltpu.VMEM((owners, pairs, cap, wide), bf),
            pltpu.VMEM((planes, pairs, cap, n * wide), bf),
            pltpu.VMEM((n,) + w_out.shape, bf),
            pltpu.VMEM((planes - 1, n, cap, width), bf),
            pltpu.VMEM((planes, n, cap, width), bf),
            pltpu.VMEM((2 * half, width), f32),
            pltpu.VMEM((2 * half, width), bf),
            pltpu.VMEM((2 * half, inner), bf),
            pltpu.VMEM((planes, 2, pairs, cap, width), bf),
            pltpu.VMEM((planes, n, cap, width), bf),
            pltpu.VMEM((planes, shard, n * cap), bf),
            pltpu.VMEM((shard, width), f32),
            sems((12,)),
            sems(()),
            sems(()),
            sems(()),
            sems((16,)),
            sems((copies,)),
            sems((copies,)),
            sems((planes,)),
            sems((planes,)),
            sems((planes,)),
            sems((planes,)),
            sems((planes,)),
            sems((planes,)),
            pltpu.SemaphoreType.REGULAR,
        ],
        compiler_params=pltpu.CompilerParams(
            collective_id=2, has_side_effects=True, vmem_limit_bytes=grant
        ),
        name="whole",
    )(*[pltpu.with_memory_space_constraint(a, pltpu.HBM) for a in operands])


def fits_whole(planes, n, keep_here, w_query, w_out, w_in):
    cap = 2 * keep_here // (planes * n)
    return (
        planes == 4
        and n == 8
        and w_query.shape[1] == HS
        and w_out.shape[0] == HS
        and w_in.shape[0] == 1
        and cap % 16 == 0
        and w_in.shape[2] % 256 == 0
    )


def body(
    tokens, kept, gain_attn, gain_ffn, w_query, w_key, w_value, w_out, expert_ids, w_in, w_back
):
    document = tokens[0]
    shard_len, width_model = document.shape
    ctx_count = lax.axis_size("ctx")
    dp_count = lax.axis_size("dp")
    if fits_whole(dp_count, ctx_count, kept.shape[1], w_query, w_out, w_in):
        ids = expert_ids.reshape(1, kept.shape[1])
        weights = (w_query, w_key, w_value, w_out, w_in, w_back)
        return whole(document, kept, ids, gain_attn, gain_ffn, *weights)[None]
    local = kept[0] - lax.axis_index("ctx") * shard_len
    keep_here = local.shape[0]
    positions = jnp.arange(shard_len, dtype=jnp.int32)
    picks = (local[:, None] == positions[None, :]).astype(jnp.bfloat16)
    rows = jnp.dot(picks, document, preferred_element_type=jnp.float32).astype(jnp.bfloat16)
    normed = rms_scale(rows, gain_attn).astype(jnp.bfloat16)
    mixed, w_out_all = attention(normed, w_query, w_key, w_value, w_out)
    inner_all = w_out.shape[0] * ctx_count
    attn = lax.dot_general(
        mixed.reshape(inner_all, keep_here),
        w_out_all.reshape(inner_all, width_model),
        (((0,), (0,)), ((), ())),
        preferred_element_type=jnp.float32,
    )
    first = rows.astype(jnp.float32) + attn
    ffn_in = rms_scale(first, gain_ffn).astype(jnp.bfloat16)
    expert_here = w_in.shape[0]
    owners = dp_count * ctx_count
    experts_all = expert_here * owners
    capacity = 2 * keep_here // experts_all
    labels = expert_ids[0, :, 0]
    order = jnp.arange(keep_here, dtype=jnp.int32)
    same = (labels[:, None] == labels[None, :]) & (order[None, :] < order[:, None])
    slots = jnp.sum(same.astype(jnp.int32), axis=1)
    place = labels * capacity + slots
    cells = jnp.arange(experts_all * capacity, dtype=jnp.int32)
    spots = (place[None, :] == cells[:, None]).astype(jnp.bfloat16)
    buffer = jnp.dot(spots, ffn_in, preferred_element_type=jnp.float32).astype(jnp.bfloat16)
    answers = experts(buffer, w_in, w_back, capacity)
    seats = (place[:, None] == cells[None, :]).astype(jnp.bfloat16)
    taken = jnp.dot(seats, answers, preferred_element_type=jnp.float32)
    second = (first + taken).astype(jnp.bfloat16)
    hits = positions[:, None] == local[None, :]
    fresh = jnp.dot(hits.astype(jnp.bfloat16), second, preferred_element_type=jnp.float32)
    touched = jnp.any(hits, axis=1, keepdims=True)
    blended = jnp.where(touched, fresh.astype(jnp.bfloat16), document)
    return blended[None]


def solution(mesh):
    return jax.shard_map(
        body,
        mesh=mesh,
        in_specs=(
            P("dp", "ctx", None),
            P("dp", "ctx"),
            P(),
            P(),
            P(None, "ctx"),
            P(None, "ctx"),
            P(None, "ctx"),
            P("ctx", None),
            P("dp", "ctx", None),
            P(("dp", "ctx"), None, None),
            P(("dp", "ctx"), None, None),
        ),
        out_specs=P("dp", "ctx", None),
        check_vma=False,
    )
```

```python
import functools
import math

import jax
import jax.numpy as jnp
from jax import lax
from jax.experimental import pallas as pl
from jax.experimental.pallas import tpu as pltpu
from jax.sharding import PartitionSpec as P

HS = 64
MESH = pl.DeviceIdType.MESH
LAST = (((1,), (1,)), ((), ()))

eps_norm = 1e-06
score_gain = 2.5


def rms_scale(values, gain):
    values = values.astype(jnp.float32)
    power = jnp.mean(values * values, axis=-1, keepdims=True)
    return values * lax.rsqrt(power + eps_norm) * gain


class Gather:
    def __init__(self, n, me, own, slots, send, recv):
        self.n, self.me, self.own, self.slots = n, me, own, slots
        self.send, self.recv = send, recv
        self.core, self.chip = me % 2, me // 2
        self.partner = me + 1 - 2 * self.core
        self.started = []

    def copy(self, ident, src, dst, target):
        return pltpu.make_async_remote_copy(
            src_ref=src,
            dst_ref=dst,
            send_sem=self.send.at[ident],
            recv_sem=self.recv.at[ident],
            device_id={"ctx": target},
            device_id_type=MESH,
        )

    def peers(self):
        chips = self.n // 2
        if chips == 4:
            x, y = self.chip % 2, self.chip // 2
            nx, ny = y * 2 + (1 - x), (1 - y) * 2 + x
            return [(nx, nx), (ny, ny)]
        return [
            ((self.chip + d) % chips, (self.chip + chips - d) % chips) for d in range(1, chips)
        ]

    def begin(self):
        own_to = self.slots.at[self.me]
        self.first = [
            self.copy(i, self.own, own_to, to * 2 + self.core)
            for i, (to, _) in enumerate(self.peers())
        ]
        self.base = len(self.first)
        self.twin = self.copy(self.base, self.own, own_to, self.partner)
        for c in self.first:
            c.start()
        self.twin.start()
        self.started = self.first + [self.twin]

    def relay(self):
        here, self.passed, self.late = [], [], []
        ident = self.base + 1
        peers = self.peers()
        square = self.n // 2 == 4
        half = self.own.shape[0] // 2
        for i, (_, source) in enumerate(peers):
            self.first[i].wait_recv()
            block = source * 2 + self.core
            here.append(block)
            if square:
                piece = self.slots.at[block, pl.ds(i * half, half)]
                c = self.copy(ident, piece, piece, peers[1 - i][0] * 2 + self.core)
                c.start()
                self.late.append(c)
                ident += 1
            c = self.copy(ident, self.slots.at[block], self.slots.at[block], self.partner)
            c.start()
            self.passed.append((source * 2 + 1 - self.core, c))
            ident += 1
        self.ident = ident
        self.started += self.late + [c for _, c in self.passed]
        return here

    def diagonal(self):
        if not self.late:
            return None
        block = (3 - self.chip) * 2 + self.core
        half = self.own.shape[0] // 2
        self.last = []
        for i, c in enumerate(self.late):
            c.wait_recv()
            piece = self.slots.at[block, pl.ds(i * half, half)]
            c = self.copy(self.ident + i, piece, piece, self.partner)
            c.start()
            self.last.append(c)
        self.started += self.last
        return block

    def final(self):
        if not self.late:
            return None
        for c in self.last:
            c.wait_recv()
        return (3 - self.chip) * 2 + 1 - self.core

    def drain(self):
        for c in self.started:
            c.wait_send()


def gather_copies(n):
    return 9 if n // 2 == 4 else 2 * (n // 2) - 1


def attention_kernel(
    n,
    heads,
    x_ref,
    wq_ref,
    wk_ref,
    wv_ref,
    wo_ref,
    mixed_ref,
    wo_all,
    x_all,
    q_all,
    k_all,
    v_all,
    stage,
    x_send,
    x_recv,
    o_send,
    o_recv,
    m_send,
    m_recv,
):
    me = lax.axis_index("ctx")
    rows = x_ref.shape[0]
    barrier = pltpu.get_barrier_semaphore()
    for d in range(1, n):
        pl.semaphore_signal(
            barrier, inc=1, device_id={"ctx": (me + d) % n}, device_id_type=MESH
        )
    pl.semaphore_wait(barrier, n - 1)

    def project(block, value):
        at = pl.ds(pl.multiple_of(block * rows, rows), rows)
        for h in range(heads):
            cols = pl.ds(h * HS, HS)
            q_all[h, at, :] = lax.dot_general(
                value, wq_ref[cols, :], LAST, preferred_element_type=jnp.float32
            ).astype(jnp.bfloat16)
            k_all[h, at, :] = lax.dot_general(
                value, wk_ref[cols, :], LAST, preferred_element_type=jnp.float32
            ).astype(jnp.bfloat16)
        v_all[:, at] = lax.dot_general(
            wv_ref[...], value, LAST, preferred_element_type=jnp.float32
        ).astype(jnp.bfloat16)

    g = Gather(n, me, x_ref, x_all, x_send, x_recv)
    o = Gather(n, me, wo_ref, wo_all, o_send, o_recv)
    g.begin()
    project(me, x_ref[...])
    wo_all[me] = wo_ref[...]
    g.twin.wait_recv()
    project(g.partner, x_all[g.partner])
    here = g.relay()
    o.begin()
    for block in here:
        project(block, x_all[block])
    for block, c in g.passed:
        c.wait_recv()
        project(block, x_all[block])
    block = g.diagonal()
    if block is not None:
        project(block, x_all[block])
    o.twin.wait_recv()
    o.relay()
    block = g.final()
    if block is not None:
        project(block, x_all[block])

    scale = score_gain / math.sqrt(HS) * math.log2(math.e)

    def send_block(step, target):
        return pltpu.make_async_remote_copy(
            src_ref=stage.at[step],
            dst_ref=mixed_ref.at[me],
            send_sem=m_send.at[step],
            recv_sem=m_recv.at[step],
            device_id={"ctx": target},
            device_id_type=MESH,
        )

    @pl.loop(0, n)
    def _(step):
        block = lax.rem(me + 1 + step, n)
        at = pl.ds(pl.multiple_of(block * rows, rows), rows)
        for h in range(heads):
            scores = lax.dot_general(
                k_all[h],
                q_all[h, at, :],
                LAST,
                preferred_element_type=jnp.float32,
            )
            top = jnp.max(scores, axis=0, keepdims=True)
            weights = jnp.exp2(scores * scale - top * scale)
            total = jnp.sum(weights, axis=0, keepdims=True)
            cols = pl.ds(h * HS, HS)
            mixed = jnp.dot(
                v_all[cols, :],
                weights.astype(jnp.bfloat16),
                preferred_element_type=jnp.float32,
            )
            stage[step, cols, :] = (mixed / total).astype(jnp.bfloat16)

        @pl.when(step < n - 1)
        def _():
            send_block(step, block).start()

    mixed_ref[me] = stage[n - 1]
    for _, c in o.passed:
        c.wait_recv()
    o.diagonal()
    o.final()

    @pl.loop(0, n - 1)
    def _(step):
        send_block(step, lax.rem(me + 1 + step, n)).wait()

    g.drain()
    o.drain()


def attention(normed, w_query, w_key, w_value, w_out):
    n = lax.axis_size("ctx")
    rows, width = normed.shape
    inner = w_query.shape[1]
    heads = inner // HS
    copies = gather_copies(n)
    vmem = pl.BlockSpec(memory_space=pltpu.VMEM)
    bf = jnp.bfloat16
    return pl.pallas_call(
        functools.partial(attention_kernel, n, heads),
        out_shape=(
            jax.ShapeDtypeStruct((n, inner, rows), bf),
            jax.ShapeDtypeStruct((n,) + w_out.shape, bf),
        ),
        in_specs=[vmem] * 5,
        out_specs=(vmem, vmem),
        scratch_shapes=[
            pltpu.VMEM((n, rows, width), bf),
            pltpu.VMEM((heads, n * rows, HS), bf),
            pltpu.VMEM((heads, n * rows, HS), bf),
            pltpu.VMEM((inner, n * rows), bf),
            pltpu.VMEM((n, inner, rows), bf),
            pltpu.SemaphoreType.DMA((copies,)),
            pltpu.SemaphoreType.DMA((copies,)),
            pltpu.SemaphoreType.DMA((copies,)),
            pltpu.SemaphoreType.DMA((copies,)),
            pltpu.SemaphoreType.DMA((n,)),
            pltpu.SemaphoreType.DMA((n,)),
        ],
        compiler_params=pltpu.CompilerParams(collective_id=0, has_side_effects=True),
        name="attention",
    )(normed, w_query.T, w_key.T, w_value.T, w_out)


def experts_plain(buffer, w_in, w_back, capacity):
    owners = lax.axis_size("dp") * lax.axis_size("ctx")
    expert_here, width = w_in.shape[0], buffer.shape[1]
    buffer = buffer.reshape(owners * expert_here, capacity, width)
    received = lax.all_to_all(buffer, ("dp", "ctx"), split_axis=0, concat_axis=0, tiled=True)
    grouped = received.reshape(owners, expert_here, capacity, width)
    hidden = jnp.einsum("sgid,gdf->sgif", grouped, w_in, preferred_element_type=jnp.float32)
    hidden = jnp.maximum(hidden, 0.0).astype(jnp.bfloat16)
    answer = jnp.einsum("sgif,gfd->sgid", hidden, w_back, preferred_element_type=jnp.float32)
    answered = answer.astype(jnp.bfloat16).reshape(owners * expert_here, capacity, width)
    back = lax.all_to_all(answered, ("dp", "ctx"), split_axis=0, concat_axis=0, tiled=True)
    return back.reshape(owners * expert_here * capacity, width)


def expert_kernel(
    planes,
    n,
    cap,
    buf_ref,
    w_in_hbm,
    w_back_hbm,
    back_ref,
    w_in_ref,
    w_back_ref,
    rows_ref,
    hidden_ref,
    answer_ref,
    w_sem,
    own_sem,
    d_send,
    d_recv,
    r_send,
    r_recv,
):
    dp, ctx = lax.axis_index("dp"), lax.axis_index("ctx")
    me = dp * n + ctx
    owners = planes * n
    loads = [
        pltpu.make_async_copy(w_in_hbm.at[0], w_in_ref, w_sem.at[0]),
        pltpu.make_async_copy(w_back_hbm.at[0], w_back_ref, w_sem.at[1]),
    ]
    for c in loads:
        c.start()
    barrier = pltpu.get_barrier_semaphore()

    @pl.loop(1, owners)
    def _(d):
        to = lax.rem(me + d, owners)
        pl.semaphore_signal(
            barrier, inc=1, device_id={"dp": to // n, "ctx": lax.rem(to, n)}, device_id_type=MESH
        )

    pl.semaphore_wait(barrier, owners - 1)

    def seat(index):
        return pl.ds(pl.multiple_of(index * cap, cap), cap)

    def at(shift):
        plane_shift, place_shift = shift // n, lax.rem(shift, n)
        half = planes // 2
        side = dp // half
        side = lax.rem(side + plane_shift // half, 2)
        plane = side * half + lax.rem(dp + plane_shift, half)
        return plane, lax.rem(ctx + place_shift, n)

    def dispatch(shift):
        plane, place = at(shift)
        return pltpu.make_async_remote_copy(
            src_ref=buf_ref.at[seat(plane * n + place)],
            dst_ref=rows_ref.at[seat(me)],
            send_sem=d_send.at[shift],
            recv_sem=d_recv.at[shift],
            device_id={"dp": plane, "ctx": place},
            device_id_type=MESH,
        )

    def give_back(shift):
        plane, place = at(shift)
        return pltpu.make_async_remote_copy(
            src_ref=answer_ref.at[seat(plane * n + place)],
            dst_ref=back_ref.at[seat(me)],
            send_sem=r_send.at[shift],
            recv_sem=r_recv.at[shift],
            device_id={"dp": plane, "ctx": place},
            device_id_type=MESH,
        )

    near = owners // 2

    @pl.loop(0, near)
    def _(shift):
        dispatch(near + shift).start()

        @pl.when(shift > 0)
        def _():
            dispatch(shift).start()

    own_in = pltpu.make_async_copy(buf_ref.at[seat(me)], rows_ref.at[seat(me)], own_sem.at[0])
    own_in.start()

    def run(first_row, count):
        inner = hidden_ref.shape[1]
        width = answer_ref.shape[1]
        take = pl.ds(pl.multiple_of(first_row, count), count)
        value = rows_ref[take, :]

        @pl.loop(0, inner // 256)
        def _(f):
            cols = pl.ds(pl.multiple_of(f * 256, 256), 256)
            hidden = jnp.dot(value, w_in_ref[:, cols], preferred_element_type=jnp.float32)
            hidden_ref[:, cols] = jnp.maximum(hidden, 0.0).astype(jnp.bfloat16)

        @pl.loop(0, width // 256)
        def _(f):
            cols = pl.ds(pl.multiple_of(f * 256, 256), 256)
            answer_ref[take, cols] = jnp.dot(
                hidden_ref[...], w_back_ref[:, cols], preferred_element_type=jnp.float32
            ).astype(jnp.bfloat16)

    half_rows = near * cap
    side = dp // (planes // 2)

    @pl.loop(1, near)
    def _(shift):
        dispatch(shift).wait_recv()

    own_in.wait()
    for c in loads:
        c.wait()

    @pl.loop(0, 2)
    def _(turn):
        @pl.when(turn == 1)
        def _():
            @pl.loop(near, owners)
            def _(shift):
                dispatch(shift).wait_recv()

        run(lax.rem(side + turn, 2) * half_rows, half_rows)

        @pl.loop(0, near)
        def _(shift):
            @pl.when(turn * near + shift > 0)
            def _():
                give_back(turn * near + shift).start()

    own_out = pltpu.make_async_copy(answer_ref.at[seat(me)], back_ref.at[seat(me)], own_sem.at[1])
    own_out.start()

    @pl.loop(1, owners)
    def _(shift):
        dispatch(shift).wait_send()
        give_back(shift).wait()

    own_out.wait()


def experts_fused(buffer, w_in, w_back, capacity):
    planes, n = lax.axis_size("dp"), lax.axis_size("ctx")
    owners = planes * n
    slots, width = buffer.shape
    inner = w_in.shape[2]
    bf = jnp.bfloat16
    vmem = pl.BlockSpec(memory_space=pltpu.VMEM)
    hbm = pl.BlockSpec(memory_space=pl.ANY)
    return pl.pallas_call(
        functools.partial(expert_kernel, planes, n, capacity),
        out_shape=jax.ShapeDtypeStruct((slots, width), bf),
        in_specs=[vmem, hbm, hbm],
        out_specs=vmem,
        scratch_shapes=[
            pltpu.VMEM(w_in.shape[1:], bf),
            pltpu.VMEM(w_back.shape[1:], bf),
            pltpu.VMEM((slots, width), bf),
            pltpu.VMEM((slots // 2, inner), bf),
            pltpu.VMEM((slots, width), bf),
            pltpu.SemaphoreType.DMA((2,)),
            pltpu.SemaphoreType.DMA((2,)),
            pltpu.SemaphoreType.DMA((owners,)),
            pltpu.SemaphoreType.DMA((owners,)),
            pltpu.SemaphoreType.DMA((owners,)),
            pltpu.SemaphoreType.DMA((owners,)),
        ],
        compiler_params=pltpu.CompilerParams(collective_id=1, has_side_effects=True),
        name="experts",
    )(buffer, w_in, w_back)


def experts(buffer, w_in, w_back, capacity):
    if capacity % 16 == 0 and w_in.shape[0] == 1:
        return experts_fused(buffer, w_in, w_back, capacity)
    return experts_plain(buffer, w_in, w_back, capacity)


def whole_kernel(
    planes,
    n,
    cap,
    kept_hbm,
    ids_hbm,
    gain_attn_hbm,
    gain_ffn_hbm,
    doc_hbm,
    wq_hbm,
    wk_hbm,
    wv_hbm,
    wo_hbm,
    w_in_hbm,
    w_back_hbm,
    out_ref,
    kept_ref,
    ids_ref,
    gain_attn_ref,
    gain_ffn_ref,
    doc_ref,
    w3_ref,
    wo_ref,
    w_in_ref,
    w_back_ref,
    place_all,
    x_all,
    q_all,
    k_all,
    v_all,
    sum_ref,
    top_ref,
    mix_ref,
    cells_ref,
    m_out,
    m_in,
    wo_all,
    r_out,
    r_in,
    first_ref,
    ffn_ref,
    hidden_ref,
    second_ref,
    back_ref,
    picks_ref,
    acc_ref,
    w_sem,
    p_send,
    p_recv,
    x_send,
    x_recv,
    o_send,
    o_recv,
    r_send,
    r_recv,
    m_send,
    m_recv,
    b_send,
    b_recv,
    ready,
):
    f32, bf = jnp.float32, jnp.bfloat16
    dp, me = lax.axis_index("dp"), lax.axis_index("ctx")
    owners = planes * n
    rows, width = x_all.shape[1], x_all.shape[2]
    shard = doc_ref.shape[0]
    inner = hidden_ref.shape[1]
    wide = 2 * HS
    share = n * cap
    pairs = n // 2

    loads = [
        pltpu.make_async_copy(ids_hbm, ids_ref, w_sem.at[8]),
        pltpu.make_async_copy(kept_hbm, kept_ref, w_sem.at[9]),
        pltpu.make_async_copy(doc_hbm, doc_ref, w_sem.at[0]),
        pltpu.make_async_copy(gain_attn_hbm, gain_attn_ref, w_sem.at[10]),
        pltpu.make_async_copy(gain_ffn_hbm, gain_ffn_ref, w_sem.at[11]),
        pltpu.make_async_copy(wq_hbm, w3_ref.at[pl.ds(0, HS)], w_sem.at[1]),
        pltpu.make_async_copy(wk_hbm, w3_ref.at[pl.ds(2 * HS, HS)], w_sem.at[2]),
        pltpu.make_async_copy(wv_hbm, w3_ref.at[pl.ds(4 * HS, HS)], w_sem.at[3]),
        pltpu.make_async_copy(wo_hbm, wo_ref, w_sem.at[5]),
        pltpu.make_async_copy(w_in_hbm.at[0], w_in_ref, w_sem.at[6]),
        pltpu.make_async_copy(w_back_hbm.at[0], w_back_ref, w_sem.at[7]),
    ]

    barrier = pltpu.get_barrier_semaphore()

    for d in range(1, n):
        pl.semaphore_signal(
            barrier, inc=1, device_id={"ctx": lax.rem(me + d, n)}, device_id_type=MESH
        )

    def column(sem):
        for d in range(1, planes):
            pl.semaphore_signal(
                sem, inc=1, device_id={"dp": lax.rem(dp + d, planes)}, device_id_type=MESH
            )

    column(barrier)
    for c in loads:
        c.start()

    def plane(g):
        high = lax.rem(dp // 2 + g // 2, 2)
        return high * 2 + lax.rem(dp + lax.rem(g, 2), 2)

    def one_hot(mask):
        return jnp.where(mask, 1.0, 0.0).astype(bf)

    def iota(shape, dim):
        return lax.broadcasted_iota(jnp.int32, shape, dim)

    loads[0].wait()
    ids = ids_ref[...]
    named = one_hot(iota((owners, rows), 0) == ids)
    earlier = one_hot(iota((rows, rows), 0) < iota((rows, rows), 1))
    before = jnp.dot(named, earlier, preferred_element_type=f32)
    slot = jnp.sum(named.astype(f32) * before, axis=0, keepdims=True).astype(jnp.int32)
    place_own = ids * cap + slot
    place_all[me] = jnp.broadcast_to(place_own, place_all.shape[1:])
    loads[1].wait()
    local = kept_ref[...] - me * shard
    picks = one_hot(iota((shard, rows), 0) == local)
    loads[2].wait()
    x_all[me] = lax.dot_general(
        picks, doc_ref[...], (((0,), (0,)), ((), ())), preferred_element_type=f32
    ).astype(bf)

    pl.semaphore_wait(barrier, n + planes - 2)
    column(ready)

    o = Gather(n, me, wo_ref, wo_all, o_send, o_recv)

    def bulk(ref, sends, recvs):
        return pltpu.make_async_remote_copy(
            src_ref=ref,
            dst_ref=ref,
            send_sem=sends,
            recv_sem=recvs,
            device_id={"ctx": o.partner},
            device_id_type=MESH,
        )

    def place_copy(d):
        return pltpu.make_async_remote_copy(
            src_ref=place_all.at[me],
            dst_ref=place_all.at[me],
            send_sem=p_send,
            recv_sem=p_recv,
            device_id={"ctx": lax.rem(me + d, n)},
            device_id_type=MESH,
        )

    for d in range(1, n):
        place_copy(d).start()

    core, chip, partner = o.core, o.chip, o.partner
    (near_x, _), (near_y, _) = o.peers()
    part, piece = rows // 2, rows // 4

    def send(ident, block, first, count, target):
        ref = x_all.at[block, pl.ds(pl.multiple_of(first, count), count)]
        return pltpu.make_async_remote_copy(
            src_ref=ref,
            dst_ref=ref,
            send_sem=x_send,
            recv_sem=x_recv.at[ident],
            device_id={"ctx": target},
            device_id_type=MESH,
        )

    to_x, to_y = near_x * 2 + core, near_y * 2 + core
    mine = core * part
    twin = send(0, me, (1 - core) * part, part, partner)
    rest = send(15, me, mine, part, partner)
    own, passed, relays, last = [], [], [], []
    for k in (0, 1):
        from_x, from_y, across = near_x * 2 + k, near_y * 2 + k, (3 - chip) * 2 + k
        own.append(
            (
                send(1 + k, chip * 2 + k, mine, part, to_x),
                send(3 + k, chip * 2 + k, mine, part, to_y),
            )
        )
        passed.append(
            (send(5 + k, from_x, mine, part, partner), send(7 + k, from_y, mine, part, partner))
        )
        relays.append(
            (
                send(9 + k, from_x, mine, piece, to_y),
                send(11 + k, from_y, mine + piece, piece, to_x),
            )
        )
        last.append(send(13 + k, across, mine, part, partner))
    twin.start()

    @pl.when(core == 0)
    def _():
        for c in own[0]:
            c.start()

    blank = jnp.zeros((HS, width), bf)
    for i in (1, 3, 5):
        w3_ref[pl.ds(i * HS, HS), :] = blank
    for c in loads[3:9]:
        c.wait()

    def row_copy(turn, block):
        return pltpu.make_async_remote_copy(
            src_ref=r_out.at[turn - 1, block],
            dst_ref=r_in.at[dp, block],
            send_sem=r_send.at[turn],
            recv_sem=r_recv.at[turn],
            device_id={"dp": plane(turn)},
            device_id_type=MESH,
        )

    def route(block, value):
        index = iota((planes * cap, rows), 0)
        turn, s = index // cap, index % cap
        high = (dp // 2 + turn // 2) % 2
        to = high * 2 + (dp + turn % 2) % 2
        cell = (to * n + me) * cap + s
        taken = jnp.dot(
            one_hot(cell == place_all[block][0:1, :]), value, preferred_element_type=f32
        ).astype(bf)
        r_in[dp, block] = taken[0:cap]
        for turn in (2, 3, 1):
            r_out[turn - 1, block] = taken[turn * cap : (turn + 1) * cap]
            row_copy(turn, block).start()

    def project(spot, value):
        at = pl.ds(pl.multiple_of(spot * rows, rows), rows)
        normed = rms_scale(value, gain_attn_ref[...]).astype(bf)
        three = lax.dot_general(normed, w3_ref[...], LAST, preferred_element_type=f32)
        q_all[at, :] = three[:, 0:wide].astype(bf)
        k_all[at, :] = three[:, wide : 2 * wide].astype(bf)
        lane = iota((rows, wide), 1)
        v_all[at, :] = jnp.where(lane < HS, three[:, 2 * wide : 3 * wide], 1.0).astype(bf)

    def take(block, spot):
        value = x_all[block]
        route(block, value)
        project(spot, value)

    scale = score_gain / math.sqrt(HS) * math.log2(math.e)

    def update(spot, spots, first, count, fresh):
        at = pl.ds(spot * rows, spots * rows)
        keys = pl.ds(first * rows, count * rows)
        scores = lax.dot_general(q_all[at, :], k_all[keys, :], LAST, preferred_element_type=f32)
        top = jnp.broadcast_to(
            jnp.max(scores, axis=1, keepdims=True), (spots * rows, wide)
        )
        if not fresh:
            known = top_ref[at, :]
            top = jnp.maximum(top, known)
        shift = jnp.concatenate([top * scale] * (count * rows // wide), axis=1)
        weights = jnp.exp2(scores * scale - shift)
        both = jnp.dot(weights.astype(bf), v_all[keys, :], preferred_element_type=f32)
        if not fresh:
            both = both + sum_ref[at, :] * jnp.exp2(known * scale - top * scale)
        sum_ref[at, :] = both
        top_ref[at, :] = top

    def match(chip):
        places = [place_all[2 * chip + side][0:1, :] for side in (0, 1)]
        cells_ref[chip] = one_hot(
            iota((owners * cap, 2 * rows), 0) == jnp.concatenate(places, axis=1)
        )

    twin.wait_recv()

    @pl.when(core == 1)
    def _():
        for c in own[0]:
            c.start()

    rest.start()
    for c in own[1]:
        c.start()
    take(me, core)
    for z in range(planes):
        cells = one_hot(iota((share, rows), 0) + z * share == place_own)
        picks_ref[z] = lax.dot_general(picks, cells, LAST, preferred_element_type=f32).astype(bf)
    wo_all[me] = wo_ref[...]
    places = bulk(place_all.at[pl.ds(0, n - 1)], p_send, p_recv)
    places.wait_recv()
    def mixed_copy(turn, d, j):
        to, c = plane(turn), lax.rem(me + d, n)
        lanes = pl.ds(pl.multiple_of(me * wide, wide), wide)
        return pltpu.make_async_remote_copy(
            src_ref=m_out.at[to * n + c, j],
            dst_ref=m_in.at[dp, j, :, lanes],
            send_sem=m_send.at[turn],
            recv_sem=m_recv.at[turn],
            device_id={"dp": to, "ctx": c},
            device_id_type=MESH,
        )

    def mixed_own(j):
        lanes = pl.ds(pl.multiple_of(me * wide, wide), wide)
        return pltpu.make_async_copy(
            m_out.at[dp * n + me, j], m_in.at[dp, j, :, lanes], m_recv.at[0]
        )

    def each(turn, act):
        @pl.loop(0, n)
        def _(d):
            @pl.when(turn + d > 0)
            def _():
                act(turn, d)

    def mixed_copies(turn, act):
        def some(turn, d):
            for j in range(pairs):
                act(mixed_copy(turn, d, j))

        each(turn, some)

    def finish(chip, spots):
        for side, spot in enumerate(spots):
            both = sum_ref[pl.ds(spot * rows, rows), :]
            mixed = jnp.where(iota((rows, wide), 1) < HS, both / pltpu.roll(both, HS, 1), 0.0)
            if side:
                mixed = pltpu.roll(mixed, HS, 1)
            mix_ref[pl.ds(side * rows, rows), :] = mixed.astype(bf)
        spread = jnp.dot(cells_ref[chip], mix_ref[...], preferred_element_type=f32).astype(bf)
        m_out[:, chip] = spread.reshape(owners, cap, wide)
        each(2, lambda turn, d: mixed_copy(turn, d, chip).start())
        each(3, lambda turn, d: mixed_copy(turn, d, chip).start())

    rest.wait_recv()
    take(partner, 1 - core)
    update(0, 2, 0, 2, True)
    for at in range(pairs):
        match(at)
    for c, p, r in zip(own[0], passed[0], relays[0]):
        c.wait_recv()
        p.start()
        r.start()
    for i, near in enumerate((near_x, near_y)):
        passed[0][i].wait_recv()
        take(near * 2, 2 + i)
    update(0, 2, 2, 2, False)
    update(2, 2, 0, 4, True)
    for c, p, r in zip(own[1], passed[1], relays[1]):
        c.wait_recv()
        p.start()
        r.start()
    for i, near in enumerate((near_x, near_y)):
        passed[1][i].wait_recv()
        take(near * 2 + 1, 4 + i)
    update(0, 4, 4, 2, False)
    for r in relays[0]:
        r.wait_recv()
    last[0].start()
    o.begin()
    update(4, 2, 0, 6, True)
    for r in relays[1]:
        r.wait_recv()
    last[1].start()
    for k in (0, 1):
        last[k].wait_recv()
        take((3 - chip) * 2 + k, 6 + k)
    update(0, 6, 6, 2, False)
    o.twin.wait_recv()
    o.relay()
    pl.semaphore_wait(ready, planes - 1)
    finish(chip, (0, 1))
    finish(near_x, (2, 4))
    finish(near_y, (3, 5))
    update(6, 2, 0, 8, True)
    finish(3 - chip, (6, 7))
    o.diagonal()

    inside = lax.rem((dp + 1) // 2, 2)

    def seat(t):
        return (1 - inside) * t + inside * (2 - 2 * t + 5 * (t // 2))

    def back_copy(turn, d):
        to, c = plane(turn), lax.rem(me + d, n)
        return pltpu.make_async_remote_copy(
            src_ref=second_ref.at[to, lax.rem(c, 2), c // 2],
            dst_ref=back_ref.at[dp, me],
            send_sem=b_send.at[turn],
            recv_sem=b_recv.at[turn],
            device_id={"dp": to, "ctx": c},
            device_id_type=MESH,
        )

    mixed_copies(0, lambda c: c.start())
    mixed_copies(1, lambda c: c.start())
    for j in range(pairs):
        mixed_own(j).start()
    touched = jnp.zeros((shard, 1), f32)
    for z in range(planes):
        touched = touched + jnp.sum(picks_ref[z].astype(f32), axis=1, keepdims=True)
    acc_ref[...] = jnp.where(touched > 0.5, 0.0, doc_ref[...].astype(f32))
    for c in loads[9:]:
        c.wait()
    for _, c in o.passed:
        c.wait_recv()
    o.final()

    half = pairs * cap

    @pl.loop(0, planes)
    def _(t):
        turn = seat(t)
        source = plane(turn)
        bulk(m_in.at[source], m_send.at[turn], m_recv.at[turn]).wait_recv()

        @pl.when(turn > 0)
        def _():
            bulk(r_in.at[source], r_send.at[turn], r_recv.at[turn]).wait_recv()

        mixed = m_in[source].reshape(half, n * wide)
        heads = [mixed[:, h * wide : (h + 1) * wide] for h in range(n)]
        low = jnp.concatenate([h[:, :HS] for h in heads], axis=1)
        high = jnp.concatenate([h[:, HS:] for h in heads], axis=1)
        base = [r_in[source, 2 * j + side] for side in (0, 1) for j in range(pairs)]
        first_ref[...] = jnp.concatenate(base, axis=0).astype(f32) + jnp.dot(
            jnp.concatenate([low, high], axis=0),
            wo_all[...].reshape(n * HS, width),
            preferred_element_type=f32,
        )
        ffn_ref[...] = rms_scale(first_ref[...], gain_ffn_ref[...]).astype(bf)
        for f in range(0, inner, 256):
            hidden = jnp.dot(ffn_ref[...], w_in_ref[:, f : f + 256], preferred_element_type=f32)
            hidden_ref[:, f : f + 256] = jnp.maximum(hidden, 0.0).astype(bf)
        for f in range(0, width, 256):
            answer = jnp.dot(
                hidden_ref[...], w_back_ref[:, f : f + 256], preferred_element_type=f32
            ).astype(bf)
            second = (first_ref[:, f : f + 256] + answer.astype(f32)).astype(bf)
            second_ref[source, :, :, :, f : f + 256] = second.reshape(2, pairs, cap, 256)
        each(turn, lambda turn, d: back_copy(turn, d).start())

    pltpu.make_async_copy(
        second_ref.at[dp, lax.rem(me, 2), me // 2], back_ref.at[dp, me], b_recv.at[0]
    ).start()

    def returned(turn):
        source = plane(turn)
        bulk(back_ref.at[source], b_send.at[turn], b_recv.at[turn]).wait_recv()
        return acc_ref[...] + jnp.dot(
            picks_ref[source], back_ref[source].reshape(share, width), preferred_element_type=f32
        )

    for turn in (0, 1, 2):
        acc_ref[...] = returned(turn)

    out_ref[...] = returned(3).astype(bf)

    places.wait_send()

    for turn in range(planes):
        count = n - (turn == 0)
        bulk(m_out.at[pl.ds(0, count)], m_send.at[turn], m_recv.at[turn]).wait_send()
        bulk(back_ref.at[0, pl.ds(0, count)], b_send.at[turn], b_recv.at[turn]).wait_send()
        if turn:
            bulk(r_in.at[0], r_send.at[turn], r_recv.at[turn]).wait_send()
    bulk(x_all.at[pl.ds(0, n - 1)], x_send, x_recv.at[0]).wait_send()
    o.drain()


def whole(document, kept, ids, gain_attn, gain_ffn, w_query, w_key, w_value, w_out, w_in, w_back):
    planes, n = lax.axis_size("dp"), lax.axis_size("ctx")
    owners = planes * n
    shard, width = document.shape
    rows = kept.shape[1]
    cap = 2 * rows // owners
    inner = w_in.shape[2]
    pairs = n // 2
    wide = 2 * HS
    half = pairs * cap
    bf, f32 = jnp.bfloat16, jnp.float32
    vmem = pl.BlockSpec(memory_space=pltpu.VMEM)
    hbm = pl.BlockSpec(memory_space=pltpu.HBM)
    sems = pltpu.SemaphoreType.DMA
    copies = gather_copies(n)
    grant = 42 * 1024 * 1024
    operands = (
        kept,
        ids,
        gain_attn.reshape(1, width),
        gain_ffn.reshape(1, width),
        document,
        w_query.T,
        w_key.T,
        w_value.T,
        w_out,
        w_in,
        w_back,
    )
    return pl.pallas_call(
        functools.partial(whole_kernel, planes, n, cap),
        out_shape=jax.ShapeDtypeStruct((shard, width), bf),
        in_specs=[hbm] * 11,
        out_specs=vmem,
        scratch_shapes=[
            pltpu.VMEM((1, rows), jnp.int32),
            pltpu.VMEM((1, rows), jnp.int32),
            pltpu.VMEM((1, width), f32),
            pltpu.VMEM((1, width), f32),
            pltpu.VMEM((shard, width), bf),
            pltpu.VMEM((6 * HS, width), bf),
            pltpu.VMEM(w_out.shape, bf),
            pltpu.VMEM(w_in.shape[1:], bf),
            pltpu.VMEM(w_back.shape[1:], bf),
            pltpu.VMEM((n, 8, rows), jnp.int32),
            pltpu.VMEM((n, rows, width), bf),
            pltpu.VMEM((n * rows, wide), bf),
            pltpu.VMEM((n * rows, wide), bf),
            pltpu.VMEM((n * rows, wide), bf),
            pltpu.VMEM((n * rows, wide), f32),
            pltpu.VMEM((n * rows, wide), f32),
            pltpu.VMEM((2 * rows, wide), bf),
            pltpu.VMEM((n // 2, owners * cap, 2 * rows), bf),
            pltpu.VMEM((owners, pairs, cap, wide), bf),
            pltpu.VMEM((planes, pairs, cap, n * wide), bf),
            pltpu.VMEM((n,) + w_out.shape, bf),
            pltpu.VMEM((planes - 1, n, cap, width), bf),
            pltpu.VMEM((planes, n, cap, width), bf),
            pltpu.VMEM((2 * half, width), f32),
            pltpu.VMEM((2 * half, width), bf),
            pltpu.VMEM((2 * half, inner), bf),
            pltpu.VMEM((planes, 2, pairs, cap, width), bf),
            pltpu.VMEM((planes, n, cap, width), bf),
            pltpu.VMEM((planes, shard, n * cap), bf),
            pltpu.VMEM((shard, width), f32),
            sems((12,)),
            sems(()),
            sems(()),
            sems(()),
            sems((16,)),
            sems((copies,)),
            sems((copies,)),
            sems((planes,)),
            sems((planes,)),
            sems((planes,)),
            sems((planes,)),
            sems((planes,)),
            sems((planes,)),
            pltpu.SemaphoreType.REGULAR,
        ],
        compiler_params=pltpu.CompilerParams(
            collective_id=2, has_side_effects=True, vmem_limit_bytes=grant
        ),
        name="whole",
    )(*[pltpu.with_memory_space_constraint(a, pltpu.HBM) for a in operands])


def fits_whole(planes, n, keep_here, w_query, w_out, w_in):
    cap = 2 * keep_here // (planes * n)
    return (
        planes == 4
        and n == 8
        and w_query.shape[1] == HS
        and w_out.shape[0] == HS
        and w_in.shape[0] == 1
        and cap % 16 == 0
        and w_in.shape[2] % 256 == 0
    )


def body(
    tokens, kept, gain_attn, gain_ffn, w_query, w_key, w_value, w_out, expert_ids, w_in, w_back
):
    document = tokens[0]
    shard_len, width_model = document.shape
    ctx_count = lax.axis_size("ctx")
    dp_count = lax.axis_size("dp")
    if fits_whole(dp_count, ctx_count, kept.shape[1], w_query, w_out, w_in):
        ids = expert_ids.reshape(1, kept.shape[1])
        weights = (w_query, w_key, w_value, w_out, w_in, w_back)
        return whole(document, kept, ids, gain_attn, gain_ffn, *weights)[None]
    local = kept[0] - lax.axis_index("ctx") * shard_len
    keep_here = local.shape[0]
    positions = jnp.arange(shard_len, dtype=jnp.int32)
    picks = (local[:, None] == positions[None, :]).astype(jnp.bfloat16)
    rows = jnp.dot(picks, document, preferred_element_type=jnp.float32).astype(jnp.bfloat16)
    normed = rms_scale(rows, gain_attn).astype(jnp.bfloat16)
    mixed, w_out_all = attention(normed, w_query, w_key, w_value, w_out)
    inner_all = w_out.shape[0] * ctx_count
    attn = lax.dot_general(
        mixed.reshape(inner_all, keep_here),
        w_out_all.reshape(inner_all, width_model),
        (((0,), (0,)), ((), ())),
        preferred_element_type=jnp.float32,
    )
    first = rows.astype(jnp.float32) + attn
    ffn_in = rms_scale(first, gain_ffn).astype(jnp.bfloat16)
    expert_here = w_in.shape[0]
    owners = dp_count * ctx_count
    experts_all = expert_here * owners
    capacity = 2 * keep_here // experts_all
    labels = expert_ids[0, :, 0]
    order = jnp.arange(keep_here, dtype=jnp.int32)
    same = (labels[:, None] == labels[None, :]) & (order[None, :] < order[:, None])
    slots = jnp.sum(same.astype(jnp.int32), axis=1)
    place = labels * capacity + slots
    cells = jnp.arange(experts_all * capacity, dtype=jnp.int32)
    spots = (place[None, :] == cells[:, None]).astype(jnp.bfloat16)
    buffer = jnp.dot(spots, ffn_in, preferred_element_type=jnp.float32).astype(jnp.bfloat16)
    answers = experts(buffer, w_in, w_back, capacity)
    seats = (place[:, None] == cells[None, :]).astype(jnp.bfloat16)
    taken = jnp.dot(seats, answers, preferred_element_type=jnp.float32)
    second = (first + taken).astype(jnp.bfloat16)
    hits = positions[:, None] == local[None, :]
    fresh = jnp.dot(hits.astype(jnp.bfloat16), second, preferred_element_type=jnp.float32)
    touched = jnp.any(hits, axis=1, keepdims=True)
    blended = jnp.where(touched, fresh.astype(jnp.bfloat16), document)
    return blended[None]


def solution(mesh):
    return jax.shard_map(
        body,
        mesh=mesh,
        in_specs=(
            P("dp", "ctx", None),
            P("dp", "ctx"),
            P(),
            P(),
            P(None, "ctx"),
            P(None, "ctx"),
            P(None, "ctx"),
            P("ctx", None),
            P("dp", "ctx", None),
            P(("dp", "ctx"), None, None),
            P(("dp", "ctx"), None, None),
        ),
        out_specs=P("dp", "ctx", None),
        check_vma=False,
    )
```
